8 devices in a mesh: dp: 1 (over z), tp: 2 (over y), sq: 4 (over x, core).
Axes of the slice: x: 2, y: 2, z: 1, core: 2. Of those that a mesh axis runs over, the one named last changes fastest.
Arguments:
- x_steps: bfloat16 [4, 48, 4608], P(None, 'dp')
- positions: int32 [48], P('dp')
- k_cache: bfloat16 [48, 4096, 4, 128], P('dp', 'sq', 'tp')
- v_cache: bfloat16 [48, 4096, 4, 128], P('dp', 'sq', 'tp')
- w_q: bfloat16 [4608, 4608], P(None, 'tp')
- b_q: bfloat16 [4608], P('tp')
- w_k: bfloat16 [4608, 512], P(None, 'tp')
- b_k: bfloat16 [512], P('tp')
- w_v: bfloat16 [4608, 512], P(None, 'tp')
- b_v: bfloat16 [512], P('tp')
- w_o: bfloat16 [4608, 4608], P('tp')
- b_o: bfloat16 [4608], replicated
- ln1_gain: bfloat16 [4608], replicated
- ln1_bias: bfloat16 [4608], replicated
- ln2_gain: bfloat16 [4608], replicated
- ln2_bias: bfloat16 [4608], replicated
- w_fc: bfloat16 [4608, 18432], P(None, 'tp')
- b_fc: bfloat16 [18432], P('tp')
- w_proj: bfloat16 [18432, 4608], P('tp')
- b_proj: bfloat16 [4608], replicated
Outputs:
- output 1: bfloat16 [4, 48, 4608], P(None, 'dp')
- output 2: bfloat16 [48, 4096, 4, 128], P('dp', 'sq', 'tp')
- output 3: bfloat16 [48, 4096, 4, 128], P('dp', 'sq', 'tp')
All inputs are finite; a program needn't handle non-finite values.
Results may differ from the reference program's by a relative error of at most 0.0162477.
Values sent between devices are 32-bit elements.
A program may use at most 1.25 GiB of HBM per device.

```python
import jax
import jax.numpy as jnp
from jax import lax

D = 4608
HEADS = 36
KV_HEADS = 4
HEAD = 128
FF = 18432
WINDOW = 4096
BATCH = 48
STEPS = 4
ROPE_BASE = 1000000
POS_LOW = 100
POS_HIGH = 15000
HOT_ODDS = 512
HOT_RUN = 8


def rope_tables(positions, head_dim):
    half_dim = head_dim // 2
    inv_freq = jnp.power(jnp.float32(ROPE_BASE), -2.0 * jnp.arange(half_dim, dtype=jnp.float32) / head_dim)
    angle = positions.astype(jnp.float32)[..., None] * inv_freq
    return jnp.cos(angle), jnp.sin(angle)


def apply_rope(vectors, cos_t, sin_t):
    half_dim = vectors.shape[-1] // 2
    first = vectors[..., :half_dim]
    second = vectors[..., half_dim:]
    return jnp.concatenate([first * cos_t - second * sin_t, second * cos_t + first * sin_t], axis=-1)


def layer_norm(vectors, gain, shift):
    row_mean = jnp.mean(vectors, axis=-1, keepdims=True)
    centered = vectors - row_mean
    row_var = jnp.mean(centered * centered, axis=-1, keepdims=True)
    return centered * lax.rsqrt(row_var + 1e-5) * gain.astype(jnp.float32) + shift.astype(jnp.float32)


def linear(rows_in, weight, bias):
    return jnp.dot(rows_in, weight, preferred_element_type=jnp.float32) + bias.astype(jnp.float32)


def hot_direction():
    dim_ids = jnp.arange(HEAD)
    marked = (dim_ids % (HEAD // 2)) >= HEAD // 2 - 4
    return jnp.where(marked, 8.0 ** -0.5, 0.0).astype(jnp.float32)


def draw_positions(key):
    key_low, key_high, key_pick, key_perm = jax.random.split(key, 4)
    short = jax.random.randint(key_low, (BATCH,), POS_LOW, WINDOW)
    longer = jax.random.randint(key_high, (BATCH,), WINDOW, POS_HIGH + 1)
    chooser = jax.random.randint(key_pick, (BATCH,), 0, 4)
    mixed = jnp.where(chooser == 0, short, longer)
    mixed = mixed.at[0].set(POS_LOW).at[1].set(POS_HIGH)
    return jax.random.permutation(key_perm, mixed).astype(jnp.int32)


def setup_inputs(seed: int = 0, part: int = 0) -> dict:
    shared = jax.random.split(jax.random.key(seed), 16)
    own = jax.random.split(jax.random.fold_in(jax.random.key(seed + 1), part), 5)
    hot_amp = (8.0 * HEAD ** 0.5) ** 0.5
    hot_vec = hot_direction() * hot_amp
    positions = draw_positions(own[0])
    slot_ids = jnp.arange(WINDOW, dtype=jnp.int32)
    last_pos = positions[:, None] - 1
    held_pos = last_pos - (last_pos - slot_ids[None, :]) % WINDOW
    hot_slot = (jax.random.randint(own[1], (BATCH, WINDOW), 0, HOT_ODDS) == 0) | ((slot_ids[None, :] - positions[:, None]) % WINDOW < HOT_RUN)
    cos_t, sin_t = rope_tables(held_pos, HEAD)
    hot_keys = apply_rope(jnp.broadcast_to(hot_vec, (BATCH, WINDOW, HEAD)), cos_t, sin_t)
    hot_keys = jnp.where(hot_slot[:, :, None], hot_keys, 0.0)
    k_cache = (jax.random.normal(own[2], (BATCH, WINDOW, KV_HEADS, HEAD), jnp.float32) + hot_keys[:, :, None, :]).astype(jnp.bfloat16)
    v_cache = jax.random.normal(own[3], (BATCH, WINDOW, KV_HEADS, HEAD), jnp.float32).astype(jnp.bfloat16)
    x_steps = jax.random.normal(own[4], (STEPS, BATCH, D), jnp.float32).astype(jnp.bfloat16)

    def scaled(key, shape, scale):
        return (jax.random.normal(key, shape, jnp.float32) * scale).astype(jnp.bfloat16)

    b_q = (0.5 * jax.random.normal(shared[1], (HEADS * HEAD,), jnp.float32) + jnp.tile(hot_vec, HEADS)).astype(jnp.bfloat16)
    b_k = (0.5 * jax.random.normal(shared[3], (KV_HEADS * HEAD,), jnp.float32) + jnp.tile(hot_vec, KV_HEADS)).astype(jnp.bfloat16)
    return {
        "x_steps": x_steps,
        "positions": positions,
        "k_cache": k_cache,
        "v_cache": v_cache,
        "w_q": scaled(shared[0], (D, HEADS * HEAD), D ** -0.5),
        "b_q": b_q,
        "w_k": scaled(shared[2], (D, KV_HEADS * HEAD), D ** -0.5),
        "b_k": b_k,
        "w_v": scaled(shared[4], (D, KV_HEADS * HEAD), D ** -0.5),
        "b_v": scaled(shared[5], (KV_HEADS * HEAD,), 0.5),
        "w_o": scaled(shared[6], (HEADS * HEAD, D), 3.0 * (HEADS * HEAD) ** -0.5),
        "b_o": scaled(shared[7], (D,), 0.2),
        "ln1_gain": (1.0 + 0.2 * jax.random.normal(shared[8], (D,), jnp.float32)).astype(jnp.bfloat16),
        "ln1_bias": scaled(shared[9], (D,), 0.2),
        "ln2_gain": (1.0 + 0.2 * jax.random.normal(shared[10], (D,), jnp.float32)).astype(jnp.bfloat16),
        "ln2_bias": scaled(shared[11], (D,), 0.2),
        "w_fc": scaled(shared[12], (D, FF), D ** -0.5),
        "b_fc": scaled(shared[13], (FF,), 0.5),
        "w_proj": scaled(shared[14], (FF, D), 1.5 * FF ** -0.5),
        "b_proj": scaled(shared[15], (D,), 0.2),
    }


def reference(x_steps, positions, k_cache, v_cache, w_q, b_q, w_k, b_k, w_v, b_v, w_o, b_o,
              ln1_gain, ln1_bias, ln2_gain, ln2_bias, w_fc, b_fc, w_proj, b_proj):
    group = HEADS // KV_HEADS
    slot_ids = jnp.arange(WINDOW, dtype=jnp.int32)
    batch_ids = jnp.arange(BATCH, dtype=jnp.int32)
    score_scale = HEAD ** -0.5

    def attend_one(packed):
        q_one, k_one, v_one, slot_ok = packed
        scores = jnp.einsum("grd,wgd->grw", q_one.reshape(KV_HEADS, group, HEAD).astype(jnp.float32), k_one.astype(jnp.float32)) * score_scale
        scores = jnp.where(slot_ok[None, None, :], scores, -1e30)
        weights = jax.nn.softmax(scores, axis=-1)
        return jnp.einsum("grw,wgd->grd", weights, v_one.astype(jnp.float32))

    def one_step(carry, step_in):
        key_buf, val_buf = carry
        x_in, step_idx = step_in
        cur_pos = positions + step_idx
        hidden = layer_norm(x_in.astype(jnp.float32), ln1_gain, ln1_bias).astype(jnp.bfloat16)
        query = linear(hidden, w_q, b_q).astype(jnp.bfloat16)
        key_new = linear(hidden, w_k, b_k).astype(jnp.bfloat16)
        val_new = linear(hidden, w_v, b_v).astype(jnp.bfloat16)
        cos_t, sin_t = rope_tables(cur_pos, HEAD)
        q_rot = apply_rope(query.reshape(BATCH, HEADS, HEAD).astype(jnp.float32), cos_t[:, None, :], sin_t[:, None, :]).astype(jnp.bfloat16)
        k_rot = apply_rope(key_new.reshape(BATCH, KV_HEADS, HEAD).astype(jnp.float32), cos_t[:, None, :], sin_t[:, None, :]).astype(jnp.bfloat16)
        write_slot = cur_pos % WINDOW
        key_buf = key_buf.at[batch_ids, write_slot].set(k_rot)
        val_buf = val_buf.at[batch_ids, write_slot].set(val_new.reshape(BATCH, KV_HEADS, HEAD))
        held_pos = cur_pos[:, None] - (cur_pos[:, None] - slot_ids[None, :]) % WINDOW
        attn = lax.map(attend_one, (q_rot, key_buf, val_buf, held_pos >= 0))
        attn_out = attn.astype(jnp.bfloat16).reshape(BATCH, HEADS * HEAD)
        x_mid = (x_in.astype(jnp.float32) + jnp.dot(attn_out, w_o, preferred_element_type=jnp.float32) + b_o.astype(jnp.float32)).astype(jnp.bfloat16)
        hidden_two = layer_norm(x_mid.astype(jnp.float32), ln2_gain, ln2_bias).astype(jnp.bfloat16)
        gelu_out = jax.nn.gelu(linear(hidden_two, w_fc, b_fc), approximate=True).astype(jnp.bfloat16)
        y_out = (x_mid.astype(jnp.float32) + jnp.dot(gelu_out, w_proj, preferred_element_type=jnp.float32) + b_proj.astype(jnp.float32)).astype(jnp.bfloat16)
        return (key_buf, val_buf), y_out

    (k_final, v_final), y_steps = lax.scan(one_step, (k_cache, v_cache), (x_steps, jnp.arange(STEPS, dtype=jnp.int32)))
    return y_steps, k_final, v_final
```

```python
import functools
import math

import jax
import jax.numpy as jnp
from jax import lax
from jax.experimental import pallas as pl
from jax.experimental.pallas import tpu as pltpu
from jax.sharding import PartitionSpec as P

ROPE_BASE = 1000000.0
LN_EPS = 1e-5
NEG_BIG = -1e30
NEG_HALF = -1e29
LOG2E = 1.4426950408889634
VMEM_CAP = 67_043_328
F32 = jnp.float32
BF16 = jnp.bfloat16
LANES = 128


def layer_norm(vectors, gain, shift):
    row_mean = jnp.mean(vectors, axis=-1, keepdims=True)
    centered = vectors - row_mean
    row_var = jnp.mean(centered * centered, axis=-1, keepdims=True)
    return centered * lax.rsqrt(row_var + LN_EPS) * gain.astype(F32) + shift.astype(F32)


def rope_tables(positions, head_dim):
    half_dim = head_dim // 2
    inv_freq = jnp.power(F32(ROPE_BASE), -2.0 * jnp.arange(half_dim, dtype=F32) / head_dim)
    angle = positions.astype(F32)[..., None] * inv_freq
    return jnp.cos(angle), jnp.sin(angle)


def apply_rope(vectors, cos_t, sin_t):
    half_dim = vectors.shape[-1] // 2
    first = vectors[..., :half_dim]
    second = vectors[..., half_dim:]
    return jnp.concatenate([first * cos_t - second * sin_t, second * cos_t + first * sin_t], axis=-1)


def linear(rows_in, weight, bias):
    return jnp.einsum("sbd,dn->sbn", rows_in, weight, preferred_element_type=F32) + bias.astype(F32)


def attend_kernel(cfg, meta, q_ref, kn_ref, vn_ref, k_ref, v_ref, ko_ref, vo_ref, o_ref, lse_ref, o_rows, stat_rows):
    steps, kvs, group, per, slots = cfg
    rows = k_ref.shape[1]
    tile = steps * kvs
    inner = pl.program_id(1)
    base = (pl.program_id(0) * pl.num_programs(1) + inner) * per
    first = meta[0]
    coef = LANES ** -0.5 * LOG2E
    contract_last = (((1,), (1,)), ((), ()))

    sub = lax.broadcasted_iota(jnp.int32, (tile, rows), 0)
    lane = lax.broadcasted_iota(jnp.int32, (tile, rows), 1)
    own_head = (lane % kvs) == (sub // steps)
    slot = first + lane // kvs
    sub2 = lax.broadcasted_iota(jnp.int32, (tile, kn_ref.shape[1]), 0)
    lane2 = lax.broadcasted_iota(jnp.int32, (tile, kn_ref.shape[1]), 1)
    new_head = (lane2 % kvs) == (sub2 // steps)
    new_step = lane2 // kvs
    stat_sub = lax.broadcasted_iota(jnp.int32, (tile, LANES), 0)
    stat_lane = lax.broadcasted_iota(jnp.int32, (tile, LANES), 1) - (stat_sub // steps) * group
    win_row = lax.broadcasted_iota(jnp.int32, (16, LANES), 0)

    for one in range(per):
        pos = meta[1 + base + one]
        q = q_ref[one]
        for src, dst, new in ((k_ref, ko_ref, kn_ref), (v_ref, vo_ref, vn_ref)):
            dst[one] = src[one]
            fresh = new[one].astype(F32)
            for t in range(steps):
                row = kvs * ((pos + t) % slots - first)
                start = pl.multiple_of(jnp.clip(row // 16, 0, rows // 16 - 1) * 16, 16)
                window = dst[one, pl.ds(start, 16), :].astype(F32)
                offset = win_row + (start - row)
                for h in range(kvs):
                    window = jnp.where(offset == h, fresh[t * kvs + h:t * kvs + h + 1, :], window)
                dst[one, pl.ds(start, 16), :] = window.astype(BF16)
        ahead = (slot - pos) & (slots - 1)
        bias = jnp.where(own_head & (slot < pos) & (ahead > sub % steps), 0.0, NEG_BIG).astype(F32)
        new_slot = ((pos + new_step) & (slots - 1)) - first
        here = (new_slot >= 0) & (new_slot < rows // kvs)
        bias2 = jnp.where(new_head & (new_step <= sub2 % steps) & here, 0.0, NEG_BIG).astype(F32)
        raw = lax.dot_general(q, k_ref[one], contract_last, preferred_element_type=F32)
        raw2 = lax.dot_general(q, kn_ref[one], contract_last, preferred_element_type=F32)
        score = raw.reshape(group, tile, rows) * coef + bias[None]
        score2 = raw2.reshape(group, tile, -1) * coef + bias2[None]
        top = jnp.maximum(jnp.max(score, axis=-1, keepdims=True), jnp.max(score2, axis=-1, keepdims=True))
        top = jnp.maximum(top, NEG_HALF)
        w = jnp.exp2(score - top)
        w2 = jnp.exp2(score2 - top)
        total = jnp.sum(w, axis=-1, keepdims=True) + jnp.sum(w2, axis=-1, keepdims=True)
        out = jnp.dot(w.reshape(group * tile, rows).astype(BF16), v_ref[one], preferred_element_type=F32)
        out = out + jnp.dot(w2.reshape(group * tile, -1).astype(BF16), vn_ref[one], preferred_element_type=F32)
        some = total > 0.0
        safe = jnp.where(some, total, 1.0)
        lse = jnp.where(some, top + jnp.log2(safe), NEG_BIG)
        out = out.reshape(group, tile, LANES) * (1.0 / safe)
        stats = jnp.zeros((tile, LANES), F32)
        for i in range(group):
            stats = jnp.where(stat_lane == i, lse[i], stats)
        seat = inner * per + one
        o_rows[pl.ds(pl.multiple_of(seat * (group * tile), 8), group * tile), :] = out.reshape(group * tile, LANES)
        stat_rows[pl.ds(pl.multiple_of(seat * tile, 8), tile), :] = stats

    @pl.when(inner == pl.num_programs(1) - 1)
    def _():
        for s in range(steps):
            lse_ref[s] = sum(stat_rows[pl.ds(h * steps + s, 8, stride=tile), :] for h in range(kvs))
            for h in range(kvs):
                for i in range(group):
                    col = (h * group + i) * LANES
                    o_ref[s, :, col:col + LANES] = o_rows[pl.ds(i * tile + h * steps + s, 8, stride=group * tile), :]


def attend(meta, q, k_new, v_new, k_rows, v_rows, steps, kvs, group, slots):
    batch, rows, dim = k_rows.shape
    per, eight = 2, 8
    inner = eight // per
    cfg = (steps, kvs, group, per, slots)
    seq = lambda g, j, meta: (g * inner + j, 0, 0)
    wide = lambda g, j, meta: (0, g, 0)
    cache_spec = pl.BlockSpec((per, rows, dim), seq)
    return pl.pallas_call(
        functools.partial(attend_kernel, cfg),
        grid_spec=pltpu.PrefetchScalarGridSpec(
            num_scalar_prefetch=1,
            grid=(batch // eight, inner),
            in_specs=[
                pl.BlockSpec((per, q.shape[1], dim), seq),
                pl.BlockSpec((per, k_new.shape[1], dim), seq),
                pl.BlockSpec((per, v_new.shape[1], dim), seq),
                cache_spec,
                cache_spec,
            ],
            out_specs=[
                cache_spec,
                cache_spec,
                pl.BlockSpec((steps, eight, kvs * group * dim), wide),
                pl.BlockSpec((steps, eight, LANES), wide),
            ],
            scratch_shapes=[
                pltpu.VMEM((eight * q.shape[1], dim), F32),
                pltpu.VMEM((eight * steps * kvs, dim), F32),
            ],
        ),
        out_shape=[
            jax.ShapeDtypeStruct(k_rows.shape, BF16),
            jax.ShapeDtypeStruct(v_rows.shape, BF16),
            jax.ShapeDtypeStruct((steps, batch, kvs * group * dim), F32),
            jax.ShapeDtypeStruct((steps, batch, LANES), F32),
        ],
        compiler_params=pltpu.CompilerParams(dimension_semantics=("arbitrary", "arbitrary")),
        cost_estimate=pl.CostEstimate(flops=4 * batch * rows * q.shape[1] * dim, bytes_accessed=8 * batch * rows * dim,
                                      transcendentals=batch * rows * q.shape[1]),
        name="attend",
    )(meta, q, k_new, v_new, k_rows, v_rows)


CHUNK = 512
RING = 6
(C_PEER_O, C_STAT, C_OWN_O, C_X_O, C_X_E, C_RS_CORE, C_RS_Y, C_AG_Y, C_AG_OWN, C_AG_FWD) = range(10)
(J_RS_CORE, J_RS_Y, J_OWN_Y, J_OWN_X, J_OWN_C, J_FWD_X, J_FWD_C, J_XOWN_C, J_XFWD_C) = range(9)


def tail_kernel(cfg, o_ref, lse_ref, x_ref, wo_hbm, wfc_hbm, wproj_hbm, bo_ref, gain_ref, shift_ref, bfc_ref, bproj_ref,
                y_ref,
                in_o_peer, in_o_own, in_lse, to_x, to_x_e, mine, in_x, in_x_e, a_buf,
                wo_buf, part, in_part, half_sum, in_y, x_buf, x_mid, hid, hid_b,
                ring, g_buf, p_chunk, in_rc, p_half, in_ry, y_all,
                send_a, recv_a, send_j, recv_j, wo_sem, x_sem, ring_sem):
    steps, batch, group, chunks, kvs = cfg
    half = batch // 2
    quarter = half
    d_model = wo_hbm.shape[1]
    head_cols = group * LANES
    ff_own = wfc_hbm.shape[1] // 2
    y = lax.axis_index("tp")
    sq = lax.axis_index("sq")
    x, c = sq // 2, sq % 2
    sib = {"sq": x * 2 + 1 - c}
    xpeer = {"sq": (1 - x) * 2 + c}
    ypeer = {"tp": 1 - y}
    MESH = pl.DeviceIdType.MESH
    my_step = 2 * c + y

    def load_item(item, slot):
        @pl.when(item < chunks)
        def _():
            col = pl.multiple_of(c * ff_own + item * CHUNK, CHUNK)
            pltpu.make_async_copy(wfc_hbm.at[:, pl.ds(col, CHUNK)], ring.at[slot], ring_sem.at[slot]).start()

        @pl.when(item >= chunks)
        def _():
            col = pl.multiple_of((item - chunks) * CHUNK, CHUNK)
            row = pl.multiple_of(c * ff_own, CHUNK)
            pltpu.make_async_copy(wproj_hbm.at[pl.ds(row, ff_own), pl.ds(col, CHUNK)], ring.at[slot], ring_sem.at[slot]).start()

    def wait_item(slot):
        pltpu.make_async_copy(wfc_hbm.at[:, pl.ds(0, CHUNK)], ring.at[slot], ring_sem.at[slot]).wait()

    wo_copy = pltpu.make_async_copy(wo_hbm.at[pl.ds(pl.multiple_of(c * head_cols, LANES), head_cols), :], wo_buf, wo_sem)
    wo_copy.start()
    x_copy = pltpu.make_async_copy(x_ref.at[my_step, pl.ds(pl.multiple_of(x * half, 8), half), :], x_buf, x_sem)
    x_copy.start()
    for k in range(RING):
        load_item(jnp.int32(k), k)

    barrier = pltpu.get_barrier_semaphore()
    for who in (sib, xpeer, ypeer):
        pl.semaphore_signal(barrier, inc=1, device_id=who, device_id_type=MESH)
    pl.semaphore_wait(barrier, 3)

    def remote(src, dst, kind, who):
        return pltpu.make_async_remote_copy(src_ref=src, dst_ref=dst, send_sem=send_a.at[kind], recv_sem=recv_a.at[kind],
                                            device_id=who, device_id_type=MESH)

    peer_rows = pl.ds(pl.multiple_of((1 - x) * half, 8), half)
    own_rows = pl.ds(pl.multiple_of(x * half, 8), half)
    sib_cols = pl.ds(pl.multiple_of((1 - c) * head_cols, LANES), head_cols)
    cp_stat = remote(lse_ref, in_lse, C_STAT, sib)
    cp_peer = remote(o_ref.at[:, peer_rows, sib_cols], in_o_peer, C_PEER_O, sib)
    cp_own = remote(o_ref.at[:, own_rows, sib_cols], in_o_own, C_OWN_O, sib)
    cp_stat.start()
    cp_peer.start()
    cp_own.start()

    def my_lanes(stat):
        return jnp.where(c == 0, stat, pltpu.roll(stat, LANES - group, 1))

    def weights_of(e1, e2):
        top = jnp.maximum(e1, e2)
        w1 = jnp.exp2(e1 - top)
        w2 = jnp.exp2(e2 - top)
        tot = w1 + w2
        inv = 1.0 / tot
        return w1 * inv, w2 * inv, top + jnp.log2(tot)

    def merge_core(rows, incoming, out, keep_e):
        for s in range(steps):
            w1, w2, e = weights_of(my_lanes(lse_ref[s, rows, :]), my_lanes(in_lse[s, rows, :]))
            keep_e[s] = e
            for i in range(group):
                col = pl.ds(pl.multiple_of(c * head_cols + i * LANES, LANES), LANES)
                out[s, :, i * LANES:(i + 1) * LANES] = (w1[:, i:i + 1] * o_ref[s, rows, col]
                                                        + w2[:, i:i + 1] * incoming[s, :, i * LANES:(i + 1) * LANES])

    mine_e = hid.at[pl.ds(0, steps * half), pl.ds(0, LANES)]
    cp_stat.wait_recv()
    cp_peer.wait_recv()
    merge_core(peer_rows, in_o_peer, to_x, to_x_e)
    cp_xe = remote(to_x_e, in_x_e, C_X_E, xpeer)
    cp_xo = remote(to_x, in_x, C_X_O, xpeer)
    cp_xe.start()
    cp_xo.start()
    cp_own.wait_recv()
    for s in range(steps):
        w1, w2, e = weights_of(my_lanes(lse_ref[s, own_rows, :]), my_lanes(in_lse[s, own_rows, :]))
        mine_e[s * half:(s + 1) * half, :] = e
        for i in range(group):
            col = pl.ds(pl.multiple_of(c * head_cols + i * LANES, LANES), LANES)
            mine[s, :, i * LANES:(i + 1) * LANES] = (w1[:, i:i + 1] * o_ref[s, own_rows, col]
                                                     + w2[:, i:i + 1] * in_o_own[s, :, i * LANES:(i + 1) * LANES])
    x_copy.wait()
    cp_xe.wait_recv()
    cp_xo.wait_recv()
    w1, w2, _ = weights_of(mine_e[...], in_x_e[...].reshape(steps * half, LANES))
    for i in range(group):
        cols = slice(i * LANES, (i + 1) * LANES)
        a_buf[:, cols] = (w1[:, i:i + 1] * mine[:, :, cols].reshape(steps * half, LANES)
                          + w2[:, i:i + 1] * in_x[:, :, cols].reshape(steps * half, LANES)).astype(BF16)

    wo_copy.wait()

    @pl.loop(0, chunks)
    def _(j):
        cols = pl.ds(pl.multiple_of(j * CHUNK, CHUNK), CHUNK)
        part[:, cols] = jnp.dot(a_buf[...], wo_buf[:, cols], preferred_element_type=F32)

    def step_rows(s, n=1):
        return pl.ds(pl.multiple_of(s * half, 8), n * half)

    cp_rs = remote(part.at[step_rows(2 * (1 - c), 2), :], in_part, C_RS_CORE, sib)
    cp_rs.start()
    cp_rs.wait_recv()
    half_sum[...] = part[step_rows(2 * c, 2), :] + in_part[...]
    cp_ry = remote(half_sum.at[step_rows(1 - y), :], in_y, C_RS_Y, ypeer)
    cp_ry.start()
    cp_ry.wait_recv()
    x_new = (x_buf[...] + (half_sum[step_rows(y), :] + in_y[...]) + bo_ref[...]).astype(BF16).astype(F32)
    x_mid[...] = x_new
    mean = jnp.mean(x_new, axis=-1, keepdims=True)
    cent = x_new - mean
    var = jnp.mean(cent * cent, axis=-1, keepdims=True)
    normed = cent * lax.rsqrt(var + LN_EPS) * gain_ref[...] + shift_ref[...]
    hid[step_rows(my_step), :] = normed.astype(BF16).astype(F32)

    own_h = hid.at[step_rows(my_step), :]
    peer_h = hid.at[step_rows(2 * c + 1 - y), :]
    cp_ay = remote(own_h, own_h, C_AG_Y, ypeer)
    cp_ac = remote(own_h, own_h, C_AG_OWN, sib)
    cp_ay.start()
    cp_ac.start()
    cp_ay.wait_recv()
    cp_af = remote(peer_h, peer_h, C_AG_FWD, sib)
    cp_af.start()
    cp_ac.wait_recv()
    cp_af.wait_recv()
    hid_b[...] = hid[...].astype(BF16)

    @pl.loop(0, chunks)
    def _(j):
        slot = lax.rem(j, RING)
        wait_item(slot)
        pre = jnp.dot(hid_b[...], ring[slot], preferred_element_type=F32) + bfc_ref[pl.ds(c * chunks + j, 1), :]
        cube = pre * pre * pre
        act = 0.5 * pre * (1.0 + jnp.tanh(math.sqrt(2.0 / math.pi) * (pre + 0.044715 * cube)))
        g_buf[:, pl.ds(pl.multiple_of(j * CHUNK, CHUNK), CHUNK)] = act.astype(BF16)
        load_item(j + RING, slot)

    def jcopy(src, dst, kind, j, who):
        return pltpu.make_async_remote_copy(src_ref=src, dst_ref=dst, send_sem=send_j.at[kind, j], recv_sem=recv_j.at[kind, j],
                                            device_id=who, device_id_type=MESH)

    def rs_core(j):
        return jcopy(p_chunk.at[j, step_rows(2 * (1 - c), 2), :], in_rc.at[j], J_RS_CORE, j, sib)

    def rs_y(j):
        return jcopy(p_half.at[j, step_rows(1 - y), :], in_ry.at[j], J_RS_Y, j, ypeer)

    def block(j, s, xx):
        return y_all.at[j, s, pl.ds(pl.multiple_of(xx * half, 8), half), :]

    def spread(kind, j):
        own = block(j, my_step, x)
        ypart = block(j, 2 * c + 1 - y, x)
        xpart = block(j, my_step, 1 - x)
        diag = block(j, 2 * c + 1 - y, 1 - x)
        ref, who = {J_OWN_Y: (own, ypeer), J_OWN_X: (own, xpeer), J_OWN_C: (own, sib),
                    J_FWD_X: (ypart, xpeer), J_FWD_C: (ypart, sib),
                    J_XOWN_C: (xpart, sib), J_XFWD_C: (diag, sib)}[kind]
        return jcopy(ref, ref, kind, j, who)

    def stage(it, lag, body):
        j = it - lag

        @pl.when((j >= 0) & (j < chunks))
        def _():
            body(j)

    def do_product(j):
        item = chunks + j
        slot = lax.rem(item, RING)
        wait_item(slot)
        p_chunk[j] = jnp.dot(g_buf[...], ring[slot], preferred_element_type=F32)

        @pl.when(item + RING < 2 * chunks)
        def _():
            load_item(item + RING, slot)

        rs_core(j).start()

    def do_core_sum(j):
        rs_core(j).wait_recv()
        p_half[j] = p_chunk[j, step_rows(2 * c, 2), :] + in_rc[j]
        rs_y(j).start()

    def do_y_sum(j):
        rs_y(j).wait_recv()
        cols = pl.ds(pl.multiple_of(j * CHUNK, CHUNK), CHUNK)
        full = x_mid[:, cols] + (p_half[j, step_rows(y), :] + in_ry[j]) + bproj_ref[:, cols]
        y_all[j, my_step, pl.ds(pl.multiple_of(x * half, 8), half), :] = full.astype(BF16).astype(F32)
        for kind in (J_OWN_Y, J_OWN_X, J_OWN_C):
            spread(kind, j).start()

    def do_forward(j):
        spread(J_OWN_Y, j).wait_recv()
        spread(J_FWD_X, j).start()
        spread(J_FWD_C, j).start()
        spread(J_OWN_X, j).wait_recv()
        spread(J_XOWN_C, j).start()

    def do_diag(j):
        spread(J_FWD_X, j).wait_recv()
        spread(J_XFWD_C, j).start()

    def do_store(j):
        for kind in (J_OWN_C, J_FWD_C, J_XOWN_C, J_XFWD_C):
            spread(kind, j).wait_recv()
        y_ref[:, :, pl.ds(pl.multiple_of(j * CHUNK, CHUNK), CHUNK)] = y_all[j].astype(BF16)

    @pl.loop(0, chunks + 7)
    def _(it):
        stage(it, 0, do_product)
        stage(it, 1, do_core_sum)
        stage(it, 3, do_y_sum)
        stage(it, 5, do_forward)
        stage(it, 6, do_diag)
        stage(it, 7, do_store)

    for cp in (cp_stat, cp_peer, cp_own, cp_xe, cp_xo, cp_rs, cp_ry, cp_ay, cp_ac, cp_af):
        cp.wait_send()

    @pl.loop(0, chunks)
    def _(j):
        rs_core(j).wait_send()
        rs_y(j).wait_send()
        for kind in (J_OWN_Y, J_OWN_X, J_OWN_C, J_FWD_X, J_FWD_C, J_XOWN_C, J_XFWD_C):
            spread(kind, j).wait_send()


def tail(o_part, lse, x_steps, w_o, w_fc, w_proj, b_o, gain, shift, b_fc, b_proj, group, kvs):
    steps, batch, cols = o_part.shape
    half = batch // 2
    rows = steps * half
    d_model = w_o.shape[1]
    chunks = d_model // CHUNK
    ff_own = w_fc.shape[1] // 2
    assert ff_own == d_model and steps == 4 and kvs == 2
    head_cols = group * LANES
    vm = pl.BlockSpec(memory_space=pltpu.VMEM)
    hbm = pl.BlockSpec(memory_space=pl.ANY)
    cfg = (steps, batch, group, chunks, kvs)
    scratch = [
        pltpu.VMEM((steps, half, head_cols), F32),
        pltpu.VMEM((steps, half, head_cols), F32),
        pltpu.VMEM((steps, batch, LANES), F32),
        pltpu.VMEM((steps, half, head_cols), F32),
        pltpu.VMEM((steps, half, LANES), F32),
        pltpu.VMEM((steps, half, head_cols), F32),
        pltpu.VMEM((steps, half, head_cols), F32),
        pltpu.VMEM((steps, half, LANES), F32),
        pltpu.VMEM((rows, head_cols), BF16),
        pltpu.VMEM((head_cols, d_model), BF16),
        pltpu.VMEM((rows, d_model), F32),
        pltpu.VMEM((2 * half, d_model), F32),
        pltpu.VMEM((2 * half, d_model), F32),
        pltpu.VMEM((half, d_model), F32),
        pltpu.VMEM((half, d_model), F32),
        pltpu.VMEM((half, d_model), F32),
        pltpu.VMEM((rows, d_model), F32),
        pltpu.VMEM((rows, d_model), BF16),
        pltpu.VMEM((RING, d_model, CHUNK), BF16),
        pltpu.VMEM((rows, ff_own), BF16),
        pltpu.VMEM((chunks, rows, CHUNK), F32),
        pltpu.VMEM((chunks, 2 * half, CHUNK), F32),
        pltpu.VMEM((chunks, 2 * half, CHUNK), F32),
        pltpu.VMEM((chunks, half, CHUNK), F32),
        pltpu.VMEM((chunks, steps, batch, CHUNK), F32),
        pltpu.SemaphoreType.DMA((10,)),
        pltpu.SemaphoreType.DMA((10,)),
        pltpu.SemaphoreType.DMA((9, chunks)),
        pltpu.SemaphoreType.DMA((9, chunks)),
        pltpu.SemaphoreType.DMA,
        pltpu.SemaphoreType.DMA,
        pltpu.SemaphoreType.DMA((RING,)),
    ]
    return pl.pallas_call(
        functools.partial(tail_kernel, cfg),
        out_shape=jax.ShapeDtypeStruct((steps, batch, d_model), BF16),
        in_specs=[vm, vm, hbm, hbm, hbm, hbm] + [vm] * 5,
        out_specs=vm,
        scratch_shapes=scratch,
        compiler_params=pltpu.CompilerParams(collective_id=0, has_side_effects=True, vmem_limit_bytes=VMEM_CAP),
        cost_estimate=pl.CostEstimate(flops=2 * rows * d_model * (head_cols + 2 * ff_own), bytes_accessed=100_000_000, transcendentals=0),
        name="tail",
    )(o_part, lse, x_steps, w_o, w_fc, w_proj, b_o, gain, shift, b_fc, b_proj)


def solution(mesh):
    sq_size = mesh.shape["sq"]
    act_spec = P(None, "dp", None)
    cache_spec = P("dp", "sq", "tp", None)
    col_spec = P(None, "tp")
    row_spec = P("tp", None)
    vec_spec = P("tp")
    rep_spec = P(None)
    in_specs = (act_spec, P("dp"), cache_spec, cache_spec, col_spec, vec_spec, col_spec, vec_spec,
                col_spec, vec_spec, row_spec, rep_spec, rep_spec, rep_spec, rep_spec, rep_spec,
                col_spec, vec_spec, row_spec, rep_spec)
    out_specs = (act_spec, cache_spec, cache_spec)

    def per_device(x_steps, positions, key_buf, val_buf, w_q, b_q, w_k, b_k, w_v, b_v, w_o, b_o,
                   ln1_gain, ln1_bias, ln2_gain, ln2_bias, w_fc, b_fc, w_proj, b_proj):
        steps, batch, d_model = x_steps.shape
        slots_local, kvs, dim = key_buf.shape[1], key_buf.shape[2], key_buf.shape[3]
        slots = slots_local * sq_size
        group = w_q.shape[1] // (kvs * dim)
        first_slot = lax.axis_index("sq") * slots_local
        meta = jnp.concatenate([first_slot[None].astype(jnp.int32), positions])
        x_wide = x_steps.astype(F32)
        hidden = layer_norm(x_wide, ln1_gain, ln1_bias).astype(BF16)
        query = linear(hidden, w_q, b_q).astype(BF16).astype(F32)
        key_new = linear(hidden, w_k, b_k).astype(BF16).astype(F32)
        val_new = linear(hidden, w_v, b_v).astype(BF16)
        cur_pos = positions[None, :] + jnp.arange(steps, dtype=jnp.int32)[:, None]
        cos_t, sin_t = rope_tables(cur_pos, dim)
        q_rot = apply_rope(query.reshape(steps, batch, kvs, group, dim), cos_t[:, :, None, None, :], sin_t[:, :, None, None, :]).astype(BF16)
        k_rot = apply_rope(key_new.reshape(steps, batch, kvs, dim), cos_t[:, :, None, :], sin_t[:, :, None, :]).astype(BF16)
        q_rows = q_rot.transpose(1, 3, 2, 0, 4).reshape(batch, group * kvs * steps, dim)
        pad = lambda rows: jnp.pad(rows.transpose(1, 0, 2, 3).reshape(batch, steps * kvs, dim), ((0, 0), (0, 16 - steps * kvs), (0, 0)))
        k_out, v_out, o_part, lse = attend(meta, q_rows, pad(k_rot), pad(val_new.reshape(steps, batch, kvs, dim)),
                                           key_buf.reshape(batch, slots_local * kvs, dim), val_buf.reshape(batch, slots_local * kvs, dim),
                                           steps, kvs, group, slots)
        row = lambda vec: vec.astype(F32).reshape(1, -1)
        ys = tail(o_part, lse, x_wide, w_o, w_fc, w_proj, row(b_o), row(ln2_gain), row(ln2_bias),
                  b_fc.astype(F32).reshape(-1, CHUNK), row(b_proj), group, kvs)
        return ys, k_out.reshape(key_buf.shape), v_out.reshape(val_buf.shape)

    return jax.shard_map(per_device, mesh=mesh, in_specs=in_specs, out_specs=out_specs, check_vma=False)
```

```python
import functools
import math

import jax
import jax.numpy as jnp
from jax import lax
from jax.experimental import pallas as pl
from jax.experimental.pallas import tpu as pltpu
from jax.sharding import PartitionSpec as P

ROPE_BASE = 1000000.0
LN_EPS = 1e-5
NEG_BIG = -1e30
NEG_HALF = -1e29
LOG2E = 1.4426950408889634
VMEM_CAP = 67_043_328
F32 = jnp.float32
BF16 = jnp.bfloat16
LANES = 128


def rope_tables(positions, head_dim):
    half_dim = head_dim // 2
    inv_freq = jnp.power(F32(ROPE_BASE), -2.0 * jnp.arange(half_dim, dtype=F32) / head_dim)
    angle = positions.astype(F32)[..., None] * inv_freq
    return jnp.cos(angle), jnp.sin(angle)


COLS = 256

def front_kernel(cfg, x_ref, gain_ref, shift_ref, cos_ref, sin_ref, bq_ref, bk_ref, bv_ref, wq_hbm, wk_hbm, wv_hbm,
                 q_out, kn_out, vn_out, hid, wq_buf, wk_buf, wv_buf, q_rows, kv_rows, bias_q, sem):
    steps, kvs, group = cfg
    batch, d_model = x_ref.shape[1], x_ref.shape[2]
    n_q = wq_hbm.shape[1] // COLS
    per_row = group * kvs * steps
    copies = [pltpu.make_async_copy(wk_hbm, wk_buf, sem.at[n_q]), pltpu.make_async_copy(wv_hbm, wv_buf, sem.at[n_q + 1])]
    for copy in copies:
        copy.start()
    for n in range(n_q):
        pltpu.make_async_copy(wq_hbm.at[:, n * COLS:(n + 1) * COLS], wq_buf.at[n], sem.at[n]).start()

    bias_q[...] = bq_ref[...].astype(F32)
    gain = gain_ref[...].astype(F32)
    shift = shift_ref[...].astype(F32)
    for s in range(steps):
        wide = x_ref[s].astype(F32)
        mean = jnp.mean(wide, axis=-1, keepdims=True)
        cent = wide - mean
        rstd = lax.rsqrt(jnp.mean(cent * cent, axis=-1, keepdims=True) + LN_EPS)
        for n in range(d_model // LANES):
            cols = slice(n * LANES, (n + 1) * LANES)
            hid[s * batch:(s + 1) * batch, cols] = (cent[:, cols] * rstd * gain[n:n + 1, :] + shift[n:n + 1, :]).astype(BF16)

    cos = cos_ref[...].reshape(steps * batch, LANES // 2)
    sin = sin_ref[...].reshape(steps * batch, LANES // 2)
    cos_full = jnp.concatenate([cos, cos], axis=-1)
    sin_full = jnp.concatenate([-sin, sin], axis=-1)

    def rotate(vec):
        return (vec * cos_full + pltpu.roll(vec, LANES // 2, 1) * sin_full).astype(BF16).astype(F32)

    def rounded(weight, bias):
        return (jnp.dot(hid[...], weight, preferred_element_type=F32) + bias).astype(BF16).astype(F32)

    for rope, copy, buf, b_ref, out in ((True, copies[0], wk_buf, bk_ref, kn_out), (False, copies[1], wv_buf, bv_ref, vn_out)):
        copy.wait()
        kv_rows[...] = jnp.zeros_like(kv_rows)
        bias = b_ref[...].astype(F32)
        both = rounded(buf[...], jnp.concatenate([bias[h:h + 1] for h in range(kvs)], axis=-1))
        for h in range(kvs):
            vec = both[:, h * LANES:(h + 1) * LANES]
            if rope:
                vec = rotate(vec)
            for s in range(steps):
                kv_rows[pl.ds(s * kvs + h, batch, stride=16), :] = vec[s * batch:(s + 1) * batch]
        out[...] = kv_rows[...].reshape(out.shape).astype(BF16)

    heads = COLS // LANES

    @pl.loop(0, n_q)
    def _(n):
        pltpu.make_async_copy(wq_hbm.at[:, 0:COLS], wq_buf.at[n], sem.at[n]).wait()
        bias = jnp.concatenate([bias_q[pl.ds(n * heads + e, 1), :] for e in range(heads)], axis=-1)
        both = rounded(wq_buf[n], bias)
        for e in range(heads):
            vec = rotate(both[:, e * LANES:(e + 1) * LANES])
            head = n * heads + e
            row = lax.rem(head, group) * (kvs * steps) + (head // group) * steps
            for s in range(steps):
                q_rows[pl.ds(row + s, batch, stride=per_row), :] = vec[s * batch:(s + 1) * batch]

    @pl.loop(0, batch)
    def _(b):
        q_out[b] = q_rows[pl.ds(pl.multiple_of(b * per_row, 8), per_row), :].astype(BF16)


def front(x_steps, gain, shift, cos_t, sin_t, b_q, b_k, b_v, w_q, w_k, w_v, kvs):
    steps, batch, d_model = x_steps.shape
    heads = w_q.shape[1] // LANES
    group = heads // kvs
    rows = group * kvs * steps
    n_q = w_q.shape[1] // COLS
    vm = pl.BlockSpec(memory_space=pltpu.VMEM)
    hbm = pl.BlockSpec(memory_space=pl.ANY)
    tiles = lambda vec: vec.reshape(-1, LANES)
    return pl.pallas_call(
        functools.partial(front_kernel, (steps, kvs, group)),
        out_shape=[
            jax.ShapeDtypeStruct((batch, rows, LANES), BF16),
            jax.ShapeDtypeStruct((batch, 16, LANES), BF16),
            jax.ShapeDtypeStruct((batch, 16, LANES), BF16),
        ],
        in_specs=[vm] * 8 + [hbm] * 3,
        out_specs=[vm] * 3,
        scratch_shapes=[
            pltpu.VMEM((steps * batch, d_model), BF16),
            pltpu.VMEM((n_q, d_model, COLS), BF16),
            pltpu.VMEM(w_k.shape, BF16),
            pltpu.VMEM(w_v.shape, BF16),
            pltpu.VMEM((batch * rows, LANES), F32),
            pltpu.VMEM((batch * 16, LANES), F32),
            pltpu.VMEM((heads, LANES), F32),
            pltpu.SemaphoreType.DMA((n_q + 2,)),
        ],
        compiler_params=pltpu.CompilerParams(vmem_limit_bytes=56 * 2**20),
        cost_estimate=pl.CostEstimate(flops=2 * steps * batch * d_model * (w_q.shape[1] + 2 * w_k.shape[1]),
                                      bytes_accessed=2 * d_model * (w_q.shape[1] + 2 * w_k.shape[1]), transcendentals=0),
        name="front",
    )(x_steps, tiles(gain), tiles(shift), cos_t, sin_t, tiles(b_q), tiles(b_k), tiles(b_v), w_q, w_k, w_v)


PER = 2
DEPTH = 8
AHEAD = 4

def attend_kernel(cfg, pos_ref, q_ref, kn_ref, vn_ref, k_hbm, v_hbm, ko_hbm, vo_hbm, o_ref, lse_ref,
                  k_buf, v_buf, o_rows, stat_rows, k_in, v_in, k_up, v_up):
    steps, kvs, group, slots, n_blocks = cfg
    rows = k_hbm.shape[1]
    tile = steps * kvs
    per_row = group * tile
    first = lax.axis_index("sq") * (rows // kvs)
    coef = LANES ** -0.5 * LOG2E
    contract_last = (((1,), (1,)), ((), ()))
    blocks_per_tile = 8 // PER

    def seqs(i):
        return pl.ds(i * PER, PER)

    def fetch(i):
        slot = lax.rem(i, DEPTH)
        return (pltpu.make_async_copy(k_hbm.at[seqs(i)], k_buf.at[slot], k_in.at[slot]),
                pltpu.make_async_copy(v_hbm.at[seqs(i)], v_buf.at[slot], v_in.at[slot]))

    def put(i):
        slot = lax.rem(i, DEPTH)
        return (pltpu.make_async_copy(k_buf.at[slot], ko_hbm.at[seqs(i)], k_up.at[slot]),
                pltpu.make_async_copy(v_buf.at[slot], vo_hbm.at[seqs(i)], v_up.at[slot]))

    for i in range(AHEAD):
        for copy in fetch(jnp.int32(i)):
            copy.start()

    sub = lax.broadcasted_iota(jnp.int32, (tile, rows), 0)
    lane = lax.broadcasted_iota(jnp.int32, (tile, rows), 1)
    sub2 = lax.broadcasted_iota(jnp.int32, (tile, 16), 0)
    lane2 = lax.broadcasted_iota(jnp.int32, (tile, 16), 1)
    new_step = lane2 // kvs
    new_ok = ((lane2 % kvs) == (sub2 // steps)) & (new_step <= sub2 % steps)
    stat_sub = lax.broadcasted_iota(jnp.int32, (tile, LANES), 0)
    stat_lane = lax.broadcasted_iota(jnp.int32, (tile, LANES), 1) - (stat_sub // steps) * group
    win_row = lax.broadcasted_iota(jnp.int32, (32, LANES), 0)

    def renew(i):
        slot_of = lax.rem(i, DEPTH)
        for one in range(PER):
            seq = i * PER + one
            goal = kvs * ((pos_ref[seq] & (slots - 1)) - first)
            goal = jnp.where(goal > kvs * (slots - steps), goal - kvs * slots, goal)
            start = pl.multiple_of(jnp.clip((goal >> 4) << 4, 0, rows - 32), 16)
            offset = win_row + (start - goal)
            for buf, new in ((k_buf, kn_ref), (v_buf, vn_ref)):
                fresh = new[seq].astype(F32)
                window = buf[slot_of, one, pl.ds(start, 32), :].astype(F32)
                for r in range(tile):
                    window = jnp.where(offset == r, fresh[r:r + 1, :], window)
                buf[slot_of, one, pl.ds(start, 32), :] = window.astype(BF16)

    @pl.loop(0, n_blocks)
    def _(i):
        slot_now = lax.rem(i, DEPTH)

        @pl.when(i >= 1)
        def _():
            renew(i - 1)

        @pl.when(i >= AHEAD)
        def _():
            for copy in put(i - AHEAD):
                copy.wait()

        @pl.when(i + AHEAD < n_blocks)
        def _():
            for copy in fetch(i + AHEAD):
                copy.start()

        @pl.when(i >= 1)
        def _():
            for copy in put(i - 1):
                copy.start()

        k_copy, v_copy = fetch(i)
        k_copy.wait()
        v_copy.wait()
        state = []
        for one in range(PER):
            seq = i * PER + one
            pos = pos_ref[seq]
            q = q_ref[seq]
            raw = lax.dot_general(q, k_buf[slot_now, one], contract_last, preferred_element_type=F32)
            raw2 = lax.dot_general(q, kn_ref[seq], contract_last, preferred_element_type=F32)
            state.append((seq, pos, raw, raw2))
        soft = []
        for seq, pos, raw, raw2 in state:
            slot = first + (lane >> 1)
            ahead = (slot - pos) & (slots - 1)
            ok = ((lane & 1) == (sub >> 2)) & (slot < pos) & (ahead > (sub & 3))
            bias = jnp.where(ok, 0.0, NEG_BIG).astype(F32)
            new_slot = ((pos + new_step) & (slots - 1)) - first
            here = (new_slot >= 0) & (new_slot < rows // kvs)
            bias2 = jnp.where(new_ok & here, 0.0, NEG_BIG).astype(F32)
            score = raw.reshape(group, tile, rows) * coef + bias[None]
            score2 = raw2.reshape(group, tile, 16) * coef + bias2[None]
            top = jnp.maximum(jnp.max(score, axis=-1, keepdims=True), jnp.max(score2, axis=-1, keepdims=True))
            top = jnp.maximum(top, NEG_HALF)
            w = jnp.exp2(score - top)
            w2 = jnp.exp2(score2 - top)
            total = jnp.sum(w, axis=-1, keepdims=True) + jnp.sum(w2, axis=-1, keepdims=True)
            soft.append((top, total, w.reshape(per_row, rows).astype(BF16), w2.reshape(per_row, 16).astype(BF16)))
        for one in range(PER):
            seq, pos = state[one][:2]
            top, total, w, w2 = soft[one]
            out = jnp.dot(w, v_buf[slot_now, one], preferred_element_type=F32)
            out = out + jnp.dot(w2, vn_ref[seq], preferred_element_type=F32)
            some = total > 0.0
            safe = jnp.where(some, total, 1.0)
            lse = jnp.where(some, top + jnp.log2(safe), NEG_BIG)
            out = out.reshape(group, tile, LANES) * (1.0 / safe)
            stats = jnp.zeros((tile, LANES), F32)
            for n in range(group):
                stats = jnp.where(stat_lane == n, lse[n], stats)
            seat = lax.rem(i, blocks_per_tile) * PER + one
            o_rows[pl.ds(pl.multiple_of(seat * per_row, 8), per_row), :] = out.reshape(per_row, LANES)
            stat_rows[pl.ds(pl.multiple_of(seat * tile, 8), tile), :] = stats
        @pl.when(lax.rem(i, blocks_per_tile) == blocks_per_tile - 1)
        def _():
            where = pl.ds(pl.multiple_of((i // blocks_per_tile) * 8, 8), 8)
            for s in range(steps):
                lse_ref[s, where, :] = sum(stat_rows[pl.ds(h * steps + s, 8, stride=tile), :] for h in range(kvs))
                for h in range(kvs):
                    for n in range(group):
                        col = (h * group + n) * LANES
                        o_ref[s, where, col:col + LANES] = o_rows[pl.ds(n * tile + h * steps + s, 8, stride=per_row), :]

    renew(jnp.int32(n_blocks - 1))
    for copy in put(n_blocks - 1):
        copy.start()
    for j in range(AHEAD):
        for copy in put(n_blocks - AHEAD + j):
            copy.wait()


def attend(positions, q, k_new, v_new, k_rows, v_rows, steps, kvs, group, slots):
    batch, rows, dim = k_rows.shape
    vm = pl.BlockSpec(memory_space=pltpu.VMEM)
    hbm = pl.BlockSpec(memory_space=pl.ANY)
    return pl.pallas_call(
        functools.partial(attend_kernel, (steps, kvs, group, slots, batch // PER)),
        in_specs=[pl.BlockSpec(memory_space=pltpu.SMEM), vm, vm, vm, hbm, hbm],
        out_specs=[hbm, hbm, vm, vm],
        out_shape=[
            jax.ShapeDtypeStruct(k_rows.shape, BF16),
            jax.ShapeDtypeStruct(v_rows.shape, BF16),
            jax.ShapeDtypeStruct((steps, batch, kvs * group * dim), F32),
            jax.ShapeDtypeStruct((steps, batch, LANES), F32),
        ],
        scratch_shapes=[
            pltpu.VMEM((DEPTH, PER, rows, dim), BF16),
            pltpu.VMEM((DEPTH, PER, rows, dim), BF16),
            pltpu.VMEM((8 * q.shape[1], dim), F32),
            pltpu.VMEM((8 * steps * kvs, dim), F32),
            pltpu.SemaphoreType.DMA((DEPTH,)),
            pltpu.SemaphoreType.DMA((DEPTH,)),
            pltpu.SemaphoreType.DMA((DEPTH,)),
            pltpu.SemaphoreType.DMA((DEPTH,)),
        ],
        compiler_params=pltpu.CompilerParams(vmem_limit_bytes=56 * 2**20),
        cost_estimate=pl.CostEstimate(flops=4 * batch * rows * q.shape[1] * dim, bytes_accessed=8 * batch * rows * dim,
                                      transcendentals=batch * rows * q.shape[1]),
        name="attend",
    )(positions, q, k_new, v_new, k_rows, v_rows)


CHUNK = 512
RING = 6
(C_PEER_O, C_STAT, C_OWN_O, C_X_O, C_X_E, C_RS_CORE, C_RS_Y, C_AG_Y, C_AG_OWN, C_AG_FWD) = range(10)
(J_RS_CORE, J_RS_Y, J_OWN_Y, J_OWN_X, J_OWN_C, J_FWD_X, J_FWD_C, J_XOWN_C, J_XFWD_C) = range(9)


def tail_kernel(cfg, o_ref, lse_ref, x_ref, wo_hbm, wfc_hbm, wproj_hbm, bo_ref, gain_ref, shift_ref, bfc_ref, bproj_ref,
                y_ref,
                in_o_peer, in_o_own, in_lse, to_x, to_x_e, mine, in_x, in_x_e, a_buf,
                wo_buf, part, in_part, half_sum, in_y, x_buf, x_mid, hid, hid_b,
                ring, g_buf, p_chunk, in_rc, p_half, in_ry, y_all,
                send_a, recv_a, send_j, recv_j, wo_sem, x_sem, ring_sem):
    steps, batch, group, chunks, kvs = cfg
    half = batch // 2
    quarter = half
    d_model = wo_hbm.shape[1]
    head_cols = group * LANES
    ff_own = wfc_hbm.shape[1] // 2
    y = lax.axis_index("tp")
    sq = lax.axis_index("sq")
    x, c = sq // 2, sq % 2
    sib = {"sq": x * 2 + 1 - c}
    xpeer = {"sq": (1 - x) * 2 + c}
    ypeer = {"tp": 1 - y}
    MESH = pl.DeviceIdType.MESH
    my_step = 2 * c + y

    def load_item(item, slot):
        @pl.when(item < chunks)
        def _():
            col = pl.multiple_of(c * ff_own + item * CHUNK, CHUNK)
            pltpu.make_async_copy(wfc_hbm.at[:, pl.ds(col, CHUNK)], ring.at[slot], ring_sem.at[slot]).start()

        @pl.when(item >= chunks)
        def _():
            col = pl.multiple_of((item - chunks) * CHUNK, CHUNK)
            row = pl.multiple_of(c * ff_own, CHUNK)
            pltpu.make_async_copy(wproj_hbm.at[pl.ds(row, ff_own), pl.ds(col, CHUNK)], ring.at[slot], ring_sem.at[slot]).start()

    def wait_item(slot):
        pltpu.make_async_copy(wfc_hbm.at[:, pl.ds(0, CHUNK)], ring.at[slot], ring_sem.at[slot]).wait()

    wo_copy = pltpu.make_async_copy(wo_hbm.at[pl.ds(pl.multiple_of(c * head_cols, LANES), head_cols), :], wo_buf, wo_sem)
    wo_copy.start()
    x_copy = pltpu.make_async_copy(x_ref.at[my_step, pl.ds(pl.multiple_of(x * half, 8), half), :], x_buf, x_sem)
    x_copy.start()
    for k in range(RING):
        load_item(jnp.int32(k), k)

    barrier = pltpu.get_barrier_semaphore()
    for who in (sib, xpeer, ypeer):
        pl.semaphore_signal(barrier, inc=1, device_id=who, device_id_type=MESH)
    pl.semaphore_wait(barrier, 3)

    def remote(src, dst, kind, who):
        return pltpu.make_async_remote_copy(src_ref=src, dst_ref=dst, send_sem=send_a.at[kind], recv_sem=recv_a.at[kind],
                                            device_id=who, device_id_type=MESH)

    peer_rows = pl.ds(pl.multiple_of((1 - x) * half, 8), half)
    own_rows = pl.ds(pl.multiple_of(x * half, 8), half)
    sib_cols = pl.ds(pl.multiple_of((1 - c) * head_cols, LANES), head_cols)
    cp_stat = remote(lse_ref, in_lse, C_STAT, sib)
    cp_peer = remote(o_ref.at[:, peer_rows, sib_cols], in_o_peer, C_PEER_O, sib)
    cp_own = remote(o_ref.at[:, own_rows, sib_cols], in_o_own, C_OWN_O, sib)
    cp_stat.start()
    cp_peer.start()
    cp_own.start()

    def my_lanes(stat):
        return jnp.where(c == 0, stat, pltpu.roll(stat, LANES - group, 1))

    def weights_of(e1, e2):
        top = jnp.maximum(e1, e2)
        w1 = jnp.exp2(e1 - top)
        w2 = jnp.exp2(e2 - top)
        tot = w1 + w2
        inv = 1.0 / tot
        return w1 * inv, w2 * inv, top + jnp.log2(tot)

    def merge_core(rows, incoming, out, keep_e):
        for s in range(steps):
            w1, w2, e = weights_of(my_lanes(lse_ref[s, rows, :]), my_lanes(in_lse[s, rows, :]))
            keep_e[s] = e
            for i in range(group):
                col = pl.ds(pl.multiple_of(c * head_cols + i * LANES, LANES), LANES)
                out[s, :, i * LANES:(i + 1) * LANES] = (w1[:, i:i + 1] * o_ref[s, rows, col]
                                                        + w2[:, i:i + 1] * incoming[s, :, i * LANES:(i + 1) * LANES])

    mine_e = hid.at[pl.ds(0, steps * half), pl.ds(0, LANES)]
    cp_stat.wait_recv()
    cp_peer.wait_recv()
    merge_core(peer_rows, in_o_peer, to_x, to_x_e)
    cp_xe = remote(to_x_e, in_x_e, C_X_E, xpeer)
    cp_xo = remote(to_x, in_x, C_X_O, xpeer)
    cp_xe.start()
    cp_xo.start()
    cp_own.wait_recv()
    for s in range(steps):
        w1, w2, e = weights_of(my_lanes(lse_ref[s, own_rows, :]), my_lanes(in_lse[s, own_rows, :]))
        mine_e[s * half:(s + 1) * half, :] = e
        for i in range(group):
            col = pl.ds(pl.multiple_of(c * head_cols + i * LANES, LANES), LANES)
            mine[s, :, i * LANES:(i + 1) * LANES] = (w1[:, i:i + 1] * o_ref[s, own_rows, col]
                                                     + w2[:, i:i + 1] * in_o_own[s, :, i * LANES:(i + 1) * LANES])
    x_copy.wait()
    cp_xe.wait_recv()
    cp_xo.wait_recv()
    w1, w2, _ = weights_of(mine_e[...], in_x_e[...].reshape(steps * half, LANES))
    for i in range(group):
        cols = slice(i * LANES, (i + 1) * LANES)
        a_buf[:, cols] = (w1[:, i:i + 1] * mine[:, :, cols].reshape(steps * half, LANES)
                          + w2[:, i:i + 1] * in_x[:, :, cols].reshape(steps * half, LANES)).astype(BF16)

    wo_copy.wait()

    @pl.loop(0, chunks)
    def _(j):
        cols = pl.ds(pl.multiple_of(j * CHUNK, CHUNK), CHUNK)
        part[:, cols] = jnp.dot(a_buf[...], wo_buf[:, cols], preferred_element_type=F32)

    def step_rows(s, n=1):
        return pl.ds(pl.multiple_of(s * half, 8), n * half)

    cp_rs = remote(part.at[step_rows(2 * (1 - c), 2), :], in_part, C_RS_CORE, sib)
    cp_rs.start()
    cp_rs.wait_recv()
    half_sum[...] = part[step_rows(2 * c, 2), :] + in_part[...]
    cp_ry = remote(half_sum.at[step_rows(1 - y), :], in_y, C_RS_Y, ypeer)
    cp_ry.start()
    cp_ry.wait_recv()
    x_new = (x_buf[...] + (half_sum[step_rows(y), :] + in_y[...]) + bo_ref[...]).astype(BF16).astype(F32)
    x_mid[...] = x_new
    mean = jnp.mean(x_new, axis=-1, keepdims=True)
    cent = x_new - mean
    var = jnp.mean(cent * cent, axis=-1, keepdims=True)
    normed = cent * lax.rsqrt(var + LN_EPS) * gain_ref[...] + shift_ref[...]
    hid[step_rows(my_step), :] = normed.astype(BF16).astype(F32)

    own_h = hid.at[step_rows(my_step), :]
    peer_h = hid.at[step_rows(2 * c + 1 - y), :]
    cp_ay = remote(own_h, own_h, C_AG_Y, ypeer)
    cp_ac = remote(own_h, own_h, C_AG_OWN, sib)
    cp_ay.start()
    cp_ac.start()
    cp_ay.wait_recv()
    cp_af = remote(peer_h, peer_h, C_AG_FWD, sib)
    cp_af.start()
    cp_ac.wait_recv()
    cp_af.wait_recv()
    hid_b[...] = hid[...].astype(BF16)

    @pl.loop(0, chunks)
    def _(j):
        slot = lax.rem(j, RING)
        wait_item(slot)
        pre = jnp.dot(hid_b[...], ring[slot], preferred_element_type=F32) + bfc_ref[pl.ds(c * chunks + j, 1), :]
        cube = pre * pre * pre
        act = 0.5 * pre * (1.0 + jnp.tanh(math.sqrt(2.0 / math.pi) * (pre + 0.044715 * cube)))
        g_buf[:, pl.ds(pl.multiple_of(j * CHUNK, CHUNK), CHUNK)] = act.astype(BF16)
        load_item(j + RING, slot)

    def jcopy(src, dst, kind, j, who):
        return pltpu.make_async_remote_copy(src_ref=src, dst_ref=dst, send_sem=send_j.at[kind, j], recv_sem=recv_j.at[kind, j],
                                            device_id=who, device_id_type=MESH)

    def rs_core(j):
        return jcopy(p_chunk.at[j, step_rows(2 * (1 - c), 2), :], in_rc.at[j], J_RS_CORE, j, sib)

    def rs_y(j):
        return jcopy(p_half.at[j, step_rows(1 - y), :], in_ry.at[j], J_RS_Y, j, ypeer)

    def block(j, s, xx):
        return y_all.at[j, s, pl.ds(pl.multiple_of(xx * half, 8), half), :]

    def spread(kind, j):
        own = block(j, my_step, x)
        ypart = block(j, 2 * c + 1 - y, x)
        xpart = block(j, my_step, 1 - x)
        diag = block(j, 2 * c + 1 - y, 1 - x)
        ref, who = {J_OWN_Y: (own, ypeer), J_OWN_X: (own, xpeer), J_OWN_C: (own, sib),
                    J_FWD_X: (ypart, xpeer), J_FWD_C: (ypart, sib),
                    J_XOWN_C: (xpart, sib), J_XFWD_C: (diag, sib)}[kind]
        return jcopy(ref, ref, kind, j, who)

    def stage(it, lag, body):
        j = it - lag

        @pl.when((j >= 0) & (j < chunks))
        def _():
            body(j)

    def do_product(j):
        item = chunks + j
        slot = lax.rem(item, RING)
        wait_item(slot)
        p_chunk[j] = jnp.dot(g_buf[...], ring[slot], preferred_element_type=F32)

        @pl.when(item + RING < 2 * chunks)
        def _():
            load_item(item + RING, slot)

        rs_core(j).start()

    def do_core_sum(j):
        rs_core(j).wait_recv()
        p_half[j] = p_chunk[j, step_rows(2 * c, 2), :] + in_rc[j]
        rs_y(j).start()

    def do_y_sum(j):
        rs_y(j).wait_recv()
        cols = pl.ds(pl.multiple_of(j * CHUNK, CHUNK), CHUNK)
        full = x_mid[:, cols] + (p_half[j, step_rows(y), :] + in_ry[j]) + bproj_ref[:, cols]
        y_all[j, my_step, pl.ds(pl.multiple_of(x * half, 8), half), :] = full.astype(BF16).astype(F32)
        for kind in (J_OWN_Y, J_OWN_X, J_OWN_C):
            spread(kind, j).start()

    def do_forward(j):
        spread(J_OWN_Y, j).wait_recv()
        spread(J_FWD_X, j).start()
        spread(J_FWD_C, j).start()
        spread(J_OWN_X, j).wait_recv()
        spread(J_XOWN_C, j).start()

    def do_diag(j):
        spread(J_FWD_X, j).wait_recv()
        spread(J_XFWD_C, j).start()

    def do_store(j):
        for kind in (J_OWN_C, J_FWD_C, J_XOWN_C, J_XFWD_C):
            spread(kind, j).wait_recv()
        y_ref[:, :, pl.ds(pl.multiple_of(j * CHUNK, CHUNK), CHUNK)] = y_all[j].astype(BF16)

    @pl.loop(0, chunks + 7)
    def _(it):
        stage(it, 0, do_product)
        stage(it, 1, do_core_sum)
        stage(it, 3, do_y_sum)
        stage(it, 5, do_forward)
        stage(it, 6, do_diag)
        stage(it, 7, do_store)

    for cp in (cp_stat, cp_peer, cp_own, cp_xe, cp_xo, cp_rs, cp_ry, cp_ay, cp_ac, cp_af):
        cp.wait_send()

    @pl.loop(0, chunks)
    def _(j):
        rs_core(j).wait_send()
        rs_y(j).wait_send()
        for kind in (J_OWN_Y, J_OWN_X, J_OWN_C, J_FWD_X, J_FWD_C, J_XOWN_C, J_XFWD_C):
            spread(kind, j).wait_send()


def tail(o_part, lse, x_steps, w_o, w_fc, w_proj, b_o, gain, shift, b_fc, b_proj, group, kvs):
    steps, batch, cols = o_part.shape
    half = batch // 2
    rows = steps * half
    d_model = w_o.shape[1]
    chunks = d_model // CHUNK
    ff_own = w_fc.shape[1] // 2
    assert ff_own == d_model and steps == 4 and kvs == 2
    head_cols = group * LANES
    vm = pl.BlockSpec(memory_space=pltpu.VMEM)
    hbm = pl.BlockSpec(memory_space=pl.ANY)
    cfg = (steps, batch, group, chunks, kvs)
    scratch = [
        pltpu.VMEM((steps, half, head_cols), F32),
        pltpu.VMEM((steps, half, head_cols), F32),
        pltpu.VMEM((steps, batch, LANES), F32),
        pltpu.VMEM((steps, half, head_cols), F32),
        pltpu.VMEM((steps, half, LANES), F32),
        pltpu.VMEM((steps, half, head_cols), F32),
        pltpu.VMEM((steps, half, head_cols), F32),
        pltpu.VMEM((steps, half, LANES), F32),
        pltpu.VMEM((rows, head_cols), BF16),
        pltpu.VMEM((head_cols, d_model), BF16),
        pltpu.VMEM((rows, d_model), F32),
        pltpu.VMEM((2 * half, d_model), F32),
        pltpu.VMEM((2 * half, d_model), F32),
        pltpu.VMEM((half, d_model), F32),
        pltpu.VMEM((half, d_model), F32),
        pltpu.VMEM((half, d_model), F32),
        pltpu.VMEM((rows, d_model), F32),
        pltpu.VMEM((rows, d_model), BF16),
        pltpu.VMEM((RING, d_model, CHUNK), BF16),
        pltpu.VMEM((rows, ff_own), BF16),
        pltpu.VMEM((chunks, rows, CHUNK), F32),
        pltpu.VMEM((chunks, 2 * half, CHUNK), F32),
        pltpu.VMEM((chunks, 2 * half, CHUNK), F32),
        pltpu.VMEM((chunks, half, CHUNK), F32),
        pltpu.VMEM((chunks, steps, batch, CHUNK), F32),
        pltpu.SemaphoreType.DMA((10,)),
        pltpu.SemaphoreType.DMA((10,)),
        pltpu.SemaphoreType.DMA((9, chunks)),
        pltpu.SemaphoreType.DMA((9, chunks)),
        pltpu.SemaphoreType.DMA,
        pltpu.SemaphoreType.DMA,
        pltpu.SemaphoreType.DMA((RING,)),
    ]
    return pl.pallas_call(
        functools.partial(tail_kernel, cfg),
        out_shape=jax.ShapeDtypeStruct((steps, batch, d_model), BF16),
        in_specs=[vm, vm, hbm, hbm, hbm, hbm] + [vm] * 5,
        out_specs=vm,
        scratch_shapes=scratch,
        compiler_params=pltpu.CompilerParams(collective_id=0, has_side_effects=True, vmem_limit_bytes=VMEM_CAP),
        cost_estimate=pl.CostEstimate(flops=2 * rows * d_model * (head_cols + 2 * ff_own), bytes_accessed=100_000_000, transcendentals=0),
        name="tail",
    )(o_part, lse, x_steps, w_o, w_fc, w_proj, b_o, gain, shift, b_fc, b_proj)


def solution(mesh):
    sq_size = mesh.shape["sq"]
    act_spec = P(None, "dp", None)
    cache_spec = P("dp", "sq", "tp", None)
    col_spec = P(None, "tp")
    row_spec = P("tp", None)
    vec_spec = P("tp")
    rep_spec = P(None)
    in_specs = (act_spec, P("dp"), cache_spec, cache_spec, col_spec, vec_spec, col_spec, vec_spec,
                col_spec, vec_spec, row_spec, rep_spec, rep_spec, rep_spec, rep_spec, rep_spec,
                col_spec, vec_spec, row_spec, rep_spec)
    out_specs = (act_spec, cache_spec, cache_spec)

    def per_device(x_steps, positions, key_buf, val_buf, w_q, b_q, w_k, b_k, w_v, b_v, w_o, b_o,
                   ln1_gain, ln1_bias, ln2_gain, ln2_bias, w_fc, b_fc, w_proj, b_proj):
        steps, batch, d_model = x_steps.shape
        slots_local, kvs, dim = key_buf.shape[1], key_buf.shape[2], key_buf.shape[3]
        slots = slots_local * sq_size
        group = w_q.shape[1] // (kvs * dim)
        cur_pos = positions[None, :] + jnp.arange(steps, dtype=jnp.int32)[:, None]
        cos_t, sin_t = rope_tables(cur_pos, dim)
        q_rows, k_new, v_new = front(x_steps, ln1_gain, ln1_bias, cos_t, sin_t, b_q, b_k, b_v, w_q, w_k, w_v, kvs)
        k_out, v_out, o_part, lse = attend(positions, q_rows, k_new, v_new, key_buf.reshape(batch, slots_local * kvs, dim),
                                           val_buf.reshape(batch, slots_local * kvs, dim), steps, kvs, group, slots)
        row = lambda vec: vec.astype(F32).reshape(1, -1)
        ys = tail(o_part, lse, x_steps.astype(F32), w_o, w_fc, w_proj, row(b_o), row(ln2_gain), row(ln2_bias),
                  b_fc.astype(F32).reshape(-1, CHUNK), row(b_proj), group, kvs)
        return ys, k_out.reshape(key_buf.shape), v_out.reshape(val_buf.shape)

    return jax.shard_map(per_device, mesh=mesh, in_specs=in_specs, out_specs=out_specs, check_vma=False)
```

```python
import functools
import math

import jax
import jax.numpy as jnp
from jax import lax
from jax.experimental import pallas as pl
from jax.experimental.pallas import tpu as pltpu
from jax.sharding import PartitionSpec as P

ROPE_BASE = 1000000.0
LN_EPS = 1e-5
NEG_BIG = -1e30
NEG_HALF = -1e29
LOG2E = 1.4426950408889634
VMEM_CAP = 67_043_328
F32 = jnp.float32
BF16 = jnp.bfloat16
LANES = 128


def rope_tables(positions, head_dim):
    half_dim = head_dim // 2
    inv_freq = jnp.power(F32(ROPE_BASE), -2.0 * jnp.arange(half_dim, dtype=F32) / head_dim)
    angle = positions.astype(F32)[..., None] * inv_freq
    return jnp.cos(angle), jnp.sin(angle)


COLS = 256

def front_kernel(cfg, x_ref, gain_ref, shift_ref, cos_ref, sin_ref, bq_ref, bk_ref, bv_ref, wq_hbm, wk_hbm, wv_hbm,
                 q_out, kn_out, vn_out, hid, wq_buf, wk_buf, wv_buf, q_rows, kv_rows, bias_q, sem):
    steps, kvs, group = cfg
    batch, d_model = x_ref.shape[1], x_ref.shape[2]
    n_q = wq_hbm.shape[1] // COLS
    per_row = group * kvs * steps
    copies = [pltpu.make_async_copy(wk_hbm, wk_buf, sem.at[n_q]), pltpu.make_async_copy(wv_hbm, wv_buf, sem.at[n_q + 1])]
    for copy in copies:
        copy.start()
    for n in range(n_q):
        pltpu.make_async_copy(wq_hbm.at[:, n * COLS:(n + 1) * COLS], wq_buf.at[n], sem.at[n]).start()

    bias_q[...] = bq_ref[...].astype(F32)
    gain = gain_ref[...].astype(F32)
    shift = shift_ref[...].astype(F32)
    for s in range(steps):
        wide = x_ref[s].astype(F32)
        mean = jnp.mean(wide, axis=-1, keepdims=True)
        cent = wide - mean
        rstd = lax.rsqrt(jnp.mean(cent * cent, axis=-1, keepdims=True) + LN_EPS)
        for n in range(d_model // LANES):
            cols = slice(n * LANES, (n + 1) * LANES)
            hid[s * batch:(s + 1) * batch, cols] = (cent[:, cols] * rstd * gain[n:n + 1, :] + shift[n:n + 1, :]).astype(BF16)

    cos = cos_ref[...].reshape(steps * batch, LANES // 2)
    sin = sin_ref[...].reshape(steps * batch, LANES // 2)
    cos_full = jnp.concatenate([cos, cos], axis=-1)
    sin_full = jnp.concatenate([-sin, sin], axis=-1)

    def rotate(vec):
        return (vec * cos_full + pltpu.roll(vec, LANES // 2, 1) * sin_full).astype(BF16).astype(F32)

    def rounded(weight, bias):
        return (jnp.dot(hid[...], weight, preferred_element_type=F32) + bias).astype(BF16).astype(F32)

    for rope, copy, buf, b_ref, out in ((True, copies[0], wk_buf, bk_ref, kn_out), (False, copies[1], wv_buf, bv_ref, vn_out)):
        copy.wait()
        kv_rows[...] = jnp.zeros_like(kv_rows)
        bias = b_ref[...].astype(F32)
        both = rounded(buf[...], jnp.concatenate([bias[h:h + 1] for h in range(kvs)], axis=-1))
        for h in range(kvs):
            vec = both[:, h * LANES:(h + 1) * LANES]
            if rope:
                vec = rotate(vec)
            for s in range(steps):
                kv_rows[pl.ds(s * kvs + h, batch, stride=16), :] = vec[s * batch:(s + 1) * batch]
        out[...] = kv_rows[...].reshape(out.shape).astype(BF16)

    heads = COLS // LANES

    @pl.loop(0, n_q)
    def _(n):
        pltpu.make_async_copy(wq_hbm.at[:, 0:COLS], wq_buf.at[n], sem.at[n]).wait()
        bias = jnp.concatenate([bias_q[pl.ds(n * heads + e, 1), :] for e in range(heads)], axis=-1)
        both = rounded(wq_buf[n], bias)
        for e in range(heads):
            vec = rotate(both[:, e * LANES:(e + 1) * LANES])
            head = n * heads + e
            row = lax.rem(head, group) * (kvs * steps) + (head // group) * steps
            for s in range(steps):
                q_rows[pl.ds(row + s, batch, stride=per_row), :] = vec[s * batch:(s + 1) * batch]

    @pl.loop(0, batch)
    def _(b):
        q_out[b] = q_rows[pl.ds(pl.multiple_of(b * per_row, 8), per_row), :].astype(BF16)


def front(x_steps, gain, shift, cos_t, sin_t, b_q, b_k, b_v, w_q, w_k, w_v, kvs):
    steps, batch, d_model = x_steps.shape
    heads = w_q.shape[1] // LANES
    group = heads // kvs
    rows = group * kvs * steps
    n_q = w_q.shape[1] // COLS
    vm = pl.BlockSpec(memory_space=pltpu.VMEM)
    hbm = pl.BlockSpec(memory_space=pl.ANY)
    tiles = lambda vec: vec.reshape(-1, LANES)
    return pl.pallas_call(
        functools.partial(front_kernel, (steps, kvs, group)),
        out_shape=[
            jax.ShapeDtypeStruct((batch, rows, LANES), BF16),
            jax.ShapeDtypeStruct((batch, 16, LANES), BF16),
            jax.ShapeDtypeStruct((batch, 16, LANES), BF16),
        ],
        in_specs=[vm] * 8 + [hbm] * 3,
        out_specs=[vm] * 3,
        scratch_shapes=[
            pltpu.VMEM((steps * batch, d_model), BF16),
            pltpu.VMEM((n_q, d_model, COLS), BF16),
            pltpu.VMEM(w_k.shape, BF16),
            pltpu.VMEM(w_v.shape, BF16),
            pltpu.VMEM((batch * rows, LANES), F32),
            pltpu.VMEM((batch * 16, LANES), F32),
            pltpu.VMEM((heads, LANES), F32),
            pltpu.SemaphoreType.DMA((n_q + 2,)),
        ],
        compiler_params=pltpu.CompilerParams(vmem_limit_bytes=56 * 2**20),
        cost_estimate=pl.CostEstimate(flops=2 * steps * batch * d_model * (w_q.shape[1] + 2 * w_k.shape[1]),
                                      bytes_accessed=2 * d_model * (w_q.shape[1] + 2 * w_k.shape[1]), transcendentals=0),
        name="front",
    )(x_steps, tiles(gain), tiles(shift), cos_t, sin_t, tiles(b_q), tiles(b_k), tiles(b_v), w_q, w_k, w_v)


PER = 2
DEPTH = 8
AHEAD = 4

def attend_kernel(cfg, pos_ref, q_ref, kn_ref, vn_ref, k_hbm, v_hbm, *refs):
    steps, kvs, group, slots, n_blocks, own_half = cfg
    ko_hbm, vo_hbm, o_ref, k_buf, v_buf, o_rows, stat_rows, k_in, v_in, k_up, v_up = refs[2 if own_half else 0:]
    x = lax.axis_index("sq") // 2
    base = (x if own_half else 1 - x) * (n_blocks * PER)
    lse_cols = slice(kvs * group * LANES, (kvs * group + 1) * LANES)
    rows = k_hbm.shape[1]
    tile = steps * kvs
    per_row = group * tile
    first = lax.axis_index("sq") * (rows // kvs)
    coef = LANES ** -0.5 * LOG2E
    contract_last = (((1,), (1,)), ((), ()))
    blocks_per_tile = 8 // PER

    def seqs(i):
        return pl.ds(base + i * PER, PER)

    def fetch(i):
        slot = lax.rem(i, DEPTH)
        return (pltpu.make_async_copy(k_hbm.at[seqs(i)], k_buf.at[slot], k_in.at[slot]),
                pltpu.make_async_copy(v_hbm.at[seqs(i)], v_buf.at[slot], v_in.at[slot]))

    def put(i):
        slot = lax.rem(i, DEPTH)
        return (pltpu.make_async_copy(k_buf.at[slot], ko_hbm.at[seqs(i)], k_up.at[slot]),
                pltpu.make_async_copy(v_buf.at[slot], vo_hbm.at[seqs(i)], v_up.at[slot]))

    for i in range(AHEAD):
        for copy in fetch(jnp.int32(i)):
            copy.start()

    sub = lax.broadcasted_iota(jnp.int32, (tile, rows), 0)
    lane = lax.broadcasted_iota(jnp.int32, (tile, rows), 1)
    sub2 = lax.broadcasted_iota(jnp.int32, (tile, 16), 0)
    lane2 = lax.broadcasted_iota(jnp.int32, (tile, 16), 1)
    new_step = lane2 // kvs
    new_ok = ((lane2 % kvs) == (sub2 // steps)) & (new_step <= sub2 % steps)
    stat_sub = lax.broadcasted_iota(jnp.int32, (tile, LANES), 0)
    stat_lane = lax.broadcasted_iota(jnp.int32, (tile, LANES), 1) - (stat_sub // steps) * group
    win_row = lax.broadcasted_iota(jnp.int32, (32, LANES), 0)

    def renew(i):
        slot_of = lax.rem(i, DEPTH)
        for one in range(PER):
            seq = base + i * PER + one
            goal = kvs * ((pos_ref[seq] & (slots - 1)) - first)
            goal = jnp.where(goal > kvs * (slots - steps), goal - kvs * slots, goal)
            start = pl.multiple_of(jnp.clip((goal >> 4) << 4, 0, rows - 32), 16)
            offset = win_row + (start - goal)
            for buf, new in ((k_buf, kn_ref), (v_buf, vn_ref)):
                fresh = new[seq].astype(F32)
                window = buf[slot_of, one, pl.ds(start, 32), :].astype(F32)
                for r in range(tile):
                    window = jnp.where(offset == r, fresh[r:r + 1, :], window)
                buf[slot_of, one, pl.ds(start, 32), :] = window.astype(BF16)

    @pl.loop(0, n_blocks)
    def _(i):
        slot_now = lax.rem(i, DEPTH)

        @pl.when(i >= 1)
        def _():
            renew(i - 1)

        @pl.when(i >= AHEAD)
        def _():
            for copy in put(i - AHEAD):
                copy.wait()

        @pl.when(i + AHEAD < n_blocks)
        def _():
            for copy in fetch(i + AHEAD):
                copy.start()

        @pl.when(i >= 1)
        def _():
            for copy in put(i - 1):
                copy.start()

        k_copy, v_copy = fetch(i)
        k_copy.wait()
        v_copy.wait()
        state = []
        for one in range(PER):
            seq = base + i * PER + one
            pos = pos_ref[seq]
            q = q_ref[seq]
            raw = lax.dot_general(q, k_buf[slot_now, one], contract_last, preferred_element_type=F32)
            raw2 = lax.dot_general(q, kn_ref[seq], contract_last, preferred_element_type=F32)
            state.append((seq, pos, raw, raw2))
        soft = []
        for seq, pos, raw, raw2 in state:
            slot = first + (lane >> 1)
            ahead = (slot - pos) & (slots - 1)
            ok = ((lane & 1) == (sub >> 2)) & (slot < pos) & (ahead > (sub & 3))
            bias = jnp.where(ok, 0.0, NEG_BIG).astype(F32)
            new_slot = ((pos + new_step) & (slots - 1)) - first
            here = (new_slot >= 0) & (new_slot < rows // kvs)
            bias2 = jnp.where(new_ok & here, 0.0, NEG_BIG).astype(F32)
            score = raw.reshape(group, tile, rows) * coef + bias[None]
            score2 = raw2.reshape(group, tile, 16) * coef + bias2[None]
            top = jnp.maximum(jnp.max(score, axis=-1, keepdims=True), jnp.max(score2, axis=-1, keepdims=True))
            top = jnp.maximum(top, NEG_HALF)
            w = jnp.exp2(score - top)
            w2 = jnp.exp2(score2 - top)
            total = jnp.sum(w, axis=-1, keepdims=True) + jnp.sum(w2, axis=-1, keepdims=True)
            soft.append((top, total, w.reshape(per_row, rows).astype(BF16), w2.reshape(per_row, 16).astype(BF16)))
        for one in range(PER):
            seq, pos = state[one][:2]
            top, total, w, w2 = soft[one]
            out = jnp.dot(w, v_buf[slot_now, one], preferred_element_type=F32)
            out = out + jnp.dot(w2, vn_ref[seq], preferred_element_type=F32)
            some = total > 0.0
            safe = jnp.where(some, total, 1.0)
            lse = jnp.where(some, top + jnp.log2(safe), NEG_BIG)
            out = out.reshape(group, tile, LANES) * (1.0 / safe)
            stats = jnp.zeros((tile, LANES), F32)
            for n in range(group):
                stats = jnp.where(stat_lane == n, lse[n], stats)
            seat = lax.rem(i, blocks_per_tile) * PER + one
            o_rows[pl.ds(pl.multiple_of(seat * per_row, 8), per_row), :] = out.reshape(per_row, LANES)
            stat_rows[pl.ds(pl.multiple_of(seat * tile, 8), tile), :] = stats
        @pl.when(lax.rem(i, blocks_per_tile) == blocks_per_tile - 1)
        def _():
            where = pl.ds(pl.multiple_of((i // blocks_per_tile) * 8, 8), 8)
            for s in range(steps):
                o_ref[s, where, lse_cols] = sum(stat_rows[pl.ds(h * steps + s, 8, stride=tile), :] for h in range(kvs))
                for h in range(kvs):
                    for n in range(group):
                        col = (h * group + n) * LANES
                        o_ref[s, where, col:col + LANES] = o_rows[pl.ds(n * tile + h * steps + s, 8, stride=per_row), :]

    renew(jnp.int32(n_blocks - 1))
    for copy in put(n_blocks - 1):
        copy.start()
    for j in range(AHEAD):
        for copy in put(n_blocks - AHEAD + j):
            copy.wait()


def attend(positions, q, k_new, v_new, k_rows, v_rows, steps, kvs, group, slots, handed=()):
    batch, rows, dim = k_rows.shape
    half = batch // 2
    vm = pl.BlockSpec(memory_space=pltpu.VMEM)
    hbm = pl.BlockSpec(memory_space=pl.ANY)
    return pl.pallas_call(
        functools.partial(attend_kernel, (steps, kvs, group, slots, half // PER, bool(handed))),
        in_specs=[pl.BlockSpec(memory_space=pltpu.SMEM), vm, vm, vm, hbm, hbm] + [hbm] * len(handed),
        out_specs=[hbm, hbm, vm],
        out_shape=[
            jax.ShapeDtypeStruct(k_rows.shape, BF16),
            jax.ShapeDtypeStruct(v_rows.shape, BF16),
            jax.ShapeDtypeStruct((steps, half, (kvs * group + 1) * dim), F32),
        ],
        input_output_aliases={6: 0, 7: 1} if handed else {},
        scratch_shapes=[
            pltpu.VMEM((DEPTH, PER, rows, dim), BF16),
            pltpu.VMEM((DEPTH, PER, rows, dim), BF16),
            pltpu.VMEM((8 * q.shape[1], dim), F32),
            pltpu.VMEM((8 * steps * kvs, dim), F32),
            pltpu.SemaphoreType.DMA((DEPTH,)),
            pltpu.SemaphoreType.DMA((DEPTH,)),
            pltpu.SemaphoreType.DMA((DEPTH,)),
            pltpu.SemaphoreType.DMA((DEPTH,)),
        ],
        compiler_params=pltpu.CompilerParams(vmem_limit_bytes=48 * 2**20),
        cost_estimate=pl.CostEstimate(flops=20_000_000_000, bytes_accessed=4 * batch * rows * dim,
                                      transcendentals=half * rows * q.shape[1]),
        name="attend_own" if handed else "attend_peer",
    )(positions, q, k_new, v_new, k_rows, v_rows, *handed)


CHUNK = 512
RING = 6
(C_OWN_O, C_X_O, C_OWN_E, C_X_E, C_HID_A, C_HID_B) = range(6)
(W_CORE, W_Y, J_CORE, J_Y, J_OWN_X, J_OWN_C, J_FWD_C) = range(7)


def tail_kernel(cfg, own_ref, xin_ref, x_hbm, wo_hbm, wfc_hbm, wproj_hbm, bo_ref, gain_ref, shift_ref, bfc_ref, bproj_ref,
                y_ref,
                sib_own, sib_x, sib_own_e, sib_x_e, a_buf, wo_buf, w_part, w_core, w_half, w_y, x_buf, x_mid, hid, hid_b,
                ring, g_buf, p_part, p_core, p_half, p_y, y_all, bo_rows, bfc_rows, bproj_rows,
                send_a, recv_a, send_j, recv_j, wo_sem, x_sem, ring_sem):
    steps, batch, group, chunks, kvs = cfg
    half = batch // 2
    pair = steps // 2 * half
    head_cols = group * LANES
    ff_own = wfc_hbm.shape[1] // 2
    per_chunk = CHUNK // LANES
    y = lax.axis_index("tp")
    sq = lax.axis_index("sq")
    x, c = sq // 2, sq % 2
    sib = {"sq": x * 2 + 1 - c}
    xpeer = {"sq": (1 - x) * 2 + c}
    ypeer = {"tp": 1 - y}
    MESH = pl.DeviceIdType.MESH

    def chunk_cols(j):
        return pl.ds(pl.multiple_of(j * CHUNK, CHUNK), CHUNK)

    def load_item(item, slot):
        @pl.when(item < chunks)
        def _():
            col = pl.multiple_of(c * ff_own + item * CHUNK, CHUNK)
            pltpu.make_async_copy(wfc_hbm.at[:, pl.ds(col, CHUNK)], ring.at[slot], ring_sem.at[slot]).start()

        @pl.when(item >= chunks)
        def _():
            row = pl.multiple_of(c * ff_own, CHUNK)
            pltpu.make_async_copy(wproj_hbm.at[pl.ds(row, ff_own), chunk_cols(item - chunks)], ring.at[slot], ring_sem.at[slot]).start()

    def wait_item(slot):
        pltpu.make_async_copy(wfc_hbm.at[:, pl.ds(0, CHUNK)], ring.at[slot], ring_sem.at[slot]).wait()

    wo_rows = pl.ds(pl.multiple_of(c * head_cols, LANES), head_cols)
    wo_copy = pltpu.make_async_copy(wo_hbm.at[wo_rows, :], wo_buf, wo_sem)
    wo_copy.start()
    x_copy = pltpu.make_async_copy(x_hbm.at[pl.ds(2 * c, 2), pl.ds(pl.multiple_of(x * half, 8), half), :], x_buf, x_sem)
    x_copy.start()
    for k in range(RING):
        load_item(jnp.int32(k), k)

    barrier = pltpu.get_barrier_semaphore()
    for who in (sib, xpeer, ypeer):
        pl.semaphore_signal(barrier, inc=1, device_id=who, device_id_type=MESH)
    pl.semaphore_wait(barrier, 3)

    def remote(src, dst, kind, who):
        return pltpu.make_async_remote_copy(src_ref=src, dst_ref=dst, send_sem=send_a.at[kind], recv_sem=recv_a.at[kind],
                                            device_id=who, device_id_type=MESH)

    sib_cols = pl.ds(pl.multiple_of((1 - c) * head_cols, LANES), head_cols)
    stat_cols = slice(kvs * head_cols, kvs * head_cols + LANES)
    swaps = [remote(own_ref.at[:, :, stat_cols], sib_own_e, C_OWN_E, sib), remote(xin_ref.at[:, :, stat_cols], sib_x_e, C_X_E, sib),
             remote(own_ref.at[:, :, sib_cols], sib_own, C_OWN_O, sib), remote(xin_ref.at[:, :, sib_cols], sib_x, C_X_O, sib)]
    for copy in swaps:
        copy.start()
    bo_rows[...] = bo_ref[...].astype(F32)
    bfc_rows[...] = bfc_ref[...].astype(F32)
    bproj_rows[...] = bproj_ref[...].astype(F32)

    def flat(block):
        return block.reshape(steps * half, LANES)

    def my_lanes(stat):
        stat = flat(stat)
        return jnp.where(c == 0, stat, pltpu.roll(stat, LANES - group, 1))

    swaps[0].wait_recv()
    swaps[1].wait_recv()
    logs = [my_lanes(own_ref[:, :, stat_cols]), my_lanes(sib_own_e[...]), my_lanes(xin_ref[:, :, stat_cols]), my_lanes(sib_x_e[...])]
    top = functools.reduce(jnp.maximum, logs)
    shares = [jnp.exp2(e - top) for e in logs]
    inv = 1.0 / sum(shares)
    shares = [w * inv for w in shares]
    swaps[2].wait_recv()
    swaps[3].wait_recv()
    for i in range(group):
        mine = pl.ds(pl.multiple_of(c * head_cols + i * LANES, LANES), LANES)
        theirs = slice(i * LANES, (i + 1) * LANES)
        parts = [own_ref[:, :, mine], sib_own[:, :, theirs], xin_ref[:, :, mine], sib_x[:, :, theirs]]
        a_buf[:, theirs] = sum(w[:, i:i + 1] * flat(part) for w, part in zip(shares, parts)).astype(BF16)

    def jcopy(src, dst, kind, j, who):
        return pltpu.make_async_remote_copy(src_ref=src, dst_ref=dst, send_sem=send_j.at[kind, j], recv_sem=recv_j.at[kind, j],
                                            device_id=who, device_id_type=MESH)

    def pair_rows(core):
        return pl.ds(pl.multiple_of(core * pair, 8), pair)

    def to_core(part, inbox, kind, j):
        return jcopy(part.at[j, pair_rows(1 - c), :], inbox.at[j], kind, j, sib)

    def to_y(total, inbox, kind, j):
        return jcopy(total.at[j], inbox.at[j], kind, j, ypeer)

    def core_sum(part, inbox, total, inbox_y, kind, kind_y, j):
        to_core(part, inbox, kind, j).wait_recv()
        total[j] = part[j, pair_rows(c), :] + inbox[j]
        to_y(total, inbox_y, kind_y, j).start()

    def bias_of(rows, j):
        return jnp.concatenate([rows[pl.ds(j * per_chunk + e, 1), :] for e in range(per_chunk)], axis=-1)

    def y_sum(total, inbox):
        low = jnp.where(y == 0, total, inbox)
        high = jnp.where(y == 0, inbox, total)
        return low + high

    def stage(it, lag, body):
        j = it - lag

        @pl.when((j >= 0) & (j < chunks))
        def _():
            body(j)

    def o_product(j):
        w_part[j] = jnp.dot(a_buf[...], wo_buf[:, chunk_cols(j)], preferred_element_type=F32)
        to_core(w_part, w_core, W_CORE, j).start()

    def o_core_sum(j):
        core_sum(w_part, w_core, w_half, w_y, W_CORE, W_Y, j)

    wo_copy.wait()
    x_copy.wait()

    @pl.loop(0, chunks + 3)
    def _(it):
        stage(it, 0, o_product)
        stage(it, 3, o_core_sum)

    @pl.loop(0, chunks)
    def _(j):
        cols = chunk_cols(j)
        to_y(w_half, w_y, W_Y, j).wait_recv()
        x_in = x_buf[:, :, cols].astype(F32).reshape(pair, CHUNK)
        x_mid[:, cols] = (x_in + y_sum(w_half[j], w_y[j]) + bias_of(bo_rows, j)).astype(BF16).astype(F32)

    gain = gain_ref[...].astype(F32)
    shift = shift_ref[...].astype(F32)
    d_model = x_mid.shape[1]
    hid_copies = []
    for part in range(2):
        src = slice(part * half, (part + 1) * half)
        dst = pl.ds(pl.multiple_of(c * pair + part * half, 8), half)
        rows = x_mid[src, :]
        mean = jnp.mean(rows, axis=-1, keepdims=True)
        cent = rows - mean
        rstd = lax.rsqrt(jnp.mean(cent * cent, axis=-1, keepdims=True) + LN_EPS)
        for n in range(d_model // LANES):
            cols = slice(n * LANES, (n + 1) * LANES)
            hid[dst, cols] = (cent[:, cols] * rstd * gain[n:n + 1, :] + shift[n:n + 1, :]).astype(BF16).astype(F32)
        copy = remote(hid.at[dst, :], hid.at[dst, :], (C_HID_A, C_HID_B)[part], sib)
        copy.start()
        hid_copies.append(copy)
    for copy in hid_copies:
        copy.wait_recv()
    hid_b[...] = hid[...].astype(BF16)

    @pl.loop(0, chunks)
    def _(j):
        slot = lax.rem(j, RING)
        wait_item(slot)
        pre = jnp.dot(hid_b[...], ring[slot], preferred_element_type=F32) + bias_of(bfc_rows, c * chunks + j)
        cube = pre * pre * pre
        act = 0.5 * pre * (1.0 + jnp.tanh(math.sqrt(2.0 / math.pi) * (pre + 0.044715 * cube)))
        g_buf[:, chunk_cols(j)] = act.astype(BF16)
        load_item(j + RING, slot)

    def block(j, core, xx):
        return y_all.at[j, pl.ds(2 * core, 2), pl.ds(pl.multiple_of(xx * half, 8), half), :]

    def spread(kind, j):
        ref, who = {J_OWN_X: (block(j, c, x), xpeer), J_OWN_C: (block(j, c, x), sib), J_FWD_C: (block(j, c, 1 - x), sib)}[kind]
        return jcopy(ref, ref, kind, j, who)

    def do_product(j):
        item = chunks + j
        slot = lax.rem(item, RING)
        wait_item(slot)
        p_part[j] = jnp.dot(g_buf[...], ring[slot], preferred_element_type=F32)

        @pl.when(item + RING < 2 * chunks)
        def _():
            load_item(item + RING, slot)

        to_core(p_part, p_core, J_CORE, j).start()

    def do_core_sum(j):
        core_sum(p_part, p_core, p_half, p_y, J_CORE, J_Y, j)

    def do_y_sum(j):
        to_y(p_half, p_y, J_Y, j).wait_recv()
        full = x_mid[:, chunk_cols(j)] + y_sum(p_half[j], p_y[j]) + bias_of(bproj_rows, j)
        y_all[j, pl.ds(2 * c, 2), pl.ds(pl.multiple_of(x * half, 8), half), :] = full.astype(BF16).astype(F32).reshape(2, half, CHUNK)
        spread(J_OWN_X, j).start()
        spread(J_OWN_C, j).start()

    def do_forward(j):
        spread(J_OWN_X, j).wait_recv()
        spread(J_FWD_C, j).start()

    def do_store(j):
        spread(J_OWN_C, j).wait_recv()
        spread(J_FWD_C, j).wait_recv()
        y_ref[:, :, chunk_cols(j)] = y_all[j].astype(BF16)

    @pl.loop(0, chunks + 7)
    def _(it):
        stage(it, 0, do_product)
        stage(it, 1, do_core_sum)
        stage(it, 3, do_y_sum)
        stage(it, 5, do_forward)
        stage(it, 7, do_store)

    for copy in swaps + hid_copies:
        copy.wait_send()

    @pl.loop(0, chunks)
    def _(j):
        to_core(w_part, w_core, W_CORE, j).wait_send()
        to_y(w_half, w_y, W_Y, j).wait_send()
        to_core(p_part, p_core, J_CORE, j).wait_send()
        to_y(p_half, p_y, J_Y, j).wait_send()
        for kind in (J_OWN_X, J_OWN_C, J_FWD_C):
            spread(kind, j).wait_send()


def tail(own, x_in, x_steps, w_o, w_fc, w_proj, b_o, gain, shift, b_fc, b_proj, group, kvs):
    steps, half, _ = own.shape
    batch = 2 * half
    rows = steps * half
    pair = rows // 2
    d_model = w_o.shape[1]
    chunks = d_model // CHUNK
    ff_own = w_fc.shape[1] // 2
    assert ff_own == d_model and steps == 4 and kvs == 2
    head_cols = group * LANES
    vm = pl.BlockSpec(memory_space=pltpu.VMEM)
    hbm = pl.BlockSpec(memory_space=pl.ANY)
    cfg = (steps, batch, group, chunks, kvs)
    tiles = lambda vec: vec.reshape(-1, LANES)
    scratch = [
        pltpu.VMEM((steps, half, head_cols), F32),
        pltpu.VMEM((steps, half, head_cols), F32),
        pltpu.VMEM((steps, half, LANES), F32),
        pltpu.VMEM((steps, half, LANES), F32),
        pltpu.VMEM((rows, head_cols), BF16),
        pltpu.VMEM((head_cols, d_model), BF16),
        pltpu.VMEM((chunks, rows, CHUNK), F32),
        pltpu.VMEM((chunks, pair, CHUNK), F32),
        pltpu.VMEM((chunks, pair, CHUNK), F32),
        pltpu.VMEM((chunks, pair, CHUNK), F32),
        pltpu.VMEM((2, half, d_model), BF16),
        pltpu.VMEM((pair, d_model), F32),
        pltpu.VMEM((rows, d_model), F32),
        pltpu.VMEM((rows, d_model), BF16),
        pltpu.VMEM((RING, d_model, CHUNK), BF16),
        pltpu.VMEM((rows, ff_own), BF16),
        pltpu.VMEM((chunks, rows, CHUNK), F32),
        pltpu.VMEM((chunks, pair, CHUNK), F32),
        pltpu.VMEM((chunks, pair, CHUNK), F32),
        pltpu.VMEM((chunks, pair, CHUNK), F32),
        pltpu.VMEM((chunks, steps, batch, CHUNK), F32),
        pltpu.VMEM((d_model // LANES, LANES), F32),
        pltpu.VMEM((2 * ff_own // LANES, LANES), F32),
        pltpu.VMEM((d_model // LANES, LANES), F32),
        pltpu.SemaphoreType.DMA((6,)),
        pltpu.SemaphoreType.DMA((6,)),
        pltpu.SemaphoreType.DMA((7, chunks)),
        pltpu.SemaphoreType.DMA((7, chunks)),
        pltpu.SemaphoreType.DMA,
        pltpu.SemaphoreType.DMA,
        pltpu.SemaphoreType.DMA((RING,)),
    ]
    return pl.pallas_call(
        functools.partial(tail_kernel, cfg),
        out_shape=jax.ShapeDtypeStruct((steps, batch, d_model), BF16),
        in_specs=[vm, vm, hbm, hbm, hbm, hbm] + [vm] * 5,
        out_specs=vm,
        scratch_shapes=scratch,
        compiler_params=pltpu.CompilerParams(collective_id=0, has_side_effects=True, vmem_limit_bytes=VMEM_CAP),
        cost_estimate=pl.CostEstimate(flops=2 * rows * d_model * (head_cols + 2 * ff_own), bytes_accessed=100_000_000, transcendentals=0),
        name="tail",
    )(own, x_in, x_steps, w_o, w_fc, w_proj, tiles(b_o), tiles(gain), tiles(shift), tiles(b_fc), tiles(b_proj))


def solution(mesh):
    sq_size = mesh.shape["sq"]
    act_spec = P(None, "dp", None)
    cache_spec = P("dp", "sq", "tp", None)
    col_spec = P(None, "tp")
    row_spec = P("tp", None)
    vec_spec = P("tp")
    rep_spec = P(None)
    in_specs = (act_spec, P("dp"), cache_spec, cache_spec, col_spec, vec_spec, col_spec, vec_spec,
                col_spec, vec_spec, row_spec, rep_spec, rep_spec, rep_spec, rep_spec, rep_spec,
                col_spec, vec_spec, row_spec, rep_spec)
    out_specs = (act_spec, cache_spec, cache_spec)

    def per_device(x_steps, positions, key_buf, val_buf, w_q, b_q, w_k, b_k, w_v, b_v, w_o, b_o,
                   ln1_gain, ln1_bias, ln2_gain, ln2_bias, w_fc, b_fc, w_proj, b_proj):
        steps, batch, d_model = x_steps.shape
        slots_local, kvs, dim = key_buf.shape[1], key_buf.shape[2], key_buf.shape[3]
        slots = slots_local * sq_size
        group = w_q.shape[1] // (kvs * dim)
        cur_pos = positions[None, :] + jnp.arange(steps, dtype=jnp.int32)[:, None]
        cos_t, sin_t = rope_tables(cur_pos, dim)
        q_rows, k_new, v_new = front(x_steps, ln1_gain, ln1_bias, cos_t, sin_t, b_q, b_k, b_v, w_q, w_k, w_v, kvs)
        k_rows = key_buf.reshape(batch, slots_local * kvs, dim)
        v_rows = val_buf.reshape(batch, slots_local * kvs, dim)
        caches = (positions, q_rows, k_new, v_new, k_rows, v_rows, steps, kvs, group, slots)
        k_out, v_out, for_peer = attend(*caches)
        from_peer = lax.ppermute(for_peer, "sq", [(d, d ^ 2) for d in range(sq_size)])
        k_out, v_out, own = attend(*caches, handed=(k_out, v_out))
        ys = tail(own, from_peer, x_steps, w_o, w_fc, w_proj, b_o, ln2_gain, ln2_bias, b_fc, b_proj, group, kvs)
        return ys, k_out.reshape(key_buf.shape), v_out.reshape(val_buf.shape)

    return jax.shard_map(per_device, mesh=mesh, in_specs=in_specs, out_specs=out_specs, check_vma=False)
```

```python
import functools
import math

import jax
import jax.numpy as jnp
from jax import lax
from jax.experimental import pallas as pl
from jax.experimental.pallas import tpu as pltpu
from jax.sharding import PartitionSpec as P

ROPE_BASE = 1000000.0
LN_EPS = 1e-5
NEG_BIG = -1e30
NEG_HALF = -1e29
LOG2E = 1.4426950408889634
VMEM_CAP = 67_043_328
F32 = jnp.float32
BF16 = jnp.bfloat16
LANES = 128


def rope_tables(positions, head_dim):
    half_dim = head_dim // 2
    inv_freq = jnp.power(F32(ROPE_BASE), -2.0 * jnp.arange(half_dim, dtype=F32) / head_dim)
    angle = positions.astype(F32)[..., None] * inv_freq
    return jnp.cos(angle), jnp.sin(angle)


COLS = 256

def front_kernel(cfg, x_ref, gain_ref, shift_ref, cos_ref, sin_ref, bq_ref, bk_ref, bv_ref, wq_hbm, wk_hbm, wv_hbm,
                 q_out, kn_out, vn_out, hid, wq_buf, wk_buf, wv_buf, q_rows, kv_rows, bias_q, sem):
    steps, kvs, group = cfg
    batch, d_model = x_ref.shape[1], x_ref.shape[2]
    n_q = wq_hbm.shape[1] // COLS
    per_row = group * kvs * steps
    copies = [pltpu.make_async_copy(wk_hbm, wk_buf, sem.at[n_q]), pltpu.make_async_copy(wv_hbm, wv_buf, sem.at[n_q + 1])]
    for copy in copies:
        copy.start()
    for n in range(n_q):
        pltpu.make_async_copy(wq_hbm.at[:, n * COLS:(n + 1) * COLS], wq_buf.at[n], sem.at[n]).start()

    bias_q[...] = bq_ref[...].astype(F32)
    gain = gain_ref[...].astype(F32)
    shift = shift_ref[...].astype(F32)
    for s in range(steps):
        wide = x_ref[s].astype(F32)
        mean = jnp.mean(wide, axis=-1, keepdims=True)
        cent = wide - mean
        rstd = lax.rsqrt(jnp.mean(cent * cent, axis=-1, keepdims=True) + LN_EPS)
        for n in range(d_model // LANES):
            cols = slice(n * LANES, (n + 1) * LANES)
            hid[s * batch:(s + 1) * batch, cols] = (cent[:, cols] * rstd * gain[n:n + 1, :] + shift[n:n + 1, :]).astype(BF16)

    cos = cos_ref[...].reshape(steps * batch, LANES // 2)
    sin = sin_ref[...].reshape(steps * batch, LANES // 2)
    cos_full = jnp.concatenate([cos, cos], axis=-1)
    sin_full = jnp.concatenate([-sin, sin], axis=-1)

    def rotate(vec):
        return (vec * cos_full + pltpu.roll(vec, LANES // 2, 1) * sin_full).astype(BF16).astype(F32)

    def rounded(weight, bias):
        return (jnp.dot(hid[...], weight, preferred_element_type=F32) + bias).astype(BF16).astype(F32)

    for rope, copy, buf, b_ref, out in ((True, copies[0], wk_buf, bk_ref, kn_out), (False, copies[1], wv_buf, bv_ref, vn_out)):
        copy.wait()
        kv_rows[...] = jnp.zeros_like(kv_rows)
        bias = b_ref[...].astype(F32)
        both = rounded(buf[...], jnp.concatenate([bias[h:h + 1] for h in range(kvs)], axis=-1))
        for h in range(kvs):
            vec = both[:, h * LANES:(h + 1) * LANES]
            if rope:
                vec = rotate(vec)
            for s in range(steps):
                kv_rows[pl.ds(s * kvs + h, batch, stride=16), :] = vec[s * batch:(s + 1) * batch]
        out[...] = kv_rows[...].reshape(out.shape).astype(BF16)

    heads = COLS // LANES

    @pl.loop(0, n_q)
    def _(n):
        pltpu.make_async_copy(wq_hbm.at[:, 0:COLS], wq_buf.at[n], sem.at[n]).wait()
        bias = jnp.concatenate([bias_q[pl.ds(n * heads + e, 1), :] for e in range(heads)], axis=-1)
        both = rounded(wq_buf[n], bias)
        for e in range(heads):
            vec = rotate(both[:, e * LANES:(e + 1) * LANES])
            head = n * heads + e
            row = lax.rem(head, group) * (kvs * steps) + (head // group) * steps
            for s in range(steps):
                q_rows[pl.ds(row + s, batch, stride=per_row), :] = vec[s * batch:(s + 1) * batch]

    @pl.loop(0, batch)
    def _(b):
        q_out[b] = q_rows[pl.ds(pl.multiple_of(b * per_row, 8), per_row), :].astype(BF16)


def front(x_steps, gain, shift, cos_t, sin_t, b_q, b_k, b_v, w_q, w_k, w_v, kvs):
    steps, batch, d_model = x_steps.shape
    heads = w_q.shape[1] // LANES
    group = heads // kvs
    rows = group * kvs * steps
    n_q = w_q.shape[1] // COLS
    vm = pl.BlockSpec(memory_space=pltpu.VMEM)
    hbm = pl.BlockSpec(memory_space=pl.ANY)
    tiles = lambda vec: vec.reshape(-1, LANES)
    return pl.pallas_call(
        functools.partial(front_kernel, (steps, kvs, group)),
        out_shape=[
            jax.ShapeDtypeStruct((batch, rows, LANES), BF16),
            jax.ShapeDtypeStruct((batch, 16, LANES), BF16),
            jax.ShapeDtypeStruct((batch, 16, LANES), BF16),
        ],
        in_specs=[vm] * 8 + [hbm] * 3,
        out_specs=[vm] * 3,
        scratch_shapes=[
            pltpu.VMEM((steps * batch, d_model), BF16),
            pltpu.VMEM((n_q, d_model, COLS), BF16),
            pltpu.VMEM(w_k.shape, BF16),
            pltpu.VMEM(w_v.shape, BF16),
            pltpu.VMEM((batch * rows, LANES), F32),
            pltpu.VMEM((batch * 16, LANES), F32),
            pltpu.VMEM((heads, LANES), F32),
            pltpu.SemaphoreType.DMA((n_q + 2,)),
        ],
        compiler_params=pltpu.CompilerParams(vmem_limit_bytes=56 * 2**20),
        cost_estimate=pl.CostEstimate(flops=2 * steps * batch * d_model * (w_q.shape[1] + 2 * w_k.shape[1]),
                                      bytes_accessed=2 * d_model * (w_q.shape[1] + 2 * w_k.shape[1]), transcendentals=0),
        name="front",
    )(x_steps, tiles(gain), tiles(shift), cos_t, sin_t, tiles(b_q), tiles(b_k), tiles(b_v), w_q, w_k, w_v)


PER = 2
DEPTH = 8
AHEAD = 4

def attend_kernel(cfg, pos_ref, q_hbm, kn_hbm, vn_hbm, k_hbm, v_hbm, *refs):
    steps, kvs, group, slots, n_blocks, own_half = cfg
    (ko_hbm, vo_hbm, o_hbm, k_buf, v_buf, q_ref, kn_ref, vn_ref, o_tile, o_rows, stat_rows,
     k_in, v_in, k_up, v_up, small_in, o_up) = refs[2 if own_half else 0:]
    x = lax.axis_index("sq") // 2
    base = (x if own_half else 1 - x) * (n_blocks * PER)
    lse_cols = slice(kvs * group * LANES, (kvs * group + 1) * LANES)
    rows = k_hbm.shape[1]
    tile = steps * kvs
    per_row = group * tile
    first = lax.axis_index("sq") * (rows // kvs)
    coef = LANES ** -0.5 * LOG2E
    contract_last = (((1,), (1,)), ((), ()))
    blocks_per_tile = 8 // PER

    def seqs(i):
        return pl.ds(base + i * PER, PER)

    def fetch(i):
        slot = lax.rem(i, DEPTH)
        return (pltpu.make_async_copy(k_hbm.at[seqs(i)], k_buf.at[slot], k_in.at[slot]),
                pltpu.make_async_copy(v_hbm.at[seqs(i)], v_buf.at[slot], v_in.at[slot]))

    def put(i):
        slot = lax.rem(i, DEPTH)
        return (pltpu.make_async_copy(k_buf.at[slot], ko_hbm.at[seqs(i)], k_up.at[slot]),
                pltpu.make_async_copy(v_buf.at[slot], vo_hbm.at[seqs(i)], v_up.at[slot]))

    half_seqs = pl.ds(base, n_blocks * PER)
    small = [pltpu.make_async_copy(src.at[half_seqs], dst, small_in.at[n])
             for n, (src, dst) in enumerate(((q_hbm, q_ref), (kn_hbm, kn_ref), (vn_hbm, vn_ref)))]
    for copy in small:
        copy.start()
    for i in range(AHEAD):
        for copy in fetch(jnp.int32(i)):
            copy.start()

    def put_tile(t):
        return pltpu.make_async_copy(o_tile.at[t], o_hbm.at[:, pl.ds(pl.multiple_of(t * 8, 8), 8), :], o_up.at[t])

    for copy in small:
        copy.wait()

    sub = lax.broadcasted_iota(jnp.int32, (tile, rows), 0)
    lane = lax.broadcasted_iota(jnp.int32, (tile, rows), 1)
    sub2 = lax.broadcasted_iota(jnp.int32, (tile, 16), 0)
    lane2 = lax.broadcasted_iota(jnp.int32, (tile, 16), 1)
    new_step = lane2 // kvs
    new_ok = ((lane2 % kvs) == (sub2 // steps)) & (new_step <= sub2 % steps)
    stat_sub = lax.broadcasted_iota(jnp.int32, (tile, LANES), 0)
    stat_lane = lax.broadcasted_iota(jnp.int32, (tile, LANES), 1) - (stat_sub // steps) * group
    win_row = lax.broadcasted_iota(jnp.int32, (32, LANES), 0)

    def renew(i):
        slot_of = lax.rem(i, DEPTH)
        for one in range(PER):
            seq = i * PER + one
            goal = kvs * ((pos_ref[base + seq] & (slots - 1)) - first)
            goal = jnp.where(goal > kvs * (slots - steps), goal - kvs * slots, goal)
            start = pl.multiple_of(jnp.clip((goal >> 4) << 4, 0, rows - 32), 16)
            offset = win_row + (start - goal)
            for buf, new in ((k_buf, kn_ref), (v_buf, vn_ref)):
                fresh = new[seq].astype(F32)
                window = buf[slot_of, one, pl.ds(start, 32), :].astype(F32)
                for r in range(tile):
                    window = jnp.where(offset == r, fresh[r:r + 1, :], window)
                buf[slot_of, one, pl.ds(start, 32), :] = window.astype(BF16)

    @pl.loop(0, n_blocks)
    def _(i):
        slot_now = lax.rem(i, DEPTH)

        @pl.when(i >= 1)
        def _():
            renew(i - 1)

        @pl.when(i >= AHEAD)
        def _():
            for copy in put(i - AHEAD):
                copy.wait()

        @pl.when(i + AHEAD < n_blocks)
        def _():
            for copy in fetch(i + AHEAD):
                copy.start()

        @pl.when(i >= 1)
        def _():
            for copy in put(i - 1):
                copy.start()

        @pl.when((i >= 1) & (lax.rem(i, blocks_per_tile) == 0))
        def _():
            put_tile(i // blocks_per_tile - 1).start()

        k_copy, v_copy = fetch(i)
        k_copy.wait()
        v_copy.wait()
        state = []
        for one in range(PER):
            seq = i * PER + one
            pos = pos_ref[base + seq]
            q = q_ref[seq]
            raw = lax.dot_general(q, k_buf[slot_now, one], contract_last, preferred_element_type=F32)
            raw2 = lax.dot_general(q, kn_ref[seq], contract_last, preferred_element_type=F32)
            state.append((seq, pos, raw, raw2))
        soft = []
        for seq, pos, raw, raw2 in state:
            slot = first + (lane >> 1)
            ahead = (slot - pos) & (slots - 1)
            ok = ((lane & 1) == (sub >> 2)) & (slot < pos) & (ahead > (sub & 3))
            bias = jnp.where(ok, 0.0, NEG_BIG).astype(F32)
            new_slot = ((pos + new_step) & (slots - 1)) - first
            here = (new_slot >= 0) & (new_slot < rows // kvs)
            bias2 = jnp.where(new_ok & here, 0.0, NEG_BIG).astype(F32)
            score = raw.reshape(group, tile, rows) * coef + bias[None]
            score2 = raw2.reshape(group, tile, 16) * coef + bias2[None]
            top = jnp.maximum(jnp.max(score, axis=-1, keepdims=True), jnp.max(score2, axis=-1, keepdims=True))
            top = jnp.maximum(top, NEG_HALF)
            w = jnp.exp2(score - top)
            w2 = jnp.exp2(score2 - top)
            total = jnp.sum(w, axis=-1, keepdims=True) + jnp.sum(w2, axis=-1, keepdims=True)
            soft.append((top, total, w.reshape(per_row, rows).astype(BF16), w2.reshape(per_row, 16).astype(BF16)))
        for one in range(PER):
            seq, pos = state[one][:2]
            top, total, w, w2 = soft[one]
            out = jnp.dot(w, v_buf[slot_now, one], preferred_element_type=F32)
            out = out + jnp.dot(w2, vn_ref[seq], preferred_element_type=F32)
            some = total > 0.0
            safe = jnp.where(some, total, 1.0)
            lse = jnp.where(some, top + jnp.log2(safe), NEG_BIG)
            out = out.reshape(group, tile, LANES) * (1.0 / safe)
            stats = jnp.zeros((tile, LANES), F32)
            for n in range(group):
                stats = jnp.where(stat_lane == n, lse[n], stats)
            seat = lax.rem(i, blocks_per_tile) * PER + one
            o_rows[pl.ds(pl.multiple_of(seat * per_row, 8), per_row), :] = out.reshape(per_row, LANES)
            stat_rows[pl.ds(pl.multiple_of(seat * tile, 8), tile), :] = stats
        @pl.when(lax.rem(i, blocks_per_tile) == blocks_per_tile - 1)
        def _():
            t = i // blocks_per_tile
            for s in range(steps):
                o_tile[t, s, :, lse_cols] = sum(stat_rows[pl.ds(h * steps + s, 8, stride=tile), :] for h in range(kvs))
                for h in range(kvs):
                    for n in range(group):
                        col = (h * group + n) * LANES
                        o_tile[t, s, :, col:col + LANES] = o_rows[pl.ds(n * tile + h * steps + s, 8, stride=per_row), :]

    renew(jnp.int32(n_blocks - 1))
    for copy in put(n_blocks - 1):
        copy.start()
    tiles = n_blocks // blocks_per_tile
    put_tile(tiles - 1).start()
    for j in range(AHEAD):
        for copy in put(n_blocks - AHEAD + j):
            copy.wait()
    for t in range(tiles):
        put_tile(t).wait()


def attend(positions, q, k_new, v_new, k_rows, v_rows, steps, kvs, group, slots, handed=()):
    batch, rows, dim = k_rows.shape
    half = batch // 2
    hbm = pl.BlockSpec(memory_space=pl.ANY)
    return pl.pallas_call(
        functools.partial(attend_kernel, (steps, kvs, group, slots, half // PER, bool(handed))),
        in_specs=[pl.BlockSpec(memory_space=pltpu.SMEM)] + [hbm] * (5 + len(handed)),
        out_specs=[hbm, hbm, hbm],
        out_shape=[
            jax.ShapeDtypeStruct(k_rows.shape, BF16),
            jax.ShapeDtypeStruct(v_rows.shape, BF16),
            jax.ShapeDtypeStruct((steps, half, (kvs * group + 1) * dim), F32),
        ],
        input_output_aliases={6: 0, 7: 1} if handed else {},
        scratch_shapes=[
            pltpu.VMEM((DEPTH, PER, rows, dim), BF16),
            pltpu.VMEM((DEPTH, PER, rows, dim), BF16),
            pltpu.VMEM((half, q.shape[1], dim), BF16),
            pltpu.VMEM((half, k_new.shape[1], dim), BF16),
            pltpu.VMEM((half, v_new.shape[1], dim), BF16),
            pltpu.VMEM((half // 8, steps, 8, (kvs * group + 1) * dim), F32),
            pltpu.VMEM((8 * q.shape[1], dim), F32),
            pltpu.VMEM((8 * steps * kvs, dim), F32),
            pltpu.SemaphoreType.DMA((DEPTH,)),
            pltpu.SemaphoreType.DMA((DEPTH,)),
            pltpu.SemaphoreType.DMA((DEPTH,)),
            pltpu.SemaphoreType.DMA((DEPTH,)),
            pltpu.SemaphoreType.DMA((3,)),
            pltpu.SemaphoreType.DMA((half // 8,)),
        ],
        compiler_params=pltpu.CompilerParams(vmem_limit_bytes=VMEM_CAP),
        cost_estimate=pl.CostEstimate(flops=20_000_000_000, bytes_accessed=4 * batch * rows * dim,
                                      transcendentals=half * rows * q.shape[1]),
        name="attend_own" if handed else "attend_peer",
    )(positions, q, k_new, v_new, k_rows, v_rows, *handed)


CHUNK = 512
RING = 9
WO_SLOTS = 3
(C_OWN_O, C_X_O, C_OWN_E, C_X_E, C_HID_A, C_HID_B) = range(6)
(W_CORE, W_Y, J_CORE, J_Y, J_OWN_X, J_OWN_C, J_FWD_C) = range(7)


def tail_kernel(cfg, own_hbm, xin_hbm, x_hbm, wo_hbm, wfc_hbm, wproj_hbm, bo_ref, gain_ref, shift_ref, bfc_ref, bproj_ref,
                y_ref,
                my_own, my_x, my_own_e, my_x_e, sib_own, sib_x, sib_own_e, sib_x_e, a_buf, w_part, w_core, w_half, w_y, x_buf, x_mid, hid, hid_b,
                ring, g_buf, p_part, p_core, p_half, p_y, y_all, bo_rows, bfc_rows, bproj_rows,
                send_a, recv_a, send_j, recv_j, local_sem, wo_sem, x_sem, ring_sem):
    steps, batch, group, chunks, kvs = cfg
    half = batch // 2
    pair = steps // 2 * half
    head_cols = group * LANES
    ff_own = wfc_hbm.shape[1] // 2
    per_chunk = CHUNK // LANES
    y = lax.axis_index("tp")
    sq = lax.axis_index("sq")
    x, c = sq // 2, sq % 2
    sib = {"sq": x * 2 + 1 - c}
    xpeer = {"sq": (1 - x) * 2 + c}
    ypeer = {"tp": 1 - y}
    MESH = pl.DeviceIdType.MESH

    def chunk_cols(j):
        return pl.ds(pl.multiple_of(j * CHUNK, CHUNK), CHUNK)

    def load_item(item, slot):
        @pl.when(item < chunks)
        def _():
            col = pl.multiple_of(c * ff_own + item * CHUNK, CHUNK)
            pltpu.make_async_copy(wfc_hbm.at[:, pl.ds(col, CHUNK)], ring.at[slot], ring_sem.at[slot]).start()

        @pl.when(item >= chunks)
        def _():
            row = pl.multiple_of(c * ff_own, CHUNK)
            pltpu.make_async_copy(wproj_hbm.at[pl.ds(row, ff_own), chunk_cols(item - chunks)], ring.at[slot], ring_sem.at[slot]).start()

    def wait_item(slot):
        pltpu.make_async_copy(wfc_hbm.at[:, pl.ds(0, CHUNK)], ring.at[slot], ring_sem.at[slot]).wait()

    wo_rows = pl.ds(pl.multiple_of(c * head_cols, LANES), head_cols)
    per_slot = ring.shape[1] // head_cols

    def wo_place(j):
        return ring.at[j // per_slot, pl.ds(pl.multiple_of(lax.rem(j, per_slot) * head_cols, LANES), head_cols), :]

    def wo_copy(j):
        return pltpu.make_async_copy(wo_hbm.at[wo_rows, chunk_cols(j)], wo_place(j), wo_sem.at[j])

    def slot_of(item):
        return lax.rem(item + WO_SLOTS, RING)

    my_cols = pl.ds(pl.multiple_of(c * head_cols, LANES), head_cols)
    stat_cols = slice(kvs * head_cols, kvs * head_cols + LANES)
    locals_ = [pltpu.make_async_copy(src, dst, local_sem.at[n]) for n, (src, dst) in enumerate((
        (own_hbm.at[:, :, stat_cols], my_own_e), (xin_hbm.at[:, :, stat_cols], my_x_e),
        (own_hbm.at[:, :, my_cols], my_own), (xin_hbm.at[:, :, my_cols], my_x)))]
    for copy in locals_:
        copy.start()
    for j in range(chunks):
        wo_copy(jnp.int32(j)).start()
    x_copy = pltpu.make_async_copy(x_hbm.at[pl.ds(2 * c, 2), pl.ds(pl.multiple_of(x * half, 8), half), :], x_buf, x_sem)
    x_copy.start()
    barrier = pltpu.get_barrier_semaphore()
    for who in (sib, xpeer, ypeer):
        pl.semaphore_signal(barrier, inc=1, device_id=who, device_id_type=MESH)
    pl.semaphore_wait(barrier, 3)

    def remote(src, dst, kind, who):
        return pltpu.make_async_remote_copy(src_ref=src, dst_ref=dst, send_sem=send_a.at[kind], recv_sem=recv_a.at[kind],
                                            device_id=who, device_id_type=MESH)

    sib_cols = pl.ds(pl.multiple_of((1 - c) * head_cols, LANES), head_cols)
    swaps = [remote(own_hbm.at[:, :, stat_cols], sib_own_e, C_OWN_E, sib), remote(xin_hbm.at[:, :, stat_cols], sib_x_e, C_X_E, sib),
             remote(own_hbm.at[:, :, sib_cols], sib_own, C_OWN_O, sib), remote(xin_hbm.at[:, :, sib_cols], sib_x, C_X_O, sib)]
    for copy in swaps:
        copy.start()
    bo_rows[...] = bo_ref[...].astype(F32)
    bfc_rows[...] = bfc_ref[...].astype(F32)
    bproj_rows[...] = bproj_ref[...].astype(F32)

    def flat(block):
        return block.reshape(steps * half, LANES)

    def my_lanes(stat):
        stat = flat(stat)
        return jnp.where(c == 0, stat, pltpu.roll(stat, LANES - group, 1))

    for copy in locals_:
        copy.wait()
    swaps[0].wait_recv()
    swaps[1].wait_recv()
    logs = [my_lanes(my_own_e[...]), my_lanes(sib_own_e[...]), my_lanes(my_x_e[...]), my_lanes(sib_x_e[...])]
    top = functools.reduce(jnp.maximum, logs)
    shares = [jnp.exp2(e - top) for e in logs]
    inv = 1.0 / sum(shares)
    shares = [w * inv for w in shares]
    swaps[2].wait_recv()
    swaps[3].wait_recv()
    for i in range(group):
        cols = slice(i * LANES, (i + 1) * LANES)
        parts = [part[:, :, cols] for part in (my_own, sib_own, my_x, sib_x)]
        a_buf[:, cols] = sum(w[:, i:i + 1] * flat(part) for w, part in zip(shares, parts)).astype(BF16)

    def jcopy(src, dst, kind, j, who):
        return pltpu.make_async_remote_copy(src_ref=src, dst_ref=dst, send_sem=send_j.at[kind, j], recv_sem=recv_j.at[kind, j],
                                            device_id=who, device_id_type=MESH)

    def pair_rows(core):
        return pl.ds(pl.multiple_of(core * pair, 8), pair)

    def to_core(part, inbox, kind, j):
        return jcopy(part.at[j, pair_rows(1 - c), :], inbox.at[j], kind, j, sib)

    def to_y(total, inbox, kind, j):
        return jcopy(total.at[j], inbox.at[j], kind, j, ypeer)

    def core_sum(part, inbox, total, inbox_y, kind, kind_y, j):
        to_core(part, inbox, kind, j).wait_recv()
        total[j] = part[j, pair_rows(c), :] + inbox[j]
        to_y(total, inbox_y, kind_y, j).start()

    def bias_of(rows, j):
        return jnp.concatenate([rows[pl.ds(j * per_chunk + e, 1), :] for e in range(per_chunk)], axis=-1)

    def y_sum(total, inbox):
        low = jnp.where(y == 0, total, inbox)
        high = jnp.where(y == 0, inbox, total)
        return low + high

    def stage(it, lag, body):
        j = it - lag

        @pl.when((j >= 0) & (j < chunks))
        def _():
            body(j)

    def o_product(j):
        wo_copy(j).wait()
        w_part[j] = jnp.dot(a_buf[...], wo_place(j)[...], preferred_element_type=F32)
        to_core(w_part, w_core, W_CORE, j).start()

    def o_core_sum(j):
        core_sum(w_part, w_core, w_half, w_y, W_CORE, W_Y, j)

    for k in range(RING - WO_SLOTS):
        load_item(jnp.int32(k), slot_of(k))

    @pl.loop(0, chunks + 3)
    def _(it):
        stage(it, 0, o_product)
        stage(it, 3, o_core_sum)

    for k in range(RING - WO_SLOTS, RING):
        load_item(jnp.int32(k), slot_of(k))
    x_copy.wait()

    @pl.loop(0, chunks)
    def _(j):
        cols = chunk_cols(j)
        to_y(w_half, w_y, W_Y, j).wait_recv()
        x_in = x_buf[:, :, cols].astype(F32).reshape(pair, CHUNK)
        x_mid[:, cols] = (x_in + y_sum(w_half[j], w_y[j]) + bias_of(bo_rows, j)).astype(BF16).astype(F32)

    gain = gain_ref[...].astype(F32)
    shift = shift_ref[...].astype(F32)
    d_model = x_mid.shape[1]
    hid_copies = []
    for part in range(2):
        src = slice(part * half, (part + 1) * half)
        dst = pl.ds(pl.multiple_of(c * pair + part * half, 8), half)
        rows = x_mid[src, :]
        mean = jnp.mean(rows, axis=-1, keepdims=True)
        cent = rows - mean
        rstd = lax.rsqrt(jnp.mean(cent * cent, axis=-1, keepdims=True) + LN_EPS)
        for n in range(d_model // LANES):
            cols = slice(n * LANES, (n + 1) * LANES)
            hid[dst, cols] = (cent[:, cols] * rstd * gain[n:n + 1, :] + shift[n:n + 1, :]).astype(BF16).astype(F32)
        copy = remote(hid.at[dst, :], hid.at[dst, :], (C_HID_A, C_HID_B)[part], sib)
        copy.start()
        hid_copies.append(copy)
    for copy in hid_copies:
        copy.wait_recv()
    hid_b[...] = hid[...].astype(BF16)

    @pl.loop(0, chunks)
    def _(j):
        slot = slot_of(j)
        wait_item(slot)
        pre = jnp.dot(hid_b[...], ring[slot], preferred_element_type=F32) + bias_of(bfc_rows, c * chunks + j)
        cube = pre * pre * pre
        act = 0.5 * pre * (1.0 + jnp.tanh(math.sqrt(2.0 / math.pi) * (pre + 0.044715 * cube)))
        g_buf[:, chunk_cols(j)] = act.astype(BF16)
        load_item(j + RING, slot)

    def block(j, core, xx):
        return y_all.at[j, pl.ds(2 * core, 2), pl.ds(pl.multiple_of(xx * half, 8), half), :]

    def spread(kind, j):
        ref, who = {J_OWN_X: (block(j, c, x), xpeer), J_OWN_C: (block(j, c, x), sib), J_FWD_C: (block(j, c, 1 - x), sib)}[kind]
        return jcopy(ref, ref, kind, j, who)

    def do_product(j):
        item = chunks + j
        slot = slot_of(item)
        wait_item(slot)
        p_part[j] = jnp.dot(g_buf[...], ring[slot], preferred_element_type=F32)

        @pl.when(item + RING < 2 * chunks)
        def _():
            load_item(item + RING, slot)

        to_core(p_part, p_core, J_CORE, j).start()

    def do_core_sum(j):
        core_sum(p_part, p_core, p_half, p_y, J_CORE, J_Y, j)

    def do_y_sum(j):
        to_y(p_half, p_y, J_Y, j).wait_recv()
        full = x_mid[:, chunk_cols(j)] + y_sum(p_half[j], p_y[j]) + bias_of(bproj_rows, j)
        y_all[j, pl.ds(2 * c, 2), pl.ds(pl.multiple_of(x * half, 8), half), :] = full.astype(BF16).astype(F32).reshape(2, half, CHUNK)
        spread(J_OWN_X, j).start()
        spread(J_OWN_C, j).start()

    def do_forward(j):
        spread(J_OWN_X, j).wait_recv()
        spread(J_FWD_C, j).start()

    def do_store(j):
        spread(J_OWN_C, j).wait_recv()
        spread(J_FWD_C, j).wait_recv()
        y_ref[:, :, chunk_cols(j)] = y_all[j].astype(BF16)

    @pl.loop(0, chunks + 7)
    def _(it):
        stage(it, 0, do_product)
        stage(it, 1, do_core_sum)
        stage(it, 3, do_y_sum)
        stage(it, 5, do_forward)
        stage(it, 7, do_store)

    for copy in swaps + hid_copies:
        copy.wait_send()

    @pl.loop(0, chunks)
    def _(j):
        to_core(w_part, w_core, W_CORE, j).wait_send()
        to_y(w_half, w_y, W_Y, j).wait_send()
        to_core(p_part, p_core, J_CORE, j).wait_send()
        to_y(p_half, p_y, J_Y, j).wait_send()
        for kind in (J_OWN_X, J_OWN_C, J_FWD_C):
            spread(kind, j).wait_send()


def tail(own, x_in, x_steps, w_o, w_fc, w_proj, b_o, gain, shift, b_fc, b_proj, group, kvs):
    steps, half, _ = own.shape
    batch = 2 * half
    rows = steps * half
    pair = rows // 2
    d_model = w_o.shape[1]
    chunks = d_model // CHUNK
    ff_own = w_fc.shape[1] // 2
    assert ff_own == d_model and steps == 4 and kvs == 2
    head_cols = group * LANES
    vm = pl.BlockSpec(memory_space=pltpu.VMEM)
    hbm = pl.BlockSpec(memory_space=pl.ANY)
    cfg = (steps, batch, group, chunks, kvs)
    tiles = lambda vec: vec.reshape(-1, LANES)
    scratch = [
        pltpu.VMEM((steps, half, head_cols), F32),
        pltpu.VMEM((steps, half, head_cols), F32),
        pltpu.VMEM((steps, half, LANES), F32),
        pltpu.VMEM((steps, half, LANES), F32),
        pltpu.VMEM((steps, half, head_cols), F32),
        pltpu.VMEM((steps, half, head_cols), F32),
        pltpu.VMEM((steps, half, LANES), F32),
        pltpu.VMEM((steps, half, LANES), F32),
        pltpu.VMEM((rows, head_cols), BF16),
        pltpu.VMEM((chunks, rows, CHUNK), F32),
        pltpu.VMEM((chunks, pair, CHUNK), F32),
        pltpu.VMEM((chunks, pair, CHUNK), F32),
        pltpu.VMEM((chunks, pair, CHUNK), F32),
        pltpu.VMEM((2, half, d_model), BF16),
        pltpu.VMEM((pair, d_model), F32),
        pltpu.VMEM((rows, d_model), F32),
        pltpu.VMEM((rows, d_model), BF16),
        pltpu.VMEM((RING, d_model, CHUNK), BF16),
        pltpu.VMEM((rows, ff_own), BF16),
        pltpu.VMEM((chunks, rows, CHUNK), F32),
        pltpu.VMEM((chunks, pair, CHUNK), F32),
        pltpu.VMEM((chunks, pair, CHUNK), F32),
        pltpu.VMEM((chunks, pair, CHUNK), F32),
        pltpu.VMEM((chunks, steps, batch, CHUNK), F32),
        pltpu.VMEM((d_model // LANES, LANES), F32),
        pltpu.VMEM((2 * ff_own // LANES, LANES), F32),
        pltpu.VMEM((d_model // LANES, LANES), F32),
        pltpu.SemaphoreType.DMA((6,)),
        pltpu.SemaphoreType.DMA((6,)),
        pltpu.SemaphoreType.DMA((7, chunks)),
        pltpu.SemaphoreType.DMA((7, chunks)),
        pltpu.SemaphoreType.DMA((4,)),
        pltpu.SemaphoreType.DMA((chunks,)),
        pltpu.SemaphoreType.DMA,
        pltpu.SemaphoreType.DMA((RING,)),
    ]
    return pl.pallas_call(
        functools.partial(tail_kernel, cfg),
        out_shape=jax.ShapeDtypeStruct((steps, batch, d_model), BF16),
        in_specs=[hbm] * 6 + [vm] * 5,
        out_specs=vm,
        scratch_shapes=scratch,
        compiler_params=pltpu.CompilerParams(collective_id=0, has_side_effects=True, vmem_limit_bytes=VMEM_CAP),
        cost_estimate=pl.CostEstimate(flops=2 * rows * d_model * (head_cols + 2 * ff_own), bytes_accessed=100_000_000, transcendentals=0),
        name="tail",
    )(own, x_in, x_steps, w_o, w_fc, w_proj, tiles(b_o), tiles(gain), tiles(shift), tiles(b_fc), tiles(b_proj))


def solution(mesh):
    sq_size = mesh.shape["sq"]
    act_spec = P(None, "dp", None)
    cache_spec = P("dp", "sq", "tp", None)
    col_spec = P(None, "tp")
    row_spec = P("tp", None)
    vec_spec = P("tp")
    rep_spec = P(None)
    in_specs = (act_spec, P("dp"), cache_spec, cache_spec, col_spec, vec_spec, col_spec, vec_spec,
                col_spec, vec_spec, row_spec, rep_spec, rep_spec, rep_spec, rep_spec, rep_spec,
                col_spec, vec_spec, row_spec, rep_spec)
    out_specs = (act_spec, cache_spec, cache_spec)

    def per_device(x_steps, positions, key_buf, val_buf, w_q, b_q, w_k, b_k, w_v, b_v, w_o, b_o,
                   ln1_gain, ln1_bias, ln2_gain, ln2_bias, w_fc, b_fc, w_proj, b_proj):
        steps, batch, d_model = x_steps.shape
        slots_local, kvs, dim = key_buf.shape[1], key_buf.shape[2], key_buf.shape[3]
        slots = slots_local * sq_size
        group = w_q.shape[1] // (kvs * dim)
        cur_pos = positions[None, :] + jnp.arange(steps, dtype=jnp.int32)[:, None]
        cos_t, sin_t = rope_tables(cur_pos, dim)
        q_rows, k_new, v_new = front(x_steps, ln1_gain, ln1_bias, cos_t, sin_t, b_q, b_k, b_v, w_q, w_k, w_v, kvs)
        k_rows = key_buf.reshape(batch, slots_local * kvs, dim)
        v_rows = val_buf.reshape(batch, slots_local * kvs, dim)
        caches = (positions, q_rows, k_new, v_new, k_rows, v_rows, steps, kvs, group, slots)
        k_out, v_out, for_peer = attend(*caches)
        from_peer = lax.ppermute(for_peer, "sq", [(d, d ^ 2) for d in range(sq_size)])
        k_out, v_out, own = attend(*caches, handed=(k_out, v_out))
        ys = tail(own, from_peer, x_steps, w_o, w_fc, w_proj, b_o, ln2_gain, ln2_bias, b_fc, b_proj, group, kvs)
        return ys, k_out.reshape(key_buf.shape), v_out.reshape(val_buf.shape)

    return jax.shard_map(per_device, mesh=mesh, in_specs=in_specs, out_specs=out_specs, check_vma=False)
```

```python
import functools
import math

import jax
import jax.numpy as jnp
from jax import lax
from jax.experimental import pallas as pl
from jax.experimental.pallas import tpu as pltpu
from jax.sharding import PartitionSpec as P

ROPE_BASE = 1000000.0
LN_EPS = 1e-5
NEG_BIG = -1e30
NEG_HALF = -1e29
LOG2E = 1.4426950408889634
VMEM_CAP = 67_043_328
F32 = jnp.float32
BF16 = jnp.bfloat16
LANES = 128


COLS = 256

def front_kernel(cfg, pos_ref, x_hbm, freq_ref, gain_ref, shift_ref, bq_ref, bk_ref, bv_ref, wq_hbm, wk_hbm, wv_hbm,
                 q_out, kn_out, vn_out, x_buf, hid, w_buf, mine, theirs, pos_rows, q_rows, kn_rows, vn_rows, bias_q,
                 sem, x_sem, send, recv):
    steps, kvs, group = cfg
    batch, d_model = x_buf.shape[1], x_buf.shape[2]
    head_cols = group * LANES
    per_row = group * kvs * steps
    sq = lax.axis_index("sq")
    c = sq % 2
    sib = {"sq": (sq // 2) * 2 + 1 - c}

    x_copies = [pltpu.make_async_copy(x_hbm.at[s], x_buf.at[s], x_sem.at[s]) for s in range(steps)]
    for copy in x_copies:
        copy.start()
    head_at = pl.multiple_of(c * LANES, LANES)
    pieces = []
    for at in range(0, head_cols, COLS):
        width = min(COLS, head_cols - at)
        pieces.append((wq_hbm.at[:, pl.ds(pl.multiple_of(c * head_cols + at, LANES), width)], at, width))
    pieces.append((wk_hbm.at[:, pl.ds(head_at, LANES)], head_cols, LANES))
    pieces.append((wv_hbm.at[:, pl.ds(head_at, LANES)], head_cols + LANES, LANES))
    w_copies = [pltpu.make_async_copy(src, w_buf.at[:, at:at + width], sem.at[n]) for n, (src, at, width) in enumerate(pieces)]
    for copy in w_copies:
        copy.start()

    barrier = pltpu.get_barrier_semaphore()
    pl.semaphore_signal(barrier, inc=1, device_id=sib, device_id_type=pl.DeviceIdType.MESH)
    pl.semaphore_wait(barrier, 1)

    for b in range(batch):
        pos_rows[b:b + 1, :] = jnp.full((1, LANES), pos_ref[b], jnp.int32).astype(F32)
    half = LANES // 2
    where = pos_rows[:, :half]
    angle = jnp.concatenate([where + float(s) for s in range(steps)], axis=0) * freq_ref[...]
    cos, sin = jnp.cos(angle), jnp.sin(angle)
    cos_full = jnp.concatenate([cos, cos], axis=-1)
    sin_full = jnp.concatenate([-sin, sin], axis=-1)

    bias_q[...] = bq_ref[...].astype(F32)
    gain = gain_ref[...].astype(F32)
    shift = shift_ref[...].astype(F32)
    for s in range(steps):
        x_copies[s].wait()
        wide = x_buf[s].astype(F32)
        mean = jnp.mean(wide, axis=-1, keepdims=True)
        cent = wide - mean
        rstd = lax.rsqrt(jnp.mean(cent * cent, axis=-1, keepdims=True) + LN_EPS)
        for n in range(d_model // LANES):
            cols = slice(n * LANES, (n + 1) * LANES)
            hid[s * batch:(s + 1) * batch, cols] = (cent[:, cols] * rstd * gain[n:n + 1, :] + shift[n:n + 1, :]).astype(BF16)

    def rotate(vec):
        return (vec * cos_full + pltpu.roll(vec, half, 1) * sin_full).astype(BF16).astype(F32)

    def swap(n):
        return pltpu.make_async_remote_copy(src_ref=mine.at[n], dst_ref=theirs.at[n], send_sem=send.at[n], recv_sem=recv.at[n],
                                            device_id=sib, device_id_type=pl.DeviceIdType.MESH)

    def place(n, core, block):
        for s in range(steps):
            rows = block[s * batch:(s + 1) * batch, :]
            if n < group:
                q_rows[pl.ds(n * kvs * steps + core * steps + s, batch, stride=per_row), :] = rows
            elif n == group:
                kn_rows[pl.ds(s * kvs + core, batch, stride=16), :] = rows
            else:
                vn_rows[pl.ds(s * kvs + core, batch, stride=16), :] = rows

    kn_rows[...] = jnp.zeros_like(kn_rows)
    vn_rows[...] = jnp.zeros_like(vn_rows)
    kv_bias = [jnp.where(c == 0, ref[0:1, :].astype(F32), ref[1:2, :].astype(F32)) for ref in (bk_ref, bv_ref)]
    total = group + 2
    per = COLS // LANES
    done = 0
    for first in range(0, total, per):
        count = min(per, total - first)
        upto = (first + count) * LANES
        while done < len(pieces) and pieces[done][1] < upto:
            w_copies[done].wait()
            done += 1
        block = jnp.dot(hid[...], w_buf[:, first * LANES:upto], preferred_element_type=F32)
        for n in range(first, first + count):
            bias = bias_q[pl.ds(c * group + n, 1), :] if n < group else kv_bias[n - group]
            vec = (block[:, (n - first) * LANES:(n - first + 1) * LANES] + bias).astype(BF16).astype(F32)
            mine[n] = rotate(vec) if n <= group else vec
            swap(n).start()
            place(n, c, mine.at[n])
    for n in range(total):
        swap(n).wait_recv()
        place(n, 1 - c, theirs.at[n])

    kn_out[...] = kn_rows[...].reshape(kn_out.shape).astype(BF16)
    vn_out[...] = vn_rows[...].reshape(vn_out.shape).astype(BF16)

    @pl.loop(0, batch)
    def _(b):
        q_out[b] = q_rows[pl.ds(pl.multiple_of(b * per_row, 8), per_row), :].astype(BF16)

    for n in range(total):
        swap(n).wait_send()


def front(positions, x_steps, gain, shift, b_q, b_k, b_v, w_q, w_k, w_v, kvs):
    steps, batch, d_model = x_steps.shape
    heads = w_q.shape[1] // LANES
    group = heads // kvs
    rows = group * kvs * steps
    assert kvs == 2
    inv_freq = jnp.power(F32(ROPE_BASE), -2.0 * jnp.arange(LANES // 2, dtype=F32) / LANES).reshape(1, -1)
    vm = pl.BlockSpec(memory_space=pltpu.VMEM)
    hbm = pl.BlockSpec(memory_space=pl.ANY)
    tiles = lambda vec: vec.reshape(-1, LANES)
    return pl.pallas_call(
        functools.partial(front_kernel, (steps, kvs, group)),
        out_shape=[
            jax.ShapeDtypeStruct((batch, rows, LANES), BF16),
            jax.ShapeDtypeStruct((batch, 16, LANES), BF16),
            jax.ShapeDtypeStruct((batch, 16, LANES), BF16),
        ],
        in_specs=[pl.BlockSpec(memory_space=pltpu.SMEM), hbm] + [vm] * 6 + [hbm] * 3,
        out_specs=[vm] * 3,
        scratch_shapes=[
            pltpu.VMEM((steps, batch, d_model), BF16),
            pltpu.VMEM((steps * batch, d_model), BF16),
            pltpu.VMEM((d_model, (group + 2) * LANES), BF16),
            pltpu.VMEM((group + 2, steps * batch, LANES), F32),
            pltpu.VMEM((group + 2, steps * batch, LANES), F32),
            pltpu.VMEM((batch, LANES), F32),
            pltpu.VMEM((batch * rows, LANES), F32),
            pltpu.VMEM((batch * 16, LANES), F32),
            pltpu.VMEM((batch * 16, LANES), F32),
            pltpu.VMEM((heads, LANES), F32),
            pltpu.SemaphoreType.DMA((group + 2,)),
            pltpu.SemaphoreType.DMA((steps,)),
            pltpu.SemaphoreType.DMA((group + 2,)),
            pltpu.SemaphoreType.DMA((group + 2,)),
        ],
        compiler_params=pltpu.CompilerParams(collective_id=1, has_side_effects=True, vmem_limit_bytes=VMEM_CAP),
        cost_estimate=pl.CostEstimate(flops=steps * batch * d_model * (w_q.shape[1] + 2 * w_k.shape[1]),
                                      bytes_accessed=d_model * (w_q.shape[1] + 2 * w_k.shape[1]), transcendentals=0),
        name="front",
    )(positions, x_steps, inv_freq, tiles(gain), tiles(shift), tiles(b_q), tiles(b_k), tiles(b_v), w_q, w_k, w_v)


PER = 2
DEPTH = 8
AHEAD = 4

def attend_kernel(cfg, pos_ref, q_hbm, kn_hbm, vn_hbm, k_hbm, v_hbm, *refs):
    steps, kvs, group, slots, n_blocks, own_half = cfg
    (ko_hbm, vo_hbm, o_hbm, k_buf, v_buf, q_ref, kn_ref, vn_ref, o_tile, o_rows, stat_rows,
     k_in, v_in, k_up, v_up, small_in, o_up) = refs[2 if own_half else 0:]
    x = lax.axis_index("sq") // 2
    base = (x if own_half else 1 - x) * (n_blocks * PER)
    lse_cols = slice(kvs * group * LANES, (kvs * group + 1) * LANES)
    rows = k_hbm.shape[1]
    tile = steps * kvs
    per_row = group * tile
    first = lax.axis_index("sq") * (rows // kvs)
    coef = LANES ** -0.5 * LOG2E
    contract_last = (((1,), (1,)), ((), ()))
    blocks_per_tile = 8 // PER

    def seqs(i):
        return pl.ds(base + i * PER, PER)

    def fetch(i):
        slot = lax.rem(i, DEPTH)
        return (pltpu.make_async_copy(k_hbm.at[seqs(i)], k_buf.at[slot], k_in.at[slot]),
                pltpu.make_async_copy(v_hbm.at[seqs(i)], v_buf.at[slot], v_in.at[slot]))

    def put(i):
        slot = lax.rem(i, DEPTH)
        return (pltpu.make_async_copy(k_buf.at[slot], ko_hbm.at[seqs(i)], k_up.at[slot]),
                pltpu.make_async_copy(v_buf.at[slot], vo_hbm.at[seqs(i)], v_up.at[slot]))

    half_seqs = pl.ds(base, n_blocks * PER)
    small = [pltpu.make_async_copy(src.at[half_seqs], dst, small_in.at[n])
             for n, (src, dst) in enumerate(((q_hbm, q_ref), (kn_hbm, kn_ref), (vn_hbm, vn_ref)))]
    for copy in small:
        copy.start()
    for i in range(2):
        for copy in fetch(jnp.int32(i)):
            copy.start()

    def put_tile(t):
        return pltpu.make_async_copy(o_tile.at[t], o_hbm.at[:, pl.ds(pl.multiple_of(t * 8, 8), 8), :], o_up.at[t])

    sub = lax.broadcasted_iota(jnp.int32, (tile, rows), 0)
    lane = lax.broadcasted_iota(jnp.int32, (tile, rows), 1)
    sub2 = lax.broadcasted_iota(jnp.int32, (tile, 16), 0)
    lane2 = lax.broadcasted_iota(jnp.int32, (tile, 16), 1)
    new_step = lane2 // kvs
    new_ok = ((lane2 % kvs) == (sub2 // steps)) & (new_step <= sub2 % steps)
    stat_sub = lax.broadcasted_iota(jnp.int32, (tile, LANES), 0)
    stat_lane = lax.broadcasted_iota(jnp.int32, (tile, LANES), 1) - (stat_sub // steps) * group
    win_row = lax.broadcasted_iota(jnp.int32, (32, LANES), 0)

    def renew(i):
        slot_of = lax.rem(i, DEPTH)
        for one in range(PER):
            seq = i * PER + one
            goal = kvs * ((pos_ref[base + seq] & (slots - 1)) - first)
            goal = jnp.where(goal > kvs * (slots - steps), goal - kvs * slots, goal)
            start = pl.multiple_of(jnp.clip((goal >> 4) << 4, 0, rows - 32), 16)
            offset = win_row + (start - goal)
            for buf, new in ((k_buf, kn_ref), (v_buf, vn_ref)):
                fresh = new[seq].astype(F32)
                window = buf[slot_of, one, pl.ds(start, 32), :].astype(F32)
                for r in range(tile):
                    window = jnp.where(offset == r, fresh[r:r + 1, :], window)
                buf[slot_of, one, pl.ds(start, 32), :] = window.astype(BF16)

    @pl.loop(0, n_blocks)
    def _(i):
        slot_now = lax.rem(i, DEPTH)

        @pl.when(i >= 1)
        def _():
            renew(i - 1)

        @pl.when(i >= AHEAD)
        def _():
            for copy in put(i - AHEAD):
                copy.wait()

        @pl.when(i == 0)
        def _():
            for later in range(2, AHEAD):
                for copy in fetch(jnp.int32(later)):
                    copy.start()

        @pl.when(i + AHEAD < n_blocks)
        def _():
            for copy in fetch(i + AHEAD):
                copy.start()

        @pl.when(i >= 1)
        def _():
            for copy in put(i - 1):
                copy.start()

        @pl.when((i >= 1) & (lax.rem(i, blocks_per_tile) == 0))
        def _():
            put_tile(i // blocks_per_tile - 1).start()

        k_copy, v_copy = fetch(i)
        @pl.when(i == 0)
        def _():
            for copy in small:
                copy.wait()

        k_copy.wait()
        v_copy.wait()
        state = []
        for one in range(PER):
            seq = i * PER + one
            pos = pos_ref[base + seq]
            q = q_ref[seq]
            raw = lax.dot_general(q, k_buf[slot_now, one], contract_last, preferred_element_type=F32)
            raw2 = lax.dot_general(q, kn_ref[seq], contract_last, preferred_element_type=F32)
            state.append((seq, pos, raw, raw2))
        soft = []
        for seq, pos, raw, raw2 in state:
            slot = first + (lane >> 1)
            ahead = (slot - pos) & (slots - 1)
            ok = ((lane & 1) == (sub >> 2)) & (slot < pos) & (ahead > (sub & 3))
            bias = jnp.where(ok, 0.0, NEG_BIG).astype(F32)
            new_slot = ((pos + new_step) & (slots - 1)) - first
            here = (new_slot >= 0) & (new_slot < rows // kvs)
            bias2 = jnp.where(new_ok & here, 0.0, NEG_BIG).astype(F32)
            score = raw.reshape(group, tile, rows) * coef + bias[None]
            score2 = raw2.reshape(group, tile, 16) * coef + bias2[None]
            top = jnp.maximum(jnp.max(score, axis=-1, keepdims=True), jnp.max(score2, axis=-1, keepdims=True))
            top = jnp.maximum(top, NEG_HALF)
            w = jnp.exp2(score - top)
            w2 = jnp.exp2(score2 - top)
            total = jnp.sum(w, axis=-1, keepdims=True) + jnp.sum(w2, axis=-1, keepdims=True)
            soft.append((top, total, w.reshape(per_row, rows).astype(BF16), w2.reshape(per_row, 16).astype(BF16)))
        for one in range(PER):
            seq, pos = state[one][:2]
            top, total, w, w2 = soft[one]
            out = jnp.dot(w, v_buf[slot_now, one], preferred_element_type=F32)
            out = out + jnp.dot(w2, vn_ref[seq], preferred_element_type=F32)
            some = total > 0.0
            safe = jnp.where(some, total, 1.0)
            lse = jnp.where(some, top + jnp.log2(safe), NEG_BIG)
            out = out.reshape(group, tile, LANES) * (1.0 / safe)
            stats = jnp.zeros((tile, LANES), F32)
            for n in range(group):
                stats = jnp.where(stat_lane == n, lse[n], stats)
            seat = lax.rem(i, blocks_per_tile) * PER + one
            o_rows[pl.ds(pl.multiple_of(seat * per_row, 8), per_row), :] = out.reshape(per_row, LANES)
            stat_rows[pl.ds(pl.multiple_of(seat * tile, 8), tile), :] = stats
        @pl.when(lax.rem(i, blocks_per_tile) == blocks_per_tile - 1)
        def _():
            t = i // blocks_per_tile
            for s in range(steps):
                o_tile[t, s, :, lse_cols] = sum(stat_rows[pl.ds(h * steps + s, 8, stride=tile), :] for h in range(kvs))
                for h in range(kvs):
                    for n in range(group):
                        col = (h * group + n) * LANES
                        o_tile[t, s, :, col:col + LANES] = o_rows[pl.ds(n * tile + h * steps + s, 8, stride=per_row), :]

    renew(jnp.int32(n_blocks - 1))
    for copy in put(n_blocks - 1):
        copy.start()
    tiles = n_blocks // blocks_per_tile
    put_tile(tiles - 1).start()
    for j in range(AHEAD):
        for copy in put(n_blocks - AHEAD + j):
            copy.wait()
    for t in range(tiles):
        put_tile(t).wait()


def attend(positions, q, k_new, v_new, k_rows, v_rows, steps, kvs, group, slots, handed=()):
    batch, rows, dim = k_rows.shape
    half = batch // 2
    hbm = pl.BlockSpec(memory_space=pl.ANY)
    return pl.pallas_call(
        functools.partial(attend_kernel, (steps, kvs, group, slots, half // PER, bool(handed))),
        in_specs=[pl.BlockSpec(memory_space=pltpu.SMEM)] + [hbm] * (5 + len(handed)),
        out_specs=[hbm, hbm, hbm],
        out_shape=[
            jax.ShapeDtypeStruct(k_rows.shape, BF16),
            jax.ShapeDtypeStruct(v_rows.shape, BF16),
            jax.ShapeDtypeStruct((steps, half, (kvs * group + 1) * dim), F32),
        ],
        input_output_aliases={6: 0, 7: 1} if handed else {},
        scratch_shapes=[
            pltpu.VMEM((DEPTH, PER, rows, dim), BF16),
            pltpu.VMEM((DEPTH, PER, rows, dim), BF16),
            pltpu.VMEM((half, q.shape[1], dim), BF16),
            pltpu.VMEM((half, k_new.shape[1], dim), BF16),
            pltpu.VMEM((half, v_new.shape[1], dim), BF16),
            pltpu.VMEM((half // 8, steps, 8, (kvs * group + 1) * dim), F32),
            pltpu.VMEM((8 * q.shape[1], dim), F32),
            pltpu.VMEM((8 * steps * kvs, dim), F32),
            pltpu.SemaphoreType.DMA((DEPTH,)),
            pltpu.SemaphoreType.DMA((DEPTH,)),
            pltpu.SemaphoreType.DMA((DEPTH,)),
            pltpu.SemaphoreType.DMA((DEPTH,)),
            pltpu.SemaphoreType.DMA((3,)),
            pltpu.SemaphoreType.DMA((half // 8,)),
        ],
        compiler_params=pltpu.CompilerParams(vmem_limit_bytes=VMEM_CAP),
        cost_estimate=pl.CostEstimate(flops=20_000_000_000, bytes_accessed=4 * batch * rows * dim,
                                      transcendentals=half * rows * q.shape[1]),
        name="attend_own" if handed else "attend_peer",
    )(positions, q, k_new, v_new, k_rows, v_rows, *handed)


CHUNK = 512
PIECE = 256
RING = 9
WO_SLOTS = 3
(C_OWN_O, C_X_O, C_OWN_E, C_X_E, C_HID_A, C_HID_B) = range(6)
(W_CORE, W_Y, J_CORE, J_Y, J_OWN_X, J_OWN_C, J_FWD_C) = range(7)


def tail_kernel(cfg, own_hbm, xin_hbm, x_hbm, wo_hbm, wfc_hbm, wproj_hbm, bo_ref, gain_ref, shift_ref, bfc_ref, bproj_ref,
                y_ref,
                my_own, my_x, my_own_e, my_x_e, sib_own, sib_x, sib_own_e, sib_x_e, a_buf, w_part, w_core, w_half, w_y, x_buf, x_mid, hid, hid_b,
                ring, g_buf, p_part, p_core, p_half, p_y, y_all, bo_rows, bfc_rows, bproj_rows,
                send_a, recv_a, send_j, recv_j, local_sem, wo_sem, x_sem, ring_sem):
    steps, batch, group, chunks, kvs = cfg
    half = batch // 2
    pair = steps // 2 * half
    head_cols = group * LANES
    ff_own = wfc_hbm.shape[1] // 2
    pieces = chunks * CHUNK // PIECE
    per = CHUNK // PIECE
    y = lax.axis_index("tp")
    sq = lax.axis_index("sq")
    x, c = sq // 2, sq % 2
    sib = {"sq": x * 2 + 1 - c}
    xpeer = {"sq": (1 - x) * 2 + c}
    ypeer = {"tp": 1 - y}
    MESH = pl.DeviceIdType.MESH

    def chunk_cols(j):
        return pl.ds(pl.multiple_of(j * CHUNK, CHUNK), CHUNK)

    def load_item(item, slot):
        @pl.when(item < chunks)
        def _():
            col = pl.multiple_of(c * ff_own + item * CHUNK, CHUNK)
            pltpu.make_async_copy(wfc_hbm.at[:, pl.ds(col, CHUNK)], ring.at[slot], ring_sem.at[slot]).start()

        @pl.when(item >= chunks)
        def _():
            row = pl.multiple_of(c * ff_own, CHUNK)
            pltpu.make_async_copy(wproj_hbm.at[pl.ds(row, ff_own), chunk_cols(item - chunks)], ring.at[slot], ring_sem.at[slot]).start()

    def wait_item(slot):
        pltpu.make_async_copy(wfc_hbm.at[:, pl.ds(0, CHUNK)], ring.at[slot], ring_sem.at[slot]).wait()

    wo_rows = pl.ds(pl.multiple_of(c * head_cols, LANES), head_cols)
    per_slot = ring.shape[1] // head_cols

    def wo_place(j):
        return ring.at[j // per_slot, pl.ds(pl.multiple_of(lax.rem(j, per_slot) * head_cols, LANES), head_cols), :]

    def wo_copy(j):
        return pltpu.make_async_copy(wo_hbm.at[wo_rows, chunk_cols(j)], wo_place(j), wo_sem.at[j])

    def slot_of(item):
        return lax.rem(item + WO_SLOTS, RING)

    my_cols = pl.ds(pl.multiple_of(c * head_cols, LANES), head_cols)
    stat_cols = slice(kvs * head_cols, kvs * head_cols + LANES)
    locals_ = [pltpu.make_async_copy(src, dst, local_sem.at[n]) for n, (src, dst) in enumerate((
        (own_hbm.at[:, :, stat_cols], my_own_e), (xin_hbm.at[:, :, stat_cols], my_x_e),
        (own_hbm.at[:, :, my_cols], my_own), (xin_hbm.at[:, :, my_cols], my_x)))]
    for copy in locals_:
        copy.start()
    for j in range(chunks):
        wo_copy(jnp.int32(j)).start()
    x_copy = pltpu.make_async_copy(x_hbm.at[pl.ds(2 * c, 2), pl.ds(pl.multiple_of(x * half, 8), half), :], x_buf, x_sem)
    x_copy.start()
    barrier = pltpu.get_barrier_semaphore()
    for who in (sib, xpeer, ypeer):
        pl.semaphore_signal(barrier, inc=1, device_id=who, device_id_type=MESH)
    pl.semaphore_wait(barrier, 3)

    def remote(src, dst, kind, who):
        return pltpu.make_async_remote_copy(src_ref=src, dst_ref=dst, send_sem=send_a.at[kind], recv_sem=recv_a.at[kind],
                                            device_id=who, device_id_type=MESH)

    sib_cols = pl.ds(pl.multiple_of((1 - c) * head_cols, LANES), head_cols)
    swaps = [remote(own_hbm.at[:, :, stat_cols], sib_own_e, C_OWN_E, sib), remote(xin_hbm.at[:, :, stat_cols], sib_x_e, C_X_E, sib),
             remote(own_hbm.at[:, :, sib_cols], sib_own, C_OWN_O, sib), remote(xin_hbm.at[:, :, sib_cols], sib_x, C_X_O, sib)]
    for copy in swaps:
        copy.start()
    bo_rows[...] = bo_ref[...].astype(F32)
    bfc_rows[...] = bfc_ref[...].astype(F32)
    bproj_rows[...] = bproj_ref[...].astype(F32)

    def flat(block):
        return block.reshape(steps * half, LANES)

    def my_lanes(stat):
        stat = flat(stat)
        return jnp.where(c == 0, stat, pltpu.roll(stat, LANES - group, 1))

    for copy in locals_:
        copy.wait()
    swaps[0].wait_recv()
    swaps[1].wait_recv()
    logs = [my_lanes(my_own_e[...]), my_lanes(sib_own_e[...]), my_lanes(my_x_e[...]), my_lanes(sib_x_e[...])]
    top = functools.reduce(jnp.maximum, logs)
    shares = [jnp.exp2(e - top) for e in logs]
    inv = 1.0 / sum(shares)
    shares = [w * inv for w in shares]
    swaps[2].wait_recv()
    swaps[3].wait_recv()
    for i in range(group):
        cols = slice(i * LANES, (i + 1) * LANES)
        parts = [part[:, :, cols] for part in (my_own, sib_own, my_x, sib_x)]
        a_buf[:, cols] = sum(w[:, i:i + 1] * flat(part) for w, part in zip(shares, parts)).astype(BF16)

    def jcopy(src, dst, kind, j, who):
        return pltpu.make_async_remote_copy(src_ref=src, dst_ref=dst, send_sem=send_j.at[kind, j], recv_sem=recv_j.at[kind, j],
                                            device_id=who, device_id_type=MESH)

    def pair_rows(core):
        return pl.ds(pl.multiple_of(core * pair, 8), pair)

    def to_core(part, inbox, kind, j):
        return jcopy(part.at[j, pair_rows(1 - c), :], inbox.at[j], kind, j, sib)

    def to_y(total, inbox, kind, j):
        return jcopy(total.at[j], inbox.at[j], kind, j, ypeer)

    def core_sum(part, inbox, total, inbox_y, kind, kind_y, j):
        to_core(part, inbox, kind, j).wait_recv()
        total[j] = part[j, pair_rows(c), :] + inbox[j]
        to_y(total, inbox_y, kind_y, j).start()

    def bias_of(rows, j, width):
        n = width // LANES
        return jnp.concatenate([rows[pl.ds(j * n + e, 1), :] for e in range(n)], axis=-1)

    def piece_cols(u):
        return pl.ds(pl.multiple_of(u * PIECE, PIECE), PIECE)

    def send_product(product, part, inbox, kind, j):
        for e in range(per):
            part[j * per + e] = product[:, e * PIECE:(e + 1) * PIECE]
        for e in range(per):
            to_core(part, inbox, kind, j * per + e).start()

    def y_sum(total, inbox):
        low = jnp.where(y == 0, total, inbox)
        high = jnp.where(y == 0, inbox, total)
        return low + high

    def stage(it, lag, body):
        u = it - lag

        @pl.when((u >= 0) & (u < pieces))
        def _():
            body(u)

    def product_stage(it, body):
        @pl.when((it < pieces) & (lax.rem(it, per) == 0))
        def _():
            body(it // per)

    def o_product(j):
        wo_copy(j).wait()
        product = jnp.dot(a_buf[...], wo_place(j)[...], preferred_element_type=F32)
        send_product(product, w_part, w_core, W_CORE, j)

    def o_core_sum(j):
        core_sum(w_part, w_core, w_half, w_y, W_CORE, W_Y, j)

    for k in range(RING - WO_SLOTS):
        load_item(jnp.int32(k), slot_of(k))

    @pl.loop(0, pieces + 6)
    def _(it):
        product_stage(it, o_product)
        stage(it, 6, o_core_sum)

    for k in range(RING - WO_SLOTS, RING):
        load_item(jnp.int32(k), slot_of(k))
    x_copy.wait()

    @pl.loop(0, pieces)
    def _(u):
        cols = piece_cols(u)
        to_y(w_half, w_y, W_Y, u).wait_recv()
        x_in = x_buf[:, :, cols].astype(F32).reshape(pair, PIECE)
        x_mid[:, cols] = (x_in + y_sum(w_half[u], w_y[u]) + bias_of(bo_rows, u, PIECE)).astype(BF16).astype(F32)

    gain = gain_ref[...].astype(F32)
    shift = shift_ref[...].astype(F32)
    d_model = x_mid.shape[1]
    hid_copies = []
    for part in range(2):
        src = slice(part * half, (part + 1) * half)
        dst = pl.ds(pl.multiple_of(c * pair + part * half, 8), half)
        rows = x_mid[src, :]
        mean = jnp.mean(rows, axis=-1, keepdims=True)
        cent = rows - mean
        rstd = lax.rsqrt(jnp.mean(cent * cent, axis=-1, keepdims=True) + LN_EPS)
        for n in range(d_model // LANES):
            cols = slice(n * LANES, (n + 1) * LANES)
            hid[dst, cols] = (cent[:, cols] * rstd * gain[n:n + 1, :] + shift[n:n + 1, :]).astype(BF16).astype(F32)
        copy = remote(hid.at[dst, :], hid.at[dst, :], (C_HID_A, C_HID_B)[part], sib)
        copy.start()
        hid_copies.append(copy)
    for copy in hid_copies:
        copy.wait_recv()
    hid_b[...] = hid[...].astype(BF16)

    @pl.loop(0, chunks)
    def _(j):
        slot = slot_of(j)
        wait_item(slot)
        pre = jnp.dot(hid_b[...], ring[slot], preferred_element_type=F32) + bias_of(bfc_rows, c * chunks + j, CHUNK)
        cube = pre * pre * pre
        act = 0.5 * pre * (1.0 + jnp.tanh(math.sqrt(2.0 / math.pi) * (pre + 0.044715 * cube)))
        g_buf[:, chunk_cols(j)] = act.astype(BF16)
        load_item(j + RING, slot)

    def block(j, core, xx):
        return y_all.at[j, pl.ds(2 * core, 2), pl.ds(pl.multiple_of(xx * half, 8), half), :]

    def spread(kind, j):
        ref, who = {J_OWN_X: (block(j, c, x), xpeer), J_OWN_C: (block(j, c, x), sib), J_FWD_C: (block(j, c, 1 - x), sib)}[kind]
        return jcopy(ref, ref, kind, j, who)

    def do_product(j):
        item = chunks + j
        slot = slot_of(item)
        wait_item(slot)
        product = jnp.dot(g_buf[...], ring[slot], preferred_element_type=F32)
        send_product(product, p_part, p_core, J_CORE, j)

        @pl.when(item + RING < 2 * chunks)
        def _():
            load_item(item + RING, slot)

    def do_core_sum(j):
        core_sum(p_part, p_core, p_half, p_y, J_CORE, J_Y, j)

    def do_y_sum(j):
        to_y(p_half, p_y, J_Y, j).wait_recv()
        full = x_mid[:, piece_cols(j)] + y_sum(p_half[j], p_y[j]) + bias_of(bproj_rows, j, PIECE)
        y_all[j, pl.ds(2 * c, 2), pl.ds(pl.multiple_of(x * half, 8), half), :] = full.astype(BF16).astype(F32).reshape(2, half, PIECE)
        spread(J_OWN_X, j).start()
        spread(J_OWN_C, j).start()

    def do_forward(j):
        spread(J_OWN_X, j).wait_recv()
        spread(J_FWD_C, j).start()

    def do_store(j):
        spread(J_OWN_C, j).wait_recv()
        spread(J_FWD_C, j).wait_recv()
        y_ref[:, :, piece_cols(j)] = y_all[j].astype(BF16)

    @pl.loop(0, pieces + 13)
    def _(it):
        product_stage(it, do_product)
        stage(it, 2, do_core_sum)
        stage(it, 7, do_y_sum)
        stage(it, 11, do_forward)
        stage(it, 13, do_store)

    for copy in swaps + hid_copies:
        copy.wait_send()

    @pl.loop(0, pieces)
    def _(j):
        to_core(w_part, w_core, W_CORE, j).wait_send()
        to_y(w_half, w_y, W_Y, j).wait_send()
        to_core(p_part, p_core, J_CORE, j).wait_send()
        to_y(p_half, p_y, J_Y, j).wait_send()
        for kind in (J_OWN_X, J_OWN_C, J_FWD_C):
            spread(kind, j).wait_send()


def tail(own, x_in, x_steps, w_o, w_fc, w_proj, b_o, gain, shift, b_fc, b_proj, group, kvs):
    steps, half, _ = own.shape
    batch = 2 * half
    rows = steps * half
    pair = rows // 2
    d_model = w_o.shape[1]
    chunks = d_model // CHUNK
    pieces = d_model // PIECE
    ff_own = w_fc.shape[1] // 2
    assert ff_own == d_model and steps == 4 and kvs == 2
    head_cols = group * LANES
    vm = pl.BlockSpec(memory_space=pltpu.VMEM)
    hbm = pl.BlockSpec(memory_space=pl.ANY)
    cfg = (steps, batch, group, chunks, kvs)
    tiles = lambda vec: vec.reshape(-1, LANES)
    scratch = [
        pltpu.VMEM((steps, half, head_cols), F32),
        pltpu.VMEM((steps, half, head_cols), F32),
        pltpu.VMEM((steps, half, LANES), F32),
        pltpu.VMEM((steps, half, LANES), F32),
        pltpu.VMEM((steps, half, head_cols), F32),
        pltpu.VMEM((steps, half, head_cols), F32),
        pltpu.VMEM((steps, half, LANES), F32),
        pltpu.VMEM((steps, half, LANES), F32),
        pltpu.VMEM((rows, head_cols), BF16),
        pltpu.VMEM((pieces, rows, PIECE), F32),
        pltpu.VMEM((pieces, pair, PIECE), F32),
        pltpu.VMEM((pieces, pair, PIECE), F32),
        pltpu.VMEM((pieces, pair, PIECE), F32),
        pltpu.VMEM((2, half, d_model), BF16),
        pltpu.VMEM((pair, d_model), F32),
        pltpu.VMEM((rows, d_model), F32),
        pltpu.VMEM((rows, d_model), BF16),
        pltpu.VMEM((RING, d_model, CHUNK), BF16),
        pltpu.VMEM((rows, ff_own), BF16),
        pltpu.VMEM((pieces, rows, PIECE), F32),
        pltpu.VMEM((pieces, pair, PIECE), F32),
        pltpu.VMEM((pieces, pair, PIECE), F32),
        pltpu.VMEM((pieces, pair, PIECE), F32),
        pltpu.VMEM((pieces, steps, batch, PIECE), F32),
        pltpu.VMEM((d_model // LANES, LANES), F32),
        pltpu.VMEM((2 * ff_own // LANES, LANES), F32),
        pltpu.VMEM((d_model // LANES, LANES), F32),
        pltpu.SemaphoreType.DMA((6,)),
        pltpu.SemaphoreType.DMA((6,)),
        pltpu.SemaphoreType.DMA((7, pieces)),
        pltpu.SemaphoreType.DMA((7, pieces)),
        pltpu.SemaphoreType.DMA((4,)),
        pltpu.SemaphoreType.DMA((chunks,)),
        pltpu.SemaphoreType.DMA,
        pltpu.SemaphoreType.DMA((RING,)),
    ]
    return pl.pallas_call(
        functools.partial(tail_kernel, cfg),
        out_shape=jax.ShapeDtypeStruct((steps, batch, d_model), BF16),
        in_specs=[hbm] * 6 + [vm] * 5,
        out_specs=vm,
        scratch_shapes=scratch,
        compiler_params=pltpu.CompilerParams(collective_id=0, has_side_effects=True, vmem_limit_bytes=VMEM_CAP),
        cost_estimate=pl.CostEstimate(flops=2 * rows * d_model * (head_cols + 2 * ff_own), bytes_accessed=100_000_000, transcendentals=0),
        name="tail",
    )(own, x_in, x_steps, w_o, w_fc, w_proj, tiles(b_o), tiles(gain), tiles(shift), tiles(b_fc), tiles(b_proj))


def solution(mesh):
    sq_size = mesh.shape["sq"]
    act_spec = P(None, "dp", None)
    cache_spec = P("dp", "sq", "tp", None)
    col_spec = P(None, "tp")
    row_spec = P("tp", None)
    vec_spec = P("tp")
    rep_spec = P(None)
    in_specs = (act_spec, P("dp"), cache_spec, cache_spec, col_spec, vec_spec, col_spec, vec_spec,
                col_spec, vec_spec, row_spec, rep_spec, rep_spec, rep_spec, rep_spec, rep_spec,
                col_spec, vec_spec, row_spec, rep_spec)
    out_specs = (act_spec, cache_spec, cache_spec)

    def per_device(x_steps, positions, key_buf, val_buf, w_q, b_q, w_k, b_k, w_v, b_v, w_o, b_o,
                   ln1_gain, ln1_bias, ln2_gain, ln2_bias, w_fc, b_fc, w_proj, b_proj):
        steps, batch, d_model = x_steps.shape
        slots_local, kvs, dim = key_buf.shape[1], key_buf.shape[2], key_buf.shape[3]
        slots = slots_local * sq_size
        group = w_q.shape[1] // (kvs * dim)
        q_rows, k_new, v_new = front(positions, x_steps, ln1_gain, ln1_bias, b_q, b_k, b_v, w_q, w_k, w_v, kvs)
        k_rows = key_buf.reshape(batch, slots_local * kvs, dim)
        v_rows = val_buf.reshape(batch, slots_local * kvs, dim)
        caches = (positions, q_rows, k_new, v_new, k_rows, v_rows, steps, kvs, group, slots)
        k_out, v_out, for_peer = attend(*caches)
        from_peer = lax.ppermute(for_peer, "sq", [(d, d ^ 2) for d in range(sq_size)])
        k_out, v_out, own = attend(*caches, handed=(k_out, v_out))
        ys = tail(own, from_peer, x_steps, w_o, w_fc, w_proj, b_o, ln2_gain, ln2_bias, b_fc, b_proj, group, kvs)
        return ys, k_out.reshape(key_buf.shape), v_out.reshape(val_buf.shape)

    return jax.shard_map(per_device, mesh=mesh, in_specs=in_specs, out_specs=out_specs, check_vma=False)
```

```python
import functools
import math

import jax
import jax.numpy as jnp
from jax import lax
from jax.experimental import pallas as pl
from jax.experimental.pallas import tpu as pltpu
from jax.sharding import PartitionSpec as P

ROPE_BASE = 1000000.0
LN_EPS = 1e-5
NEG_BIG = -1e30
NEG_HALF = -1e29
LOG2E = 1.4426950408889634
VMEM_CAP = 67_043_328
TAIL_VMEM = 64_900_000
F32 = jnp.float32
BF16 = jnp.bfloat16
LANES = 128


COLS = 384

def front_kernel(cfg, pos_ref, x_hbm, freq_ref, gain_ref, shift_ref, bq_ref, bk_ref, bv_ref, wq_hbm, wk_hbm, wv_hbm,
                 q_out, kn_out, vn_out, x_buf, hid, wq_buf, wkv_buf, mine, theirs, pos_rows, q_rows, kn_rows, vn_rows, bias_q,
                 sem, x_sem, send, recv):
    steps, kvs, group = cfg
    batch, d_model = x_buf.shape[1], x_buf.shape[2]
    head_cols = group * LANES
    per_row = group * kvs * steps
    sq = lax.axis_index("sq")
    c = sq % 2
    sib = {"sq": (sq // 2) * 2 + 1 - c}

    x_copies = [pltpu.make_async_copy(x_hbm.at[s], x_buf.at[s], x_sem.at[s]) for s in range(steps)]
    for copy in x_copies:
        copy.start()
    head_at = pl.multiple_of(c * LANES, LANES)
    n_q = head_cols // COLS
    w_copies = [pltpu.make_async_copy(wq_hbm.at[:, pl.ds(pl.multiple_of(c * head_cols + n * COLS, LANES), COLS)], wq_buf.at[n], sem.at[n])
                for n in range(n_q)]
    w_copies += [pltpu.make_async_copy(src.at[:, pl.ds(head_at, LANES)], wkv_buf.at[n], sem.at[n_q + n])
                 for n, src in enumerate((wk_hbm, wv_hbm))]
    for copy in w_copies:
        copy.start()

    barrier = pltpu.get_barrier_semaphore()
    pl.semaphore_signal(barrier, inc=1, device_id=sib, device_id_type=pl.DeviceIdType.MESH)
    pl.semaphore_wait(barrier, 1)

    for b in range(batch):
        pos_rows[b:b + 1, :] = jnp.full((1, LANES), pos_ref[b], jnp.int32).astype(F32)
    half = LANES // 2
    where = pos_rows[:, :half]
    angle = jnp.concatenate([where + float(s) for s in range(steps)], axis=0) * freq_ref[...]
    cos, sin = jnp.cos(angle), jnp.sin(angle)
    cos_full = jnp.concatenate([cos, cos], axis=-1)
    sin_full = jnp.concatenate([-sin, sin], axis=-1)

    bias_q[...] = bq_ref[...].astype(F32)
    gain = gain_ref[...].astype(F32)
    shift = shift_ref[...].astype(F32)
    for s in range(steps):
        x_copies[s].wait()
        wide = x_buf[s].astype(F32)
        mean = jnp.mean(wide, axis=-1, keepdims=True)
        cent = wide - mean
        rstd = lax.rsqrt(jnp.mean(cent * cent, axis=-1, keepdims=True) + LN_EPS)
        for n in range(d_model // LANES):
            cols = slice(n * LANES, (n + 1) * LANES)
            hid[s * batch:(s + 1) * batch, cols] = (cent[:, cols] * rstd * gain[n:n + 1, :] + shift[n:n + 1, :]).astype(BF16)

    def rotate(vec):
        return (vec * cos_full + pltpu.roll(vec, half, 1) * sin_full).astype(BF16).astype(F32)

    def swap(n):
        return pltpu.make_async_remote_copy(src_ref=mine.at[n], dst_ref=theirs.at[n], send_sem=send.at[n], recv_sem=recv.at[n],
                                            device_id=sib, device_id_type=pl.DeviceIdType.MESH)

    def place(n, core, block):
        for s in range(steps):
            rows = block[s * batch:(s + 1) * batch, :]
            if n < group:
                q_rows[pl.ds(n * kvs * steps + core * steps + s, batch, stride=per_row), :] = rows
            elif n == group:
                kn_rows[pl.ds(s * kvs + core, batch, stride=16), :] = rows
            else:
                vn_rows[pl.ds(s * kvs + core, batch, stride=16), :] = rows

    kn_rows[...] = jnp.zeros_like(kn_rows)
    vn_rows[...] = jnp.zeros_like(vn_rows)
    kv_bias = [jnp.where(c == 0, ref[0:1, :].astype(F32), ref[1:2, :].astype(F32)) for ref in (bk_ref, bv_ref)]
    total = group + 2
    per = COLS // LANES
    groups = [(range(n * per, (n + 1) * per), wq_buf.at[n], w_copies[n]) for n in range(n_q)]
    groups += [((group + n,), wkv_buf.at[n], w_copies[n_q + n]) for n in range(2)]
    for heads, weight, copy in groups:
        copy.wait()
        block = jnp.dot(hid[...], weight[...], preferred_element_type=F32)
        for at, n in enumerate(heads):
            bias = bias_q[pl.ds(c * group + n, 1), :] if n < group else kv_bias[n - group]
            vec = (block[:, at * LANES:(at + 1) * LANES] + bias).astype(BF16).astype(F32)
            mine[n] = rotate(vec) if n <= group else vec
            swap(n).start()
            place(n, c, mine.at[n])
    for n in range(total):
        swap(n).wait_recv()
        place(n, 1 - c, theirs.at[n])

    kn_out[...] = kn_rows[...].reshape(kn_out.shape).astype(BF16)
    vn_out[...] = vn_rows[...].reshape(vn_out.shape).astype(BF16)

    @pl.loop(0, batch)
    def _(b):
        q_out[b] = q_rows[pl.ds(pl.multiple_of(b * per_row, 8), per_row), :].astype(BF16)

    for n in range(total):
        swap(n).wait_send()


def front(positions, x_steps, gain, shift, b_q, b_k, b_v, w_q, w_k, w_v, kvs):
    steps, batch, d_model = x_steps.shape
    heads = w_q.shape[1] // LANES
    group = heads // kvs
    rows = group * kvs * steps
    assert kvs == 2
    inv_freq = jnp.power(F32(ROPE_BASE), -2.0 * jnp.arange(LANES // 2, dtype=F32) / LANES).reshape(1, -1)
    vm = pl.BlockSpec(memory_space=pltpu.VMEM)
    hbm = pl.BlockSpec(memory_space=pl.ANY)
    tiles = lambda vec: vec.reshape(-1, LANES)
    return pl.pallas_call(
        functools.partial(front_kernel, (steps, kvs, group)),
        out_shape=[
            jax.ShapeDtypeStruct((batch, rows, LANES), BF16),
            jax.ShapeDtypeStruct((batch, 16, LANES), BF16),
            jax.ShapeDtypeStruct((batch, 16, LANES), BF16),
        ],
        in_specs=[pl.BlockSpec(memory_space=pltpu.SMEM), hbm] + [vm] * 6 + [hbm] * 3,
        out_specs=[vm] * 3,
        scratch_shapes=[
            pltpu.VMEM((steps, batch, d_model), BF16),
            pltpu.VMEM((steps * batch, d_model), BF16),
            pltpu.VMEM((group * LANES // COLS, d_model, COLS), BF16),
            pltpu.VMEM((2, d_model, LANES), BF16),
            pltpu.VMEM((group + 2, steps * batch, LANES), F32),
            pltpu.VMEM((group + 2, steps * batch, LANES), F32),
            pltpu.VMEM((batch, LANES), F32),
            pltpu.VMEM((batch * rows, LANES), F32),
            pltpu.VMEM((batch * 16, LANES), F32),
            pltpu.VMEM((batch * 16, LANES), F32),
            pltpu.VMEM((heads, LANES), F32),
            pltpu.SemaphoreType.DMA((group + 2,)),
            pltpu.SemaphoreType.DMA((steps,)),
            pltpu.SemaphoreType.DMA((group + 2,)),
            pltpu.SemaphoreType.DMA((group + 2,)),
        ],
        compiler_params=pltpu.CompilerParams(collective_id=1, has_side_effects=True, vmem_limit_bytes=VMEM_CAP),
        cost_estimate=pl.CostEstimate(flops=steps * batch * d_model * (w_q.shape[1] + 2 * w_k.shape[1]),
                                      bytes_accessed=d_model * (w_q.shape[1] + 2 * w_k.shape[1]), transcendentals=0),
        name="front",
    )(positions, x_steps, inv_freq, tiles(gain), tiles(shift), tiles(b_q), tiles(b_k), tiles(b_v), w_q, w_k, w_v)


PER = 2
DEPTH = 8
AHEAD = 4

def attend_kernel(cfg, pos_ref, q_hbm, kn_hbm, vn_hbm, k_hbm, v_hbm, *refs):
    steps, kvs, group, slots, n_blocks, own_half = cfg
    (ko_hbm, vo_hbm, o_hbm, k_buf, v_buf, q_ref, kn_ref, vn_ref, o_tile, o_rows, stat_rows,
     k_in, v_in, k_up, v_up, small_in, o_up) = refs[2 if own_half else 0:]
    x = lax.axis_index("sq") // 2
    base = (x if own_half else 1 - x) * (n_blocks * PER)
    lse_cols = slice(kvs * group * LANES, (kvs * group + 1) * LANES)
    rows = k_hbm.shape[1]
    tile = steps * kvs
    per_row = group * tile
    first = lax.axis_index("sq") * (rows // kvs)
    coef = LANES ** -0.5 * LOG2E
    contract_last = (((1,), (1,)), ((), ()))
    blocks_per_tile = 8 // PER

    def seqs(i):
        return pl.ds(base + i * PER, PER)

    def fetch(i):
        slot = lax.rem(i, DEPTH)
        return (pltpu.make_async_copy(k_hbm.at[seqs(i)], k_buf.at[slot], k_in.at[slot]),
                pltpu.make_async_copy(v_hbm.at[seqs(i)], v_buf.at[slot], v_in.at[slot]))

    def put(i):
        slot = lax.rem(i, DEPTH)
        return (pltpu.make_async_copy(k_buf.at[slot], ko_hbm.at[seqs(i)], k_up.at[slot]),
                pltpu.make_async_copy(v_buf.at[slot], vo_hbm.at[seqs(i)], v_up.at[slot]))

    half_seqs = pl.ds(base, n_blocks * PER)
    small = [pltpu.make_async_copy(src.at[half_seqs], dst, small_in.at[n])
             for n, (src, dst) in enumerate(((q_hbm, q_ref), (kn_hbm, kn_ref), (vn_hbm, vn_ref)))]
    for copy in small:
        copy.start()
    for i in range(2):
        for copy in fetch(jnp.int32(i)):
            copy.start()

    def put_tile(t):
        return pltpu.make_async_copy(o_tile.at[t], o_hbm.at[:, pl.ds(pl.multiple_of(t * 8, 8), 8), :], o_up.at[t])

    sub = lax.broadcasted_iota(jnp.int32, (tile, rows), 0)
    lane = lax.broadcasted_iota(jnp.int32, (tile, rows), 1)
    sub2 = lax.broadcasted_iota(jnp.int32, (tile, 16), 0)
    lane2 = lax.broadcasted_iota(jnp.int32, (tile, 16), 1)
    new_step = lane2 // kvs
    new_ok = ((lane2 % kvs) == (sub2 // steps)) & (new_step <= sub2 % steps)
    stat_sub = lax.broadcasted_iota(jnp.int32, (tile, LANES), 0)
    stat_lane = lax.broadcasted_iota(jnp.int32, (tile, LANES), 1) - (stat_sub // steps) * group
    win_row = lax.broadcasted_iota(jnp.int32, (32, LANES), 0)

    def renew(i):
        slot_of = lax.rem(i, DEPTH)
        for one in range(PER):
            seq = i * PER + one
            goal = kvs * ((pos_ref[base + seq] & (slots - 1)) - first)
            goal = jnp.where(goal > kvs * (slots - steps), goal - kvs * slots, goal)
            start = pl.multiple_of(jnp.clip((goal >> 4) << 4, 0, rows - 32), 16)
            offset = win_row + (start - goal)
            for buf, new in ((k_buf, kn_ref), (v_buf, vn_ref)):
                fresh = new[seq].astype(F32)
                window = buf[slot_of, one, pl.ds(start, 32), :].astype(F32)
                for r in range(tile):
                    window = jnp.where(offset == r, fresh[r:r + 1, :], window)
                buf[slot_of, one, pl.ds(start, 32), :] = window.astype(BF16)

    @pl.loop(0, n_blocks)
    def _(i):
        slot_now = lax.rem(i, DEPTH)

        @pl.when(i >= 1)
        def _():
            renew(i - 1)

        @pl.when(i >= AHEAD)
        def _():
            for copy in put(i - AHEAD):
                copy.wait()

        @pl.when(i == 0)
        def _():
            for later in range(2, AHEAD):
                for copy in fetch(jnp.int32(later)):
                    copy.start()

        @pl.when(i + AHEAD < n_blocks)
        def _():
            for copy in fetch(i + AHEAD):
                copy.start()

        @pl.when(i >= 1)
        def _():
            for copy in put(i - 1):
                copy.start()

        @pl.when((i >= 1) & (lax.rem(i, blocks_per_tile) == 0))
        def _():
            put_tile(i // blocks_per_tile - 1).start()

        k_copy, v_copy = fetch(i)
        @pl.when(i == 0)
        def _():
            for copy in small:
                copy.wait()

        k_copy.wait()
        v_copy.wait()
        state = []
        for one in range(PER):
            seq = i * PER + one
            pos = pos_ref[base + seq]
            q = q_ref[seq]
            raw = lax.dot_general(q, k_buf[slot_now, one], contract_last, preferred_element_type=F32)
            raw2 = lax.dot_general(q, kn_ref[seq], contract_last, preferred_element_type=F32)
            state.append((seq, pos, raw, raw2))
        soft = []
        for seq, pos, raw, raw2 in state:
            slot = first + (lane >> 1)
            ahead = (slot - pos) & (slots - 1)
            ok = ((lane & 1) == (sub >> 2)) & (slot < pos) & (ahead > (sub & 3))
            bias = jnp.where(ok, 0.0, NEG_BIG).astype(F32)
            new_slot = ((pos + new_step) & (slots - 1)) - first
            here = (new_slot >= 0) & (new_slot < rows // kvs)
            bias2 = jnp.where(new_ok & here, 0.0, NEG_BIG).astype(F32)
            score = raw.reshape(group, tile, rows) * coef + bias[None]
            score2 = raw2.reshape(group, tile, 16) * coef + bias2[None]
            top = jnp.maximum(jnp.max(score, axis=-1, keepdims=True), jnp.max(score2, axis=-1, keepdims=True))
            top = jnp.maximum(top, NEG_HALF)
            w = jnp.exp2(score - top)
            w2 = jnp.exp2(score2 - top)
            total = jnp.sum(w, axis=-1, keepdims=True) + jnp.sum(w2, axis=-1, keepdims=True)
            soft.append((top, total, w.reshape(per_row, rows).astype(BF16), w2.reshape(per_row, 16).astype(BF16)))
        for one in range(PER):
            seq, pos = state[one][:2]
            top, total, w, w2 = soft[one]
            out = jnp.dot(w, v_buf[slot_now, one], preferred_element_type=F32)
            out = out + jnp.dot(w2, vn_ref[seq], preferred_element_type=F32)
            some = total > 0.0
            safe = jnp.where(some, total, 1.0)
            lse = jnp.where(some, top + jnp.log2(safe), NEG_BIG)
            out = out.reshape(group, tile, LANES) * (1.0 / safe)
            stats = jnp.zeros((tile, LANES), F32)
            for n in range(group):
                stats = jnp.where(stat_lane == n, lse[n], stats)
            seat = lax.rem(i, blocks_per_tile) * PER + one
            o_rows[pl.ds(pl.multiple_of(seat * per_row, 8), per_row), :] = out.reshape(per_row, LANES)
            stat_rows[pl.ds(pl.multiple_of(seat * tile, 8), tile), :] = stats
        @pl.when(lax.rem(i, blocks_per_tile) == blocks_per_tile - 1)
        def _():
            t = i // blocks_per_tile
            for s in range(steps):
                o_tile[t, s, :, lse_cols] = sum(stat_rows[pl.ds(h * steps + s, 8, stride=tile), :] for h in range(kvs))
                for h in range(kvs):
                    for n in range(group):
                        col = (h * group + n) * LANES
                        o_tile[t, s, :, col:col + LANES] = o_rows[pl.ds(n * tile + h * steps + s, 8, stride=per_row), :]

    renew(jnp.int32(n_blocks - 1))
    for copy in put(n_blocks - 1):
        copy.start()
    tiles = n_blocks // blocks_per_tile
    put_tile(tiles - 1).start()
    for j in range(AHEAD):
        for copy in put(n_blocks - AHEAD + j):
            copy.wait()
    for t in range(tiles):
        put_tile(t).wait()


def attend(positions, q, k_new, v_new, k_rows, v_rows, steps, kvs, group, slots, handed=()):
    batch, rows, dim = k_rows.shape
    half = batch // 2
    hbm = pl.BlockSpec(memory_space=pl.ANY)
    return pl.pallas_call(
        functools.partial(attend_kernel, (steps, kvs, group, slots, half // PER, bool(handed))),
        in_specs=[pl.BlockSpec(memory_space=pltpu.SMEM)] + [hbm] * (5 + len(handed)),
        out_specs=[hbm, hbm, hbm],
        out_shape=[
            jax.ShapeDtypeStruct(k_rows.shape, BF16),
            jax.ShapeDtypeStruct(v_rows.shape, BF16),
            jax.ShapeDtypeStruct((steps, half, (kvs * group + 1) * dim), F32),
        ],
        input_output_aliases={6: 0, 7: 1} if handed else {},
        scratch_shapes=[
            pltpu.VMEM((DEPTH, PER, rows, dim), BF16),
            pltpu.VMEM((DEPTH, PER, rows, dim), BF16),
            pltpu.VMEM((half, q.shape[1], dim), BF16),
            pltpu.VMEM((half, k_new.shape[1], dim), BF16),
            pltpu.VMEM((half, v_new.shape[1], dim), BF16),
            pltpu.VMEM((half // 8, steps, 8, (kvs * group + 1) * dim), F32),
            pltpu.VMEM((8 * q.shape[1], dim), F32),
            pltpu.VMEM((8 * steps * kvs, dim), F32),
            pltpu.SemaphoreType.DMA((DEPTH,)),
            pltpu.SemaphoreType.DMA((DEPTH,)),
            pltpu.SemaphoreType.DMA((DEPTH,)),
            pltpu.SemaphoreType.DMA((DEPTH,)),
            pltpu.SemaphoreType.DMA((3,)),
            pltpu.SemaphoreType.DMA((half // 8,)),
        ],
        compiler_params=pltpu.CompilerParams(vmem_limit_bytes=VMEM_CAP),
        cost_estimate=pl.CostEstimate(flops=20_000_000_000, bytes_accessed=4 * batch * rows * dim,
                                      transcendentals=half * rows * q.shape[1]),
        name="attend_own" if handed else "attend_peer",
    )(positions, q, k_new, v_new, k_rows, v_rows, *handed)


CHUNK = 512
PIECE = 256
RING = 9
WO_SLOTS = 3
(C_OWN_O, C_X_O, C_OWN_E, C_X_E, C_HID_A, C_HID_B) = range(6)
(W_CORE, W_Y, J_CORE, J_Y, J_OWN_X, J_OWN_C, J_FWD_C) = range(7)


def tail_kernel(cfg, own_hbm, xin_hbm, x_hbm, wo_hbm, wfc_hbm, wproj_hbm, bo_ref, gain_ref, shift_ref, bfc_ref, bproj_ref,
                y_ref,
                my_own, my_x, my_own_e, my_x_e, sib_own, sib_x, sib_own_e, sib_x_e, a_buf, w_part, w_core, w_half, w_y, x_buf, x_mid, hid, hid_b,
                ring, g_buf, p_part, p_core, p_half, p_y, y_all, bo_rows, bfc_rows, bproj_rows,
                send_a, recv_a, send_j, recv_j, local_sem, wo_sem, x_sem, ring_sem):
    steps, batch, group, chunks, kvs = cfg
    half = batch // 2
    pair = steps // 2 * half
    head_cols = group * LANES
    ff_own = wfc_hbm.shape[1] // 2
    pieces = chunks * CHUNK // PIECE
    per = CHUNK // PIECE
    y = lax.axis_index("tp")
    sq = lax.axis_index("sq")
    x, c = sq // 2, sq % 2
    sib = {"sq": x * 2 + 1 - c}
    xpeer = {"sq": (1 - x) * 2 + c}
    ypeer = {"tp": 1 - y}
    MESH = pl.DeviceIdType.MESH

    def chunk_cols(j):
        return pl.ds(pl.multiple_of(j * CHUNK, CHUNK), CHUNK)

    def load_item(item, slot):
        @pl.when(item < chunks)
        def _():
            col = pl.multiple_of(c * ff_own + item * CHUNK, CHUNK)
            pltpu.make_async_copy(wfc_hbm.at[:, pl.ds(col, CHUNK)], ring.at[slot], ring_sem.at[slot]).start()

        @pl.when(item >= chunks)
        def _():
            row = pl.multiple_of(c * ff_own, CHUNK)
            pltpu.make_async_copy(wproj_hbm.at[pl.ds(row, ff_own), chunk_cols(item - chunks)], ring.at[slot], ring_sem.at[slot]).start()

    def wait_item(slot):
        pltpu.make_async_copy(wfc_hbm.at[:, pl.ds(0, CHUNK)], ring.at[slot], ring_sem.at[slot]).wait()

    wo_rows = pl.ds(pl.multiple_of(c * head_cols, LANES), head_cols)
    per_slot = ring.shape[1] // head_cols

    def wo_place(j):
        return ring.at[j // per_slot, pl.ds(pl.multiple_of(lax.rem(j, per_slot) * head_cols, LANES), head_cols), :]

    def wo_copy(j):
        return pltpu.make_async_copy(wo_hbm.at[wo_rows, chunk_cols(j)], wo_place(j), wo_sem.at[j])

    def slot_of(item):
        return lax.rem(item + WO_SLOTS, RING)

    my_cols = pl.ds(pl.multiple_of(c * head_cols, LANES), head_cols)
    stat_cols = slice(kvs * head_cols, kvs * head_cols + LANES)
    locals_ = [pltpu.make_async_copy(src, dst, local_sem.at[n]) for n, (src, dst) in enumerate((
        (own_hbm.at[:, :, stat_cols], my_own_e), (xin_hbm.at[:, :, stat_cols], my_x_e),
        (own_hbm.at[:, :, my_cols], my_own), (xin_hbm.at[:, :, my_cols], my_x)))]
    for copy in locals_:
        copy.start()
    for j in range(chunks):
        wo_copy(jnp.int32(j)).start()
    x_copy = pltpu.make_async_copy(x_hbm.at[pl.ds(2 * c, 2), pl.ds(pl.multiple_of(x * half, 8), half), :], x_buf, x_sem)
    x_copy.start()
    barrier = pltpu.get_barrier_semaphore()
    for who in (sib, xpeer, ypeer):
        pl.semaphore_signal(barrier, inc=1, device_id=who, device_id_type=MESH)
    pl.semaphore_wait(barrier, 3)

    def remote(src, dst, kind, who):
        return pltpu.make_async_remote_copy(src_ref=src, dst_ref=dst, send_sem=send_a.at[kind], recv_sem=recv_a.at[kind],
                                            device_id=who, device_id_type=MESH)

    sib_cols = pl.ds(pl.multiple_of((1 - c) * head_cols, LANES), head_cols)
    swaps = [remote(own_hbm.at[:, :, stat_cols], sib_own_e, C_OWN_E, sib), remote(xin_hbm.at[:, :, stat_cols], sib_x_e, C_X_E, sib),
             remote(own_hbm.at[:, :, sib_cols], sib_own, C_OWN_O, sib), remote(xin_hbm.at[:, :, sib_cols], sib_x, C_X_O, sib)]
    for copy in swaps:
        copy.start()
    bo_rows[...] = bo_ref[...].astype(F32)
    bfc_rows[...] = bfc_ref[...].astype(F32)
    bproj_rows[...] = bproj_ref[...].astype(F32)

    def flat(block):
        return block.reshape(steps * half, LANES)

    def my_lanes(stat):
        stat = flat(stat)
        return jnp.where(c == 0, stat, pltpu.roll(stat, LANES - group, 1))

    for copy in locals_:
        copy.wait()
    swaps[0].wait_recv()
    swaps[1].wait_recv()
    logs = [my_lanes(my_own_e[...]), my_lanes(sib_own_e[...]), my_lanes(my_x_e[...]), my_lanes(sib_x_e[...])]
    top = functools.reduce(jnp.maximum, logs)
    shares = [jnp.exp2(e - top) for e in logs]
    inv = 1.0 / sum(shares)
    shares = [w * inv for w in shares]
    swaps[2].wait_recv()
    swaps[3].wait_recv()
    for i in range(group):
        cols = slice(i * LANES, (i + 1) * LANES)
        parts = [part[:, :, cols] for part in (my_own, sib_own, my_x, sib_x)]
        a_buf[:, cols] = sum(w[:, i:i + 1] * flat(part) for w, part in zip(shares, parts)).astype(BF16)

    def jcopy(src, dst, kind, j, who):
        return pltpu.make_async_remote_copy(src_ref=src, dst_ref=dst, send_sem=send_j.at[kind, j], recv_sem=recv_j.at[kind, j],
                                            device_id=who, device_id_type=MESH)

    def pair_rows(core):
        return pl.ds(pl.multiple_of(core * pair, 8), pair)

    def to_core(part, inbox, kind, j):
        return jcopy(part.at[j, pair_rows(1 - c), :], inbox.at[j], kind, j, sib)

    def to_y(total, inbox, kind, j):
        return jcopy(total.at[j], inbox.at[j], kind, j, ypeer)

    def core_sum(part, inbox, total, inbox_y, kind, kind_y, j):
        to_core(part, inbox, kind, j).wait_recv()
        total[j] = part[j, pair_rows(c), :] + inbox[j]
        to_y(total, inbox_y, kind_y, j).start()

    def bias_of(rows, j, width):
        n = width // LANES
        return jnp.concatenate([rows[pl.ds(j * n + e, 1), :] for e in range(n)], axis=-1)

    def piece_cols(u):
        return pl.ds(pl.multiple_of(u * PIECE, PIECE), PIECE)

    def send_product(product, part, inbox, kind, j):
        for e in range(per):
            part[j * per + e] = product[:, e * PIECE:(e + 1) * PIECE]
        for e in range(per):
            to_core(part, inbox, kind, j * per + e).start()

    def y_sum(total, inbox):
        low = jnp.where(y == 0, total, inbox)
        high = jnp.where(y == 0, inbox, total)
        return low + high

    def stage(it, lag, body):
        u = it - lag

        @pl.when((u >= 0) & (u < pieces))
        def _():
            body(u)

    def product_stage(it, body):
        @pl.when((it < pieces) & (lax.rem(it, per) == 0))
        def _():
            body(it // per)

    def o_product(j):
        wo_copy(j).wait()
        product = jnp.dot(a_buf[...], wo_place(j)[...], preferred_element_type=F32)
        send_product(product, w_part, w_core, W_CORE, j)

    def o_core_sum(j):
        core_sum(w_part, w_core, w_half, w_y, W_CORE, W_Y, j)

    for k in range(RING - WO_SLOTS):
        load_item(jnp.int32(k), slot_of(k))

    @pl.loop(0, pieces + 6)
    def _(it):
        product_stage(it, o_product)
        stage(it, 6, o_core_sum)

    for k in range(RING - WO_SLOTS, RING):
        load_item(jnp.int32(k), slot_of(k))
    x_copy.wait()

    @pl.loop(0, pieces)
    def _(u):
        cols = piece_cols(u)
        to_y(w_half, w_y, W_Y, u).wait_recv()
        x_in = x_buf[:, :, cols].astype(F32).reshape(pair, PIECE)
        x_mid[:, cols] = (x_in + y_sum(w_half[u], w_y[u]) + bias_of(bo_rows, u, PIECE)).astype(BF16).astype(F32)

    gain = gain_ref[...].astype(F32)
    shift = shift_ref[...].astype(F32)
    d_model = x_mid.shape[1]
    hid_copies = []
    for part in range(2):
        src = slice(part * half, (part + 1) * half)
        dst = pl.ds(pl.multiple_of(c * pair + part * half, 8), half)
        rows = x_mid[src, :]
        mean = jnp.mean(rows, axis=-1, keepdims=True)
        cent = rows - mean
        rstd = lax.rsqrt(jnp.mean(cent * cent, axis=-1, keepdims=True) + LN_EPS)
        for n in range(d_model // LANES):
            cols = slice(n * LANES, (n + 1) * LANES)
            hid[dst, cols] = (cent[:, cols] * rstd * gain[n:n + 1, :] + shift[n:n + 1, :]).astype(BF16).astype(F32)
        copy = remote(hid.at[dst, :], hid.at[dst, :], (C_HID_A, C_HID_B)[part], sib)
        copy.start()
        hid_copies.append(copy)
    for copy in hid_copies:
        copy.wait_recv()
    hid_b[...] = hid[...].astype(BF16)

    together = 3

    @pl.loop(0, chunks // together)
    def _(first):
        group_of = [first * together + e for e in range(together)]
        for j in group_of:
            wait_item(slot_of(j))
        for j in group_of:
            pre = jnp.dot(hid_b[...], ring[slot_of(j)], preferred_element_type=F32) + bias_of(bfc_rows, c * chunks + j, CHUNK)
            cube = pre * pre * pre
            act = 0.5 * pre * (1.0 + jnp.tanh(math.sqrt(2.0 / math.pi) * (pre + 0.044715 * cube)))
            g_buf[:, chunk_cols(j)] = act.astype(BF16)
        for j in group_of:
            load_item(j + RING, slot_of(j))

    def block(j, core, xx):
        return y_all.at[j, pl.ds(2 * core, 2), pl.ds(pl.multiple_of(xx * half, 8), half), :]

    def spread(kind, j):
        ref, who = {J_OWN_X: (block(j, c, x), xpeer), J_OWN_C: (block(j, c, x), sib), J_FWD_C: (block(j, c, 1 - x), sib)}[kind]
        return jcopy(ref, ref, kind, j, who)

    def do_product(j):
        item = chunks + j
        slot = slot_of(item)
        wait_item(slot)
        product = jnp.dot(g_buf[...], ring[slot], preferred_element_type=F32)
        send_product(product, p_part, p_core, J_CORE, j)

        @pl.when(item + RING < 2 * chunks)
        def _():
            load_item(item + RING, slot)

    def do_core_sum(j):
        core_sum(p_part, p_core, p_half, p_y, J_CORE, J_Y, j)

    def do_y_sum(j):
        to_y(p_half, p_y, J_Y, j).wait_recv()
        full = x_mid[:, piece_cols(j)] + y_sum(p_half[j], p_y[j]) + bias_of(bproj_rows, j, PIECE)
        y_all[j, pl.ds(2 * c, 2), pl.ds(pl.multiple_of(x * half, 8), half), :] = full.astype(BF16).astype(F32).reshape(2, half, PIECE)
        spread(J_OWN_X, j).start()
        spread(J_OWN_C, j).start()

    def do_forward(j):
        spread(J_OWN_X, j).wait_recv()
        spread(J_FWD_C, j).start()

    def do_store(j):
        spread(J_OWN_C, j).wait_recv()
        spread(J_FWD_C, j).wait_recv()
        y_ref[:, :, piece_cols(j)] = y_all[j].astype(BF16)

    @pl.loop(0, pieces + 13)
    def _(it):
        product_stage(it, do_product)
        stage(it, 2, do_core_sum)
        stage(it, 7, do_y_sum)
        stage(it, 11, do_forward)
        stage(it, 13, do_store)

    for copy in swaps + hid_copies:
        copy.wait_send()

    @pl.loop(0, pieces)
    def _(j):
        to_core(w_part, w_core, W_CORE, j).wait_send()
        to_y(w_half, w_y, W_Y, j).wait_send()
        to_core(p_part, p_core, J_CORE, j).wait_send()
        to_y(p_half, p_y, J_Y, j).wait_send()
        for kind in (J_OWN_X, J_OWN_C, J_FWD_C):
            spread(kind, j).wait_send()


def tail(own, x_in, x_steps, w_o, w_fc, w_proj, b_o, gain, shift, b_fc, b_proj, group, kvs):
    steps, half, _ = own.shape
    batch = 2 * half
    rows = steps * half
    pair = rows // 2
    d_model = w_o.shape[1]
    chunks = d_model // CHUNK
    pieces = d_model // PIECE
    ff_own = w_fc.shape[1] // 2
    assert ff_own == d_model and steps == 4 and kvs == 2
    head_cols = group * LANES
    vm = pl.BlockSpec(memory_space=pltpu.VMEM)
    hbm = pl.BlockSpec(memory_space=pl.ANY)
    cfg = (steps, batch, group, chunks, kvs)
    tiles = lambda vec: vec.reshape(-1, LANES)
    scratch = [
        pltpu.VMEM((steps, half, head_cols), F32),
        pltpu.VMEM((steps, half, head_cols), F32),
        pltpu.VMEM((steps, half, LANES), F32),
        pltpu.VMEM((steps, half, LANES), F32),
        pltpu.VMEM((steps, half, head_cols), F32),
        pltpu.VMEM((steps, half, head_cols), F32),
        pltpu.VMEM((steps, half, LANES), F32),
        pltpu.VMEM((steps, half, LANES), F32),
        pltpu.VMEM((rows, head_cols), BF16),
        pltpu.VMEM((pieces, rows, PIECE), F32),
        pltpu.VMEM((pieces, pair, PIECE), F32),
        pltpu.VMEM((pieces, pair, PIECE), F32),
        pltpu.VMEM((pieces, pair, PIECE), F32),
        pltpu.VMEM((2, half, d_model), BF16),
        pltpu.VMEM((pair, d_model), F32),
        pltpu.VMEM((rows, d_model), F32),
        pltpu.VMEM((rows, d_model), BF16),
        pltpu.VMEM((RING, d_model, CHUNK), BF16),
        pltpu.VMEM((rows, ff_own), BF16),
        pltpu.VMEM((pieces, rows, PIECE), F32),
        pltpu.VMEM((pieces, pair, PIECE), F32),
        pltpu.VMEM((pieces, pair, PIECE), F32),
        pltpu.VMEM((pieces, pair, PIECE), F32),
        pltpu.VMEM((pieces, steps, batch, PIECE), F32),
        pltpu.VMEM((d_model // LANES, LANES), F32),
        pltpu.VMEM((2 * ff_own // LANES, LANES), F32),
        pltpu.VMEM((d_model // LANES, LANES), F32),
        pltpu.SemaphoreType.DMA((6,)),
        pltpu.SemaphoreType.DMA((6,)),
        pltpu.SemaphoreType.DMA((7, pieces)),
        pltpu.SemaphoreType.DMA((7, pieces)),
        pltpu.SemaphoreType.DMA((4,)),
        pltpu.SemaphoreType.DMA((chunks,)),
        pltpu.SemaphoreType.DMA,
        pltpu.SemaphoreType.DMA((RING,)),
    ]
    return pl.pallas_call(
        functools.partial(tail_kernel, cfg),
        out_shape=pltpu.VMEM((steps, batch, d_model), BF16),
        in_specs=[hbm] * 6 + [vm] * 5,
        out_specs=vm,
        scratch_shapes=scratch,
        compiler_params=pltpu.CompilerParams(collective_id=0, has_side_effects=True, vmem_limit_bytes=TAIL_VMEM),
        cost_estimate=pl.CostEstimate(flops=2 * rows * d_model * (head_cols + 2 * ff_own), bytes_accessed=100_000_000, transcendentals=0),
        name="tail",
    )(own, x_in, x_steps, w_o, w_fc, w_proj, tiles(b_o), tiles(gain), tiles(shift), tiles(b_fc), tiles(b_proj))


def solution(mesh):
    sq_size = mesh.shape["sq"]
    act_spec = P(None, "dp", None)
    cache_spec = P("dp", "sq", "tp", None)
    col_spec = P(None, "tp")
    row_spec = P("tp", None)
    vec_spec = P("tp")
    rep_spec = P(None)
    in_specs = (act_spec, P("dp"), cache_spec, cache_spec, col_spec, vec_spec, col_spec, vec_spec,
                col_spec, vec_spec, row_spec, rep_spec, rep_spec, rep_spec, rep_spec, rep_spec,
                col_spec, vec_spec, row_spec, rep_spec)
    out_specs = (act_spec, cache_spec, cache_spec)

    def per_device(x_steps, positions, key_buf, val_buf, w_q, b_q, w_k, b_k, w_v, b_v, w_o, b_o,
                   ln1_gain, ln1_bias, ln2_gain, ln2_bias, w_fc, b_fc, w_proj, b_proj):
        steps, batch, d_model = x_steps.shape
        slots_local, kvs, dim = key_buf.shape[1], key_buf.shape[2], key_buf.shape[3]
        slots = slots_local * sq_size
        group = w_q.shape[1] // (kvs * dim)
        q_rows, k_new, v_new = front(positions, x_steps, ln1_gain, ln1_bias, b_q, b_k, b_v, w_q, w_k, w_v, kvs)
        k_rows = key_buf.reshape(batch, slots_local * kvs, dim)
        v_rows = val_buf.reshape(batch, slots_local * kvs, dim)
        caches = (positions, q_rows, k_new, v_new, k_rows, v_rows, steps, kvs, group, slots)
        k_out, v_out, for_peer = attend(*caches)
        from_peer = lax.ppermute(for_peer, "sq", [(d, d ^ 2) for d in range(sq_size)])
        k_out, v_out, own = attend(*caches, handed=(k_out, v_out))
        ys = tail(own, from_peer, x_steps, w_o, w_fc, w_proj, b_o, ln2_gain, ln2_bias, b_fc, b_proj, group, kvs)
        return ys, k_out.reshape(key_buf.shape), v_out.reshape(val_buf.shape)

    return jax.shard_map(per_device, mesh=mesh, in_specs=in_specs, out_specs=out_specs, check_vma=False)
```

```python
import functools
import math

import jax
import jax.numpy as jnp
from jax import lax
from jax.experimental import pallas as pl
from jax.experimental.pallas import tpu as pltpu
from jax.sharding import PartitionSpec as P

ROPE_BASE = 1000000.0
LN_EPS = 1e-5
NEG_BIG = -1e30
NEG_HALF = -1e29
LOG2E = 1.4426950408889634
VMEM_CAP = 67_043_328
TAIL_VMEM = 64_900_000
F32 = jnp.float32
BF16 = jnp.bfloat16
LANES = 128


COLS = 384

def front_kernel(cfg, pos_ref, x_hbm, freq_ref, gain_ref, shift_ref, bq_ref, bk_ref, bv_ref, wq_hbm, wk_hbm, wv_hbm,
                 q_out, kn_out, vn_out, x_buf, hid, wq_buf, wkv_buf, mine, theirs, pos_rows, q_rows, kn_rows, vn_rows, bias_q,
                 sem, x_sem, send, recv):
    steps, kvs, group = cfg
    batch, d_model = x_buf.shape[1], x_buf.shape[2]
    head_cols = group * LANES
    per_row = group * kvs * steps
    sq = lax.axis_index("sq")
    c = sq % 2
    sib = {"sq": (sq // 2) * 2 + 1 - c}

    x_copies = [pltpu.make_async_copy(x_hbm.at[s], x_buf.at[s], x_sem.at[s]) for s in range(steps)]
    for copy in x_copies:
        copy.start()
    head_at = pl.multiple_of(c * LANES, LANES)
    n_q = head_cols // COLS
    w_copies = [pltpu.make_async_copy(wq_hbm.at[:, pl.ds(pl.multiple_of(c * head_cols + n * COLS, LANES), COLS)], wq_buf.at[n], sem.at[n])
                for n in range(n_q)]
    w_copies += [pltpu.make_async_copy(src.at[:, pl.ds(head_at, LANES)], wkv_buf.at[n], sem.at[n_q + n])
                 for n, src in enumerate((wk_hbm, wv_hbm))]
    for copy in w_copies[:2]:
        copy.start()

    barrier = pltpu.get_barrier_semaphore()
    pl.semaphore_signal(barrier, inc=1, device_id=sib, device_id_type=pl.DeviceIdType.MESH)
    pl.semaphore_wait(barrier, 1)

    for b in range(batch):
        pos_rows[b:b + 1, :] = jnp.full((1, LANES), pos_ref[b], jnp.int32).astype(F32)
    half = LANES // 2
    where = pos_rows[:, :half]
    angle = jnp.concatenate([where + float(s) for s in range(steps)], axis=0) * freq_ref[...]
    cos, sin = jnp.cos(angle), jnp.sin(angle)
    cos_full = jnp.concatenate([cos, cos], axis=-1)
    sin_full = jnp.concatenate([-sin, sin], axis=-1)

    bias_q[...] = bq_ref[...].astype(F32)
    gain = gain_ref[...].astype(F32)
    shift = shift_ref[...].astype(F32)
    for s in range(steps):
        x_copies[s].wait()
        wide = x_buf[s].astype(F32)
        mean = jnp.mean(wide, axis=-1, keepdims=True)
        cent = wide - mean
        rstd = lax.rsqrt(jnp.mean(cent * cent, axis=-1, keepdims=True) + LN_EPS)
        for copy in {1: w_copies[2:3], 3: w_copies[3:]}.get(s, ()):
            copy.start()
        for n in range(d_model // LANES):
            cols = slice(n * LANES, (n + 1) * LANES)
            hid[s * batch:(s + 1) * batch, cols] = (cent[:, cols] * rstd * gain[n:n + 1, :] + shift[n:n + 1, :]).astype(BF16)

    def rotate(vec):
        return (vec * cos_full + pltpu.roll(vec, half, 1) * sin_full).astype(BF16).astype(F32)

    def swap(n):
        return pltpu.make_async_remote_copy(src_ref=mine.at[n], dst_ref=theirs.at[n], send_sem=send.at[n], recv_sem=recv.at[n],
                                            device_id=sib, device_id_type=pl.DeviceIdType.MESH)

    def place(n, core, block):
        for s in range(steps):
            rows = block[s * batch:(s + 1) * batch, :]
            if n < group:
                q_rows[pl.ds(n * kvs * steps + core * steps + s, batch, stride=per_row), :] = rows
            elif n == group:
                kn_rows[pl.ds(s * kvs + core, batch, stride=16), :] = rows
            else:
                vn_rows[pl.ds(s * kvs + core, batch, stride=16), :] = rows

    kn_rows[...] = jnp.zeros_like(kn_rows)
    vn_rows[...] = jnp.zeros_like(vn_rows)
    kv_bias = [jnp.where(c == 0, ref[0:1, :].astype(F32), ref[1:2, :].astype(F32)) for ref in (bk_ref, bv_ref)]
    total = group + 2
    per = COLS // LANES
    groups = [(range(n * per, (n + 1) * per), wq_buf.at[n], w_copies[n]) for n in range(n_q)]
    groups += [((group + n,), wkv_buf.at[n], w_copies[n_q + n]) for n in range(2)]
    for heads, weight, copy in groups:
        copy.wait()
        block = jnp.dot(hid[...], weight[...], preferred_element_type=F32)
        for at, n in enumerate(heads):
            bias = bias_q[pl.ds(c * group + n, 1), :] if n < group else kv_bias[n - group]
            vec = (block[:, at * LANES:(at + 1) * LANES] + bias).astype(BF16).astype(F32)
            mine[n] = rotate(vec) if n <= group else vec
            swap(n).start()
            place(n, c, mine.at[n])
    for n in range(total):
        swap(n).wait_recv()
        place(n, 1 - c, theirs.at[n])

    kn_out[...] = kn_rows[...].reshape(kn_out.shape).astype(BF16)
    vn_out[...] = vn_rows[...].reshape(vn_out.shape).astype(BF16)

    @pl.loop(0, batch)
    def _(b):
        q_out[b] = q_rows[pl.ds(pl.multiple_of(b * per_row, 8), per_row), :].astype(BF16)

    for n in range(total):
        swap(n).wait_send()


def front(positions, x_steps, gain, shift, b_q, b_k, b_v, w_q, w_k, w_v, kvs):
    steps, batch, d_model = x_steps.shape
    heads = w_q.shape[1] // LANES
    group = heads // kvs
    rows = group * kvs * steps
    assert kvs == 2
    inv_freq = jnp.power(F32(ROPE_BASE), -2.0 * jnp.arange(LANES // 2, dtype=F32) / LANES).reshape(1, -1)
    vm = pl.BlockSpec(memory_space=pltpu.VMEM)
    hbm = pl.BlockSpec(memory_space=pl.ANY)
    tiles = lambda vec: vec.reshape(-1, LANES)
    return pl.pallas_call(
        functools.partial(front_kernel, (steps, kvs, group)),
        out_shape=[
            jax.ShapeDtypeStruct((batch, rows, LANES), BF16),
            jax.ShapeDtypeStruct((batch, 16, LANES), BF16),
            jax.ShapeDtypeStruct((batch, 16, LANES), BF16),
        ],
        in_specs=[pl.BlockSpec(memory_space=pltpu.SMEM), hbm] + [vm] * 6 + [hbm] * 3,
        out_specs=[vm] * 3,
        scratch_shapes=[
            pltpu.VMEM((steps, batch, d_model), BF16),
            pltpu.VMEM((steps * batch, d_model), BF16),
            pltpu.VMEM((group * LANES // COLS, d_model, COLS), BF16),
            pltpu.VMEM((2, d_model, LANES), BF16),
            pltpu.VMEM((group + 2, steps * batch, LANES), F32),
            pltpu.VMEM((group + 2, steps * batch, LANES), F32),
            pltpu.VMEM((batch, LANES), F32),
            pltpu.VMEM((batch * rows, LANES), F32),
            pltpu.VMEM((batch * 16, LANES), F32),
            pltpu.VMEM((batch * 16, LANES), F32),
            pltpu.VMEM((heads, LANES), F32),
            pltpu.SemaphoreType.DMA((group + 2,)),
            pltpu.SemaphoreType.DMA((steps,)),
            pltpu.SemaphoreType.DMA((group + 2,)),
            pltpu.SemaphoreType.DMA((group + 2,)),
        ],
        compiler_params=pltpu.CompilerParams(collective_id=1, has_side_effects=True, vmem_limit_bytes=VMEM_CAP),
        cost_estimate=pl.CostEstimate(flops=steps * batch * d_model * (w_q.shape[1] + 2 * w_k.shape[1]),
                                      bytes_accessed=d_model * (w_q.shape[1] + 2 * w_k.shape[1]), transcendentals=0),
        name="front",
    )(positions, x_steps, inv_freq, tiles(gain), tiles(shift), tiles(b_q), tiles(b_k), tiles(b_v), w_q, w_k, w_v)


PER = 2
DEPTH = 8
AHEAD = 4

def attend_kernel(cfg, pos_ref, q_hbm, kn_hbm, vn_hbm, k_hbm, v_hbm, *refs):
    steps, kvs, group, slots, n_blocks, own_half = cfg
    (ko_hbm, vo_hbm, o_hbm, k_buf, v_buf, q_ref, kn_ref, vn_ref, o_tile, o_rows, stat_rows,
     k_in, v_in, k_up, v_up, small_in, o_up) = refs[2 if own_half else 0:]
    x = lax.axis_index("sq") // 2
    base = (x if own_half else 1 - x) * (n_blocks * PER)
    lse_cols = slice(kvs * group * LANES, (kvs * group + 1) * LANES)
    rows = k_hbm.shape[1]
    tile = steps * kvs
    per_row = group * tile
    first = lax.axis_index("sq") * (rows // kvs)
    coef = LANES ** -0.5 * LOG2E
    contract_last = (((1,), (1,)), ((), ()))
    blocks_per_tile = 8 // PER

    def seqs(i):
        return pl.ds(base + i * PER, PER)

    def fetch(i):
        slot = lax.rem(i, DEPTH)
        return (pltpu.make_async_copy(k_hbm.at[seqs(i)], k_buf.at[slot], k_in.at[slot]),
                pltpu.make_async_copy(v_hbm.at[seqs(i)], v_buf.at[slot], v_in.at[slot]))

    def put(i):
        slot = lax.rem(i, DEPTH)
        return (pltpu.make_async_copy(k_buf.at[slot], ko_hbm.at[seqs(i)], k_up.at[slot]),
                pltpu.make_async_copy(v_buf.at[slot], vo_hbm.at[seqs(i)], v_up.at[slot]))

    half_seqs = pl.ds(base, n_blocks * PER)
    small = [pltpu.make_async_copy(src.at[half_seqs], dst, small_in.at[n])
             for n, (src, dst) in enumerate(((q_hbm, q_ref), (kn_hbm, kn_ref), (vn_hbm, vn_ref)))]
    for copy in small:
        copy.start()
    for i in range(2):
        for copy in fetch(jnp.int32(i)):
            copy.start()

    def put_tile(t):
        return pltpu.make_async_copy(o_tile.at[t], o_hbm.at[:, pl.ds(pl.multiple_of(t * 8, 8), 8), :], o_up.at[t])

    sub = lax.broadcasted_iota(jnp.int32, (tile, rows), 0)
    lane = lax.broadcasted_iota(jnp.int32, (tile, rows), 1)
    sub2 = lax.broadcasted_iota(jnp.int32, (tile, 16), 0)
    lane2 = lax.broadcasted_iota(jnp.int32, (tile, 16), 1)
    new_step = lane2 // kvs
    new_ok = ((lane2 % kvs) == (sub2 // steps)) & (new_step <= sub2 % steps)
    stat_sub = lax.broadcasted_iota(jnp.int32, (tile, LANES), 0)
    stat_lane = lax.broadcasted_iota(jnp.int32, (tile, LANES), 1) - (stat_sub // steps) * group
    win_row = lax.broadcasted_iota(jnp.int32, (32, LANES), 0)

    def renew(i):
        slot_of = lax.rem(i, DEPTH)
        for one in range(PER):
            seq = i * PER + one
            goal = kvs * ((pos_ref[base + seq] & (slots - 1)) - first)
            goal = jnp.where(goal > kvs * (slots - steps), goal - kvs * slots, goal)
            start = pl.multiple_of(jnp.clip((goal >> 4) << 4, 0, rows - 32), 16)
            offset = win_row + (start - goal)
            for buf, new in ((k_buf, kn_ref), (v_buf, vn_ref)):
                fresh = new[seq].astype(F32)
                window = buf[slot_of, one, pl.ds(start, 32), :].astype(F32)
                for r in range(tile):
                    window = jnp.where(offset == r, fresh[r:r + 1, :], window)
                buf[slot_of, one, pl.ds(start, 32), :] = window.astype(BF16)

    @pl.loop(0, n_blocks)
    def _(i):
        slot_now = lax.rem(i, DEPTH)

        @pl.when(i >= 1)
        def _():
            renew(i - 1)

        @pl.when(i >= AHEAD)
        def _():
            for copy in put(i - AHEAD):
                copy.wait()

        @pl.when(i == 0)
        def _():
            for later in range(2, AHEAD):
                for copy in fetch(jnp.int32(later)):
                    copy.start()

        @pl.when(i + AHEAD < n_blocks)
        def _():
            for copy in fetch(i + AHEAD):
                copy.start()

        @pl.when(i >= 1)
        def _():
            for copy in put(i - 1):
                copy.start()

        @pl.when((i >= 1) & (lax.rem(i, blocks_per_tile) == 0))
        def _():
            put_tile(i // blocks_per_tile - 1).start()

        k_copy, v_copy = fetch(i)
        @pl.when(i == 0)
        def _():
            for copy in small:
                copy.wait()

        k_copy.wait()
        v_copy.wait()
        state = []
        for one in range(PER):
            seq = i * PER + one
            pos = pos_ref[base + seq]
            q = q_ref[seq]
            raw = lax.dot_general(q, k_buf[slot_now, one], contract_last, preferred_element_type=F32)
            raw2 = lax.dot_general(q, kn_ref[seq], contract_last, preferred_element_type=F32)
            state.append((seq, pos, raw, raw2))
        soft = []
        for seq, pos, raw, raw2 in state:
            slot = first + (lane >> 1)
            ahead = (slot - pos) & (slots - 1)
            ok = ((lane & 1) == (sub >> 2)) & (slot < pos) & (ahead > (sub & 3))
            bias = jnp.where(ok, 0.0, NEG_BIG).astype(F32)
            new_slot = ((pos + new_step) & (slots - 1)) - first
            here = (new_slot >= 0) & (new_slot < rows // kvs)
            bias2 = jnp.where(new_ok & here, 0.0, NEG_BIG).astype(F32)
            score = raw.reshape(group, tile, rows) * coef + bias[None]
            score2 = raw2.reshape(group, tile, 16) * coef + bias2[None]
            top = jnp.maximum(jnp.max(score, axis=-1, keepdims=True), jnp.max(score2, axis=-1, keepdims=True))
            top = jnp.maximum(top, NEG_HALF)
            w = jnp.exp2(score - top)
            w2 = jnp.exp2(score2 - top)
            total = jnp.sum(w, axis=-1, keepdims=True) + jnp.sum(w2, axis=-1, keepdims=True)
            soft.append((top, total, w.reshape(per_row, rows).astype(BF16), w2.reshape(per_row, 16).astype(BF16)))
        for one in range(PER):
            seq, pos = state[one][:2]
            top, total, w, w2 = soft[one]
            out = jnp.dot(w, v_buf[slot_now, one], preferred_element_type=F32)
            out = out + jnp.dot(w2, vn_ref[seq], preferred_element_type=F32)
            some = total > 0.0
            safe = jnp.where(some, total, 1.0)
            lse = jnp.where(some, top + jnp.log2(safe), NEG_BIG)
            out = out.reshape(group, tile, LANES) * (1.0 / safe)
            stats = jnp.zeros((tile, LANES), F32)
            for n in range(group):
                stats = jnp.where(stat_lane == n, lse[n], stats)
            seat = lax.rem(i, blocks_per_tile) * PER + one
            o_rows[pl.ds(pl.multiple_of(seat * per_row, 8), per_row), :] = out.reshape(per_row, LANES)
            stat_rows[pl.ds(pl.multiple_of(seat * tile, 8), tile), :] = stats
        @pl.when(lax.rem(i, blocks_per_tile) == blocks_per_tile - 1)
        def _():
            t = i // blocks_per_tile
            for s in range(steps):
                o_tile[t, s, :, lse_cols] = sum(stat_rows[pl.ds(h * steps + s, 8, stride=tile), :] for h in range(kvs))
                for h in range(kvs):
                    for n in range(group):
                        col = (h * group + n) * LANES
                        o_tile[t, s, :, col:col + LANES] = o_rows[pl.ds(n * tile + h * steps + s, 8, stride=per_row), :]

    renew(jnp.int32(n_blocks - 1))
    for copy in put(n_blocks - 1):
        copy.start()
    tiles = n_blocks // blocks_per_tile
    put_tile(tiles - 1).start()
    for j in range(AHEAD):
        for copy in put(n_blocks - AHEAD + j):
            copy.wait()
    for t in range(tiles):
        put_tile(t).wait()


def attend(positions, q, k_new, v_new, k_rows, v_rows, steps, kvs, group, slots, handed=()):
    batch, rows, dim = k_rows.shape
    half = batch // 2
    hbm = pl.BlockSpec(memory_space=pl.ANY)
    return pl.pallas_call(
        functools.partial(attend_kernel, (steps, kvs, group, slots, half // PER, bool(handed))),
        in_specs=[pl.BlockSpec(memory_space=pltpu.SMEM)] + [hbm] * (5 + len(handed)),
        out_specs=[hbm, hbm, hbm],
        out_shape=[
            jax.ShapeDtypeStruct(k_rows.shape, BF16),
            jax.ShapeDtypeStruct(v_rows.shape, BF16),
            jax.ShapeDtypeStruct((steps, half, (kvs * group + 1) * dim), F32),
        ],
        input_output_aliases={6: 0, 7: 1} if handed else {},
        scratch_shapes=[
            pltpu.VMEM((DEPTH, PER, rows, dim), BF16),
            pltpu.VMEM((DEPTH, PER, rows, dim), BF16),
            pltpu.VMEM((half, q.shape[1], dim), BF16),
            pltpu.VMEM((half, k_new.shape[1], dim), BF16),
            pltpu.VMEM((half, v_new.shape[1], dim), BF16),
            pltpu.VMEM((half // 8, steps, 8, (kvs * group + 1) * dim), F32),
            pltpu.VMEM((8 * q.shape[1], dim), F32),
            pltpu.VMEM((8 * steps * kvs, dim), F32),
            pltpu.SemaphoreType.DMA((DEPTH,)),
            pltpu.SemaphoreType.DMA((DEPTH,)),
            pltpu.SemaphoreType.DMA((DEPTH,)),
            pltpu.SemaphoreType.DMA((DEPTH,)),
            pltpu.SemaphoreType.DMA((3,)),
            pltpu.SemaphoreType.DMA((half // 8,)),
        ],
        compiler_params=pltpu.CompilerParams(vmem_limit_bytes=VMEM_CAP),
        cost_estimate=pl.CostEstimate(flops=20_000_000_000, bytes_accessed=4 * batch * rows * dim,
                                      transcendentals=half * rows * q.shape[1]),
        name="attend_own" if handed else "attend_peer",
    )(positions, q, k_new, v_new, k_rows, v_rows, *handed)


CHUNK = 512
PIECE = 256
RING = 9
WO_SLOTS = 3
(C_OWN_O, C_X_O, C_OWN_E, C_X_E, C_HID_A, C_HID_B) = range(6)
(W_CORE, W_Y, J_CORE, J_Y, J_OWN_X, J_OWN_C, J_FWD_C) = range(7)


def tail_kernel(cfg, own_hbm, xin_hbm, x_hbm, wo_hbm, wfc_hbm, wproj_hbm, bo_ref, gain_ref, shift_ref, bfc_ref, bproj_ref,
                y_ref,
                my_own, my_x, my_own_e, my_x_e, sib_own, sib_x, sib_own_e, sib_x_e, a_buf, w_part, w_core, w_half, w_y, x_buf, x_mid, hid, hid_b,
                ring, g_buf, p_part, p_core, p_half, p_y, y_all, bo_rows, bfc_rows, bproj_rows,
                send_a, recv_a, send_j, recv_j, local_sem, wo_sem, x_sem, ring_sem):
    steps, batch, group, chunks, kvs = cfg
    half = batch // 2
    pair = steps // 2 * half
    head_cols = group * LANES
    ff_own = wfc_hbm.shape[1] // 2
    pieces = chunks * CHUNK // PIECE
    per = CHUNK // PIECE
    y = lax.axis_index("tp")
    sq = lax.axis_index("sq")
    x, c = sq // 2, sq % 2
    sib = {"sq": x * 2 + 1 - c}
    xpeer = {"sq": (1 - x) * 2 + c}
    ypeer = {"tp": 1 - y}
    MESH = pl.DeviceIdType.MESH

    barrier = pltpu.get_barrier_semaphore()
    for who in (sib, xpeer, ypeer):
        pl.semaphore_signal(barrier, inc=1, device_id=who, device_id_type=MESH)

    def chunk_cols(j):
        return pl.ds(pl.multiple_of(j * CHUNK, CHUNK), CHUNK)

    def load_item(item, slot):
        @pl.when(item < chunks)
        def _():
            col = pl.multiple_of(c * ff_own + item * CHUNK, CHUNK)
            pltpu.make_async_copy(wfc_hbm.at[:, pl.ds(col, CHUNK)], ring.at[slot], ring_sem.at[slot]).start()

        @pl.when(item >= chunks)
        def _():
            row = pl.multiple_of(c * ff_own, CHUNK)
            pltpu.make_async_copy(wproj_hbm.at[pl.ds(row, ff_own), chunk_cols(item - chunks)], ring.at[slot], ring_sem.at[slot]).start()

    def wait_item(slot):
        pltpu.make_async_copy(wfc_hbm.at[:, pl.ds(0, CHUNK)], ring.at[slot], ring_sem.at[slot]).wait()

    wo_rows = pl.ds(pl.multiple_of(c * head_cols, LANES), head_cols)
    per_slot = ring.shape[1] // head_cols

    def wo_place(j):
        return ring.at[j // per_slot, pl.ds(pl.multiple_of(lax.rem(j, per_slot) * head_cols, LANES), head_cols), :]

    def wo_copy(j):
        return pltpu.make_async_copy(wo_hbm.at[wo_rows, chunk_cols(j)], wo_place(j), wo_sem.at[j])

    def slot_of(item):
        return lax.rem(item + WO_SLOTS, RING)

    my_cols = pl.ds(pl.multiple_of(c * head_cols, LANES), head_cols)
    stat_cols = slice(kvs * head_cols, kvs * head_cols + LANES)
    locals_ = [pltpu.make_async_copy(src, dst, local_sem.at[n]) for n, (src, dst) in enumerate((
        (own_hbm.at[:, :, stat_cols], my_own_e), (xin_hbm.at[:, :, stat_cols], my_x_e),
        (own_hbm.at[:, :, my_cols], my_own), (xin_hbm.at[:, :, my_cols], my_x)))]
    for copy in locals_:
        copy.start()
    x_copy = pltpu.make_async_copy(x_hbm.at[pl.ds(2 * c, 2), pl.ds(pl.multiple_of(x * half, 8), half), :], x_buf, x_sem)
    x_copy.start()
    pl.semaphore_wait(barrier, 3)

    def remote(src, dst, kind, who):
        return pltpu.make_async_remote_copy(src_ref=src, dst_ref=dst, send_sem=send_a.at[kind], recv_sem=recv_a.at[kind],
                                            device_id=who, device_id_type=MESH)

    sib_cols = pl.ds(pl.multiple_of((1 - c) * head_cols, LANES), head_cols)
    swaps = [remote(own_hbm.at[:, :, stat_cols], sib_own_e, C_OWN_E, sib), remote(xin_hbm.at[:, :, stat_cols], sib_x_e, C_X_E, sib),
             remote(own_hbm.at[:, :, sib_cols], sib_own, C_OWN_O, sib), remote(xin_hbm.at[:, :, sib_cols], sib_x, C_X_O, sib)]
    for copy in swaps:
        copy.start()
    for j in range(chunks):
        wo_copy(jnp.int32(j)).start()
    bo_rows[...] = bo_ref[...].astype(F32)
    bfc_rows[...] = bfc_ref[...].astype(F32)
    bproj_rows[...] = bproj_ref[...].astype(F32)

    def flat(block):
        return block.reshape(steps * half, LANES)

    def my_lanes(stat):
        stat = flat(stat)
        return jnp.where(c == 0, stat, pltpu.roll(stat, LANES - group, 1))

    for copy in locals_:
        copy.wait()
    swaps[0].wait_recv()
    swaps[1].wait_recv()
    logs = [my_lanes(my_own_e[...]), my_lanes(sib_own_e[...]), my_lanes(my_x_e[...]), my_lanes(sib_x_e[...])]
    top = functools.reduce(jnp.maximum, logs)
    shares = [jnp.exp2(e - top) for e in logs]
    inv = 1.0 / sum(shares)
    shares = [w * inv for w in shares]
    swaps[2].wait_recv()
    swaps[3].wait_recv()
    for i in range(group):
        cols = slice(i * LANES, (i + 1) * LANES)
        parts = [part[:, :, cols] for part in (my_own, sib_own, my_x, sib_x)]
        a_buf[:, cols] = sum(w[:, i:i + 1] * flat(part) for w, part in zip(shares, parts)).astype(BF16)

    def jcopy(src, dst, kind, j, who):
        return pltpu.make_async_remote_copy(src_ref=src, dst_ref=dst, send_sem=send_j.at[kind, j], recv_sem=recv_j.at[kind, j],
                                            device_id=who, device_id_type=MESH)

    def pair_rows(core):
        return pl.ds(pl.multiple_of(core * pair, 8), pair)

    def to_core(part, inbox, kind, j):
        return jcopy(part.at[j, pair_rows(1 - c), :], inbox.at[j], kind, j, sib)

    def to_y(total, inbox, kind, j):
        return jcopy(total.at[j], inbox.at[j], kind, j, ypeer)

    def core_sum(part, inbox, total, inbox_y, kind, kind_y, j):
        to_core(part, inbox, kind, j).wait_recv()
        total[j] = part[j, pair_rows(c), :] + inbox[j]
        to_y(total, inbox_y, kind_y, j).start()

    def bias_of(rows, j, width):
        n = width // LANES
        return jnp.concatenate([rows[pl.ds(j * n + e, 1), :] for e in range(n)], axis=-1)

    def piece_cols(u):
        return pl.ds(pl.multiple_of(u * PIECE, PIECE), PIECE)

    def send_product(product, part, inbox, kind, j):
        for e in range(per):
            part[j * per + e] = product[:, e * PIECE:(e + 1) * PIECE]
        for e in range(per):
            to_core(part, inbox, kind, j * per + e).start()

    def y_sum(total, inbox):
        low = jnp.where(y == 0, total, inbox)
        high = jnp.where(y == 0, inbox, total)
        return low + high

    def stage(it, lag, body):
        u = it - lag

        @pl.when((u >= 0) & (u < pieces))
        def _():
            body(u)

    def product_stage(it, body):
        @pl.when((it < pieces) & (lax.rem(it, per) == 0))
        def _():
            body(it // per)

    def o_product(j):
        wo_copy(j).wait()
        product = jnp.dot(a_buf[...], wo_place(j)[...], preferred_element_type=F32)
        send_product(product, w_part, w_core, W_CORE, j)

    def o_core_sum(j):
        core_sum(w_part, w_core, w_half, w_y, W_CORE, W_Y, j)

    for k in range(RING - WO_SLOTS):
        load_item(jnp.int32(k), slot_of(k))

    @pl.loop(0, pieces + 6)
    def _(it):
        product_stage(it, o_product)
        stage(it, 6, o_core_sum)

    for k in range(RING - WO_SLOTS, RING):
        load_item(jnp.int32(k), slot_of(k))
    x_copy.wait()

    @pl.loop(0, pieces)
    def _(u):
        cols = piece_cols(u)
        to_y(w_half, w_y, W_Y, u).wait_recv()
        x_in = x_buf[:, :, cols].astype(F32).reshape(pair, PIECE)
        x_mid[:, cols] = (x_in + y_sum(w_half[u], w_y[u]) + bias_of(bo_rows, u, PIECE)).astype(BF16).astype(F32)

    gain = gain_ref[...].astype(F32)
    shift = shift_ref[...].astype(F32)
    d_model = x_mid.shape[1]
    hid_copies = []
    for part in range(2):
        src = slice(part * half, (part + 1) * half)
        dst = pl.ds(pl.multiple_of(c * pair + part * half, 8), half)
        rows = x_mid[src, :]
        mean = jnp.mean(rows, axis=-1, keepdims=True)
        cent = rows - mean
        rstd = lax.rsqrt(jnp.mean(cent * cent, axis=-1, keepdims=True) + LN_EPS)
        for n in range(d_model // LANES):
            cols = slice(n * LANES, (n + 1) * LANES)
            hid[dst, cols] = (cent[:, cols] * rstd * gain[n:n + 1, :] + shift[n:n + 1, :]).astype(BF16).astype(F32)
        copy = remote(hid.at[dst, :], hid.at[dst, :], (C_HID_A, C_HID_B)[part], sib)
        copy.start()
        hid_copies.append(copy)
    for copy in hid_copies:
        copy.wait_recv()
    hid_b[...] = hid[...].astype(BF16)

    together = 3

    @pl.loop(0, chunks // together)
    def _(first):
        group_of = [first * together + e for e in range(together)]
        for j in group_of:
            wait_item(slot_of(j))
        for j in group_of:
            pre = jnp.dot(hid_b[...], ring[slot_of(j)], preferred_element_type=F32) + bias_of(bfc_rows, c * chunks + j, CHUNK)
            cube = pre * pre * pre
            act = 0.5 * pre * (1.0 + jnp.tanh(math.sqrt(2.0 / math.pi) * (pre + 0.044715 * cube)))
            g_buf[:, chunk_cols(j)] = act.astype(BF16)
        for j in group_of:
            load_item(j + RING, slot_of(j))

    def block(j, core, xx):
        return y_all.at[j, pl.ds(2 * core, 2), pl.ds(pl.multiple_of(xx * half, 8), half), :]

    def spread(kind, j):
        ref, who = {J_OWN_X: (block(j, c, x), xpeer), J_OWN_C: (block(j, c, x), sib), J_FWD_C: (block(j, c, 1 - x), sib)}[kind]
        return jcopy(ref, ref, kind, j, who)

    def do_product(j):
        item = chunks + j
        slot = slot_of(item)
        wait_item(slot)
        product = jnp.dot(g_buf[...], ring[slot], preferred_element_type=F32)
        send_product(product, p_part, p_core, J_CORE, j)

        @pl.when(item + RING < 2 * chunks)
        def _():
            load_item(item + RING, slot)

    def do_core_sum(j):
        core_sum(p_part, p_core, p_half, p_y, J_CORE, J_Y, j)

    def do_y_sum(j):
        to_y(p_half, p_y, J_Y, j).wait_recv()
        full = x_mid[:, piece_cols(j)] + y_sum(p_half[j], p_y[j]) + bias_of(bproj_rows, j, PIECE)
        y_all[j, pl.ds(2 * c, 2), pl.ds(pl.multiple_of(x * half, 8), half), :] = full.astype(BF16).astype(F32).reshape(2, half, PIECE)
        spread(J_OWN_X, j).start()
        spread(J_OWN_C, j).start()

    def do_forward(j):
        spread(J_OWN_X, j).wait_recv()
        spread(J_FWD_C, j).start()

    def do_store(j):
        spread(J_OWN_C, j).wait_recv()
        spread(J_FWD_C, j).wait_recv()
        y_ref[:, :, piece_cols(j)] = y_all[j].astype(BF16)

    @pl.loop(0, pieces + 13)
    def _(it):
        product_stage(it, do_product)
        stage(it, 2, do_core_sum)
        stage(it, 7, do_y_sum)
        stage(it, 11, do_forward)
        stage(it, 13, do_store)

    for copy in swaps + hid_copies:
        copy.wait_send()

    @pl.loop(0, pieces)
    def _(j):
        to_core(w_part, w_core, W_CORE, j).wait_send()
        to_y(w_half, w_y, W_Y, j).wait_send()
        to_core(p_part, p_core, J_CORE, j).wait_send()
        to_y(p_half, p_y, J_Y, j).wait_send()
        for kind in (J_OWN_X, J_OWN_C, J_FWD_C):
            spread(kind, j).wait_send()


def tail(own, x_in, x_steps, w_o, w_fc, w_proj, b_o, gain, shift, b_fc, b_proj, group, kvs):
    steps, half, _ = own.shape
    batch = 2 * half
    rows = steps * half
    pair = rows // 2
    d_model = w_o.shape[1]
    chunks = d_model // CHUNK
    pieces = d_model // PIECE
    ff_own = w_fc.shape[1] // 2
    assert ff_own == d_model and steps == 4 and kvs == 2
    head_cols = group * LANES
    vm = pl.BlockSpec(memory_space=pltpu.VMEM)
    hbm = pl.BlockSpec(memory_space=pl.ANY)
    cfg = (steps, batch, group, chunks, kvs)
    tiles = lambda vec: vec.reshape(-1, LANES)
    scratch = [
        pltpu.VMEM((steps, half, head_cols), F32),
        pltpu.VMEM((steps, half, head_cols), F32),
        pltpu.VMEM((steps, half, LANES), F32),
        pltpu.VMEM((steps, half, LANES), F32),
        pltpu.VMEM((steps, half, head_cols), F32),
        pltpu.VMEM((steps, half, head_cols), F32),
        pltpu.VMEM((steps, half, LANES), F32),
        pltpu.VMEM((steps, half, LANES), F32),
        pltpu.VMEM((rows, head_cols), BF16),
        pltpu.VMEM((pieces, rows, PIECE), F32),
        pltpu.VMEM((pieces, pair, PIECE), F32),
        pltpu.VMEM((pieces, pair, PIECE), F32),
        pltpu.VMEM((pieces, pair, PIECE), F32),
        pltpu.VMEM((2, half, d_model), BF16),
        pltpu.VMEM((pair, d_model), F32),
        pltpu.VMEM((rows, d_model), F32),
        pltpu.VMEM((rows, d_model), BF16),
        pltpu.VMEM((RING, d_model, CHUNK), BF16),
        pltpu.VMEM((rows, ff_own), BF16),
        pltpu.VMEM((pieces, rows, PIECE), F32),
        pltpu.VMEM((pieces, pair, PIECE), F32),
        pltpu.VMEM((pieces, pair, PIECE), F32),
        pltpu.VMEM((pieces, pair, PIECE), F32),
        pltpu.VMEM((pieces, steps, batch, PIECE), F32),
        pltpu.VMEM((d_model // LANES, LANES), F32),
        pltpu.VMEM((2 * ff_own // LANES, LANES), F32),
        pltpu.VMEM((d_model // LANES, LANES), F32),
        pltpu.SemaphoreType.DMA((6,)),
        pltpu.SemaphoreType.DMA((6,)),
        pltpu.SemaphoreType.DMA((7, pieces)),
        pltpu.SemaphoreType.DMA((7, pieces)),
        pltpu.SemaphoreType.DMA((4,)),
        pltpu.SemaphoreType.DMA((chunks,)),
        pltpu.SemaphoreType.DMA,
        pltpu.SemaphoreType.DMA((RING,)),
    ]
    return pl.pallas_call(
        functools.partial(tail_kernel, cfg),
        out_shape=pltpu.VMEM((steps, batch, d_model), BF16),
        in_specs=[hbm] * 6 + [vm] * 5,
        out_specs=vm,
        scratch_shapes=scratch,
        compiler_params=pltpu.CompilerParams(collective_id=0, has_side_effects=True, vmem_limit_bytes=TAIL_VMEM),
        cost_estimate=pl.CostEstimate(flops=2 * rows * d_model * (head_cols + 2 * ff_own), bytes_accessed=100_000_000, transcendentals=0),
        name="tail",
    )(own, x_in, x_steps, w_o, w_fc, w_proj, tiles(b_o), tiles(gain), tiles(shift), tiles(b_fc), tiles(b_proj))


def solution(mesh):
    sq_size = mesh.shape["sq"]
    act_spec = P(None, "dp", None)
    cache_spec = P("dp", "sq", "tp", None)
    col_spec = P(None, "tp")
    row_spec = P("tp", None)
    vec_spec = P("tp")
    rep_spec = P(None)
    in_specs = (act_spec, P("dp"), cache_spec, cache_spec, col_spec, vec_spec, col_spec, vec_spec,
                col_spec, vec_spec, row_spec, rep_spec, rep_spec, rep_spec, rep_spec, rep_spec,
                col_spec, vec_spec, row_spec, rep_spec)
    out_specs = (act_spec, cache_spec, cache_spec)

    def per_device(x_steps, positions, key_buf, val_buf, w_q, b_q, w_k, b_k, w_v, b_v, w_o, b_o,
                   ln1_gain, ln1_bias, ln2_gain, ln2_bias, w_fc, b_fc, w_proj, b_proj):
        steps, batch, d_model = x_steps.shape
        slots_local, kvs, dim = key_buf.shape[1], key_buf.shape[2], key_buf.shape[3]
        slots = slots_local * sq_size
        group = w_q.shape[1] // (kvs * dim)
        q_rows, k_new, v_new = front(positions, x_steps, ln1_gain, ln1_bias, b_q, b_k, b_v, w_q, w_k, w_v, kvs)
        k_rows = key_buf.reshape(batch, slots_local * kvs, dim)
        v_rows = val_buf.reshape(batch, slots_local * kvs, dim)
        caches = (positions, q_rows, k_new, v_new, k_rows, v_rows, steps, kvs, group, slots)
        k_out, v_out, for_peer = attend(*caches)
        from_peer = lax.ppermute(for_peer, "sq", [(d, d ^ 2) for d in range(sq_size)])
        k_out, v_out, own = attend(*caches, handed=(k_out, v_out))
        ys = tail(own, from_peer, x_steps, w_o, w_fc, w_proj, b_o, ln2_gain, ln2_bias, b_fc, b_proj, group, kvs)
        return ys, k_out.reshape(key_buf.shape), v_out.reshape(val_buf.shape)

    return jax.shard_map(per_device, mesh=mesh, in_specs=in_specs, out_specs=out_specs, check_vma=False)
```

```python
import functools
import math

import jax
import jax.numpy as jnp
from jax import lax
from jax.experimental import pallas as pl
from jax.experimental.pallas import tpu as pltpu
from jax.sharding import PartitionSpec as P

ROPE_BASE = 1000000.0
LN_EPS = 1e-5
NEG_BIG = -1e30
NEG_HALF = -1e29
LOG2E = 1.4426950408889634
VMEM_CAP = 67_043_328
TAIL_VMEM = 64_900_000
F32 = jnp.float32
BF16 = jnp.bfloat16
LANES = 128


COLS = 384

def front_kernel(cfg, pos_ref, x_hbm, freq_ref, gain_ref, shift_ref, bq_ref, bk_ref, bv_ref, wq_hbm, wk_hbm, wv_hbm,
                 q_out, kn_out, vn_out, x_buf, hid, wq_buf, wkv_buf, mine, theirs, pos_rows, q_rows, kn_rows, vn_rows, bias_q,
                 sem, x_sem, send, recv):
    steps, kvs, group = cfg
    batch, d_model = x_buf.shape[1], x_buf.shape[2]
    head_cols = group * LANES
    per_row = group * kvs * steps
    sq = lax.axis_index("sq")
    c = sq % 2
    sib = {"sq": (sq // 2) * 2 + 1 - c}

    x_copies = [pltpu.make_async_copy(x_hbm.at[s], x_buf.at[s], x_sem.at[s]) for s in range(steps)]
    for copy in x_copies:
        copy.start()
    head_at = pl.multiple_of(c * LANES, LANES)
    n_q = head_cols // COLS
    w_copies = [pltpu.make_async_copy(wq_hbm.at[:, pl.ds(pl.multiple_of(c * head_cols + n * COLS, LANES), COLS)], wq_buf.at[n], sem.at[n])
                for n in range(n_q)]
    w_copies += [pltpu.make_async_copy(src.at[:, pl.ds(head_at, LANES)], wkv_buf.at[n], sem.at[n_q + n])
                 for n, src in enumerate((wk_hbm, wv_hbm))]
    for copy in w_copies[:2]:
        copy.start()

    barrier = pltpu.get_barrier_semaphore()
    pl.semaphore_signal(barrier, inc=1, device_id=sib, device_id_type=pl.DeviceIdType.MESH)
    pl.semaphore_wait(barrier, 1)

    for b in range(batch):
        pos_rows[b:b + 1, :] = jnp.full((1, LANES), pos_ref[b], jnp.int32).astype(F32)
    half = LANES // 2
    where = pos_rows[:, :half]
    angle = jnp.concatenate([where + float(s) for s in range(steps)], axis=0) * freq_ref[...]
    cos, sin = jnp.cos(angle), jnp.sin(angle)
    cos_full = jnp.concatenate([cos, cos], axis=-1)
    sin_full = jnp.concatenate([-sin, sin], axis=-1)

    bias_q[...] = bq_ref[...].astype(F32)
    gain = gain_ref[...].astype(F32)
    shift = shift_ref[...].astype(F32)
    for s in range(steps):
        x_copies[s].wait()
        wide = x_buf[s].astype(F32)
        mean = jnp.mean(wide, axis=-1, keepdims=True)
        cent = wide - mean
        rstd = lax.rsqrt(jnp.mean(cent * cent, axis=-1, keepdims=True) + LN_EPS)
        for copy in {1: w_copies[2:3], 3: w_copies[3:]}.get(s, ()):
            copy.start()
        for n in range(d_model // LANES):
            cols = slice(n * LANES, (n + 1) * LANES)
            hid[s * batch:(s + 1) * batch, cols] = (cent[:, cols] * rstd * gain[n:n + 1, :] + shift[n:n + 1, :]).astype(BF16)

    def rotate(vec):
        return (vec * cos_full + pltpu.roll(vec, half, 1) * sin_full).astype(BF16).astype(F32)

    def swap(n):
        return pltpu.make_async_remote_copy(src_ref=mine.at[n], dst_ref=theirs.at[n], send_sem=send.at[n], recv_sem=recv.at[n],
                                            device_id=sib, device_id_type=pl.DeviceIdType.MESH)

    def place(n, core, block):
        for s in range(steps):
            rows = block[s * batch:(s + 1) * batch, :]
            if n < group:
                q_rows[pl.ds(n * kvs * steps + core * steps + s, batch, stride=per_row), :] = rows
            elif n == group:
                kn_rows[pl.ds(s * kvs + core, batch, stride=16), :] = rows
            else:
                vn_rows[pl.ds(s * kvs + core, batch, stride=16), :] = rows

    kn_rows[...] = jnp.zeros_like(kn_rows)
    vn_rows[...] = jnp.zeros_like(vn_rows)
    kv_bias = [jnp.where(c == 0, ref[0:1, :].astype(F32), ref[1:2, :].astype(F32)) for ref in (bk_ref, bv_ref)]
    total = group + 2
    per = COLS // LANES
    groups = [(range(n * per, (n + 1) * per), wq_buf.at[n], w_copies[n]) for n in range(n_q)]
    groups += [((group + n,), wkv_buf.at[n], w_copies[n_q + n]) for n in range(2)]
    for heads, weight, copy in groups:
        copy.wait()
        block = jnp.dot(hid[...], weight[...], preferred_element_type=F32)
        for at, n in enumerate(heads):
            bias = bias_q[pl.ds(c * group + n, 1), :] if n < group else kv_bias[n - group]
            vec = (block[:, at * LANES:(at + 1) * LANES] + bias).astype(BF16).astype(F32)
            mine[n] = rotate(vec) if n <= group else vec
            swap(n).start()
            place(n, c, mine.at[n])
    for n in range(total):
        swap(n).wait_recv()
        place(n, 1 - c, theirs.at[n])

    kn_out[...] = kn_rows[...].reshape(kn_out.shape).astype(BF16)
    vn_out[...] = vn_rows[...].reshape(vn_out.shape).astype(BF16)

    @pl.loop(0, batch)
    def _(b):
        q_out[b] = q_rows[pl.ds(pl.multiple_of(b * per_row, 8), per_row), :].astype(BF16)

    for n in range(total):
        swap(n).wait_send()


def front(positions, x_steps, gain, shift, b_q, b_k, b_v, w_q, w_k, w_v, kvs):
    steps, batch, d_model = x_steps.shape
    heads = w_q.shape[1] // LANES
    group = heads // kvs
    rows = group * kvs * steps
    assert kvs == 2
    inv_freq = jnp.power(F32(ROPE_BASE), -2.0 * jnp.arange(LANES // 2, dtype=F32) / LANES).reshape(1, -1)
    vm = pl.BlockSpec(memory_space=pltpu.VMEM)
    hbm = pl.BlockSpec(memory_space=pl.ANY)
    tiles = lambda vec: vec.reshape(-1, LANES)
    return pl.pallas_call(
        functools.partial(front_kernel, (steps, kvs, group)),
        out_shape=[
            jax.ShapeDtypeStruct((batch, rows, LANES), BF16),
            jax.ShapeDtypeStruct((batch, 16, LANES), BF16),
            jax.ShapeDtypeStruct((batch, 16, LANES), BF16),
        ],
        in_specs=[pl.BlockSpec(memory_space=pltpu.SMEM), hbm] + [vm] * 6 + [hbm] * 3,
        out_specs=[vm] * 3,
        scratch_shapes=[
            pltpu.VMEM((steps, batch, d_model), BF16),
            pltpu.VMEM((steps * batch, d_model), BF16),
            pltpu.VMEM((group * LANES // COLS, d_model, COLS), BF16),
            pltpu.VMEM((2, d_model, LANES), BF16),
            pltpu.VMEM((group + 2, steps * batch, LANES), F32),
            pltpu.VMEM((group + 2, steps * batch, LANES), F32),
            pltpu.VMEM((batch, LANES), F32),
            pltpu.VMEM((batch * rows, LANES), F32),
            pltpu.VMEM((batch * 16, LANES), F32),
            pltpu.VMEM((batch * 16, LANES), F32),
            pltpu.VMEM((heads, LANES), F32),
            pltpu.SemaphoreType.DMA((group + 2,)),
            pltpu.SemaphoreType.DMA((steps,)),
            pltpu.SemaphoreType.DMA((group + 2,)),
            pltpu.SemaphoreType.DMA((group + 2,)),
        ],
        compiler_params=pltpu.CompilerParams(collective_id=1, has_side_effects=True, vmem_limit_bytes=VMEM_CAP),
        cost_estimate=pl.CostEstimate(flops=steps * batch * d_model * (w_q.shape[1] + 2 * w_k.shape[1]),
                                      bytes_accessed=d_model * (w_q.shape[1] + 2 * w_k.shape[1]), transcendentals=0),
        name="front",
    )(positions, x_steps, inv_freq, tiles(gain), tiles(shift), tiles(b_q), tiles(b_k), tiles(b_v), w_q, w_k, w_v)


PER = 2
DEPTH = 8
AHEAD = 4

def attend_kernel(cfg, pos_ref, q_hbm, kn_hbm, vn_hbm, k_hbm, v_hbm, *refs):
    steps, kvs, group, slots, n_blocks, own_half = cfg
    (ko_hbm, vo_hbm, o_hbm, k_buf, v_buf, q_ref, kn_ref, vn_ref, o_tile, o_rows, stat_rows,
     k_in, v_in, k_up, v_up, small_in, o_up) = refs[2 if own_half else 0:]
    x = lax.axis_index("sq") // 2
    base = (x if own_half else 1 - x) * (n_blocks * PER)
    lse_cols = slice(kvs * group * LANES, (kvs * group + 1) * LANES)
    rows = k_hbm.shape[1]
    tile = steps * kvs
    per_row = group * tile
    first = lax.axis_index("sq") * (rows // kvs)
    coef = LANES ** -0.5 * LOG2E
    contract_last = (((1,), (1,)), ((), ()))
    blocks_per_tile = 8 // PER

    def seqs(i):
        return pl.ds(base + i * PER, PER)

    def fetch(i):
        slot = lax.rem(i, DEPTH)
        return (pltpu.make_async_copy(k_hbm.at[seqs(i)], k_buf.at[slot], k_in.at[slot]),
                pltpu.make_async_copy(v_hbm.at[seqs(i)], v_buf.at[slot], v_in.at[slot]))

    def put(i):
        slot = lax.rem(i, DEPTH)
        return (pltpu.make_async_copy(k_buf.at[slot], ko_hbm.at[seqs(i)], k_up.at[slot]),
                pltpu.make_async_copy(v_buf.at[slot], vo_hbm.at[seqs(i)], v_up.at[slot]))

    half_seqs = pl.ds(base, n_blocks * PER)
    small = [pltpu.make_async_copy(src.at[half_seqs], dst, small_in.at[n])
             for n, (src, dst) in enumerate(((q_hbm, q_ref), (kn_hbm, kn_ref), (vn_hbm, vn_ref)))]
    for copy in small:
        copy.start()
    for i in range(2):
        for copy in fetch(jnp.int32(i)):
            copy.start()

    def put_tile(t):
        return pltpu.make_async_copy(o_tile.at[t], o_hbm.at[:, pl.ds(pl.multiple_of(t * 8, 8), 8), :], o_up.at[t])

    sub = lax.broadcasted_iota(jnp.int32, (tile, rows), 0)
    lane = lax.broadcasted_iota(jnp.int32, (tile, rows), 1)
    sub2 = lax.broadcasted_iota(jnp.int32, (tile, 16), 0)
    lane2 = lax.broadcasted_iota(jnp.int32, (tile, 16), 1)
    new_step = lane2 // kvs
    new_ok = ((lane2 % kvs) == (sub2 // steps)) & (new_step <= sub2 % steps)
    stat_sub = lax.broadcasted_iota(jnp.int32, (tile, LANES), 0)
    stat_lane = lax.broadcasted_iota(jnp.int32, (tile, LANES), 1) - (stat_sub // steps) * group
    win_row = lax.broadcasted_iota(jnp.int32, (32, LANES), 0)

    def renew(i):
        slot_of = lax.rem(i, DEPTH)
        for one in range(PER):
            seq = i * PER + one
            goal = kvs * ((pos_ref[base + seq] & (slots - 1)) - first)
            goal = jnp.where(goal > kvs * (slots - steps), goal - kvs * slots, goal)
            start = pl.multiple_of(jnp.clip((goal >> 4) << 4, 0, rows - 32), 16)
            offset = win_row + (start - goal)
            for buf, new in ((k_buf, kn_ref), (v_buf, vn_ref)):
                fresh = new[seq].astype(F32)
                window = buf[slot_of, one, pl.ds(start, 32), :].astype(F32)
                for r in range(tile):
                    window = jnp.where(offset == r, fresh[r:r + 1, :], window)
                buf[slot_of, one, pl.ds(start, 32), :] = window.astype(BF16)

    @pl.loop(0, n_blocks)
    def _(i):
        slot_now = lax.rem(i, DEPTH)

        @pl.when(i >= 1)
        def _():
            renew(i - 1)

        @pl.when(i >= AHEAD)
        def _():
            for copy in put(i - AHEAD):
                copy.wait()

        @pl.when(i == 0)
        def _():
            for later in range(2, AHEAD):
                for copy in fetch(jnp.int32(later)):
                    copy.start()

        @pl.when(i + AHEAD < n_blocks)
        def _():
            for copy in fetch(i + AHEAD):
                copy.start()

        @pl.when(i >= 1)
        def _():
            for copy in put(i - 1):
                copy.start()

        @pl.when((i >= 1) & (lax.rem(i, blocks_per_tile) == 0))
        def _():
            put_tile(i // blocks_per_tile - 1).start()

        k_copy, v_copy = fetch(i)
        @pl.when(i == 0)
        def _():
            for copy in small:
                copy.wait()

        k_copy.wait()
        v_copy.wait()
        state = []
        for one in range(PER):
            seq = i * PER + one
            pos = pos_ref[base + seq]
            q = q_ref[seq]
            raw = lax.dot_general(q, k_buf[slot_now, one], contract_last, preferred_element_type=F32)
            raw2 = lax.dot_general(q, kn_ref[seq], contract_last, preferred_element_type=F32)
            state.append((seq, pos, raw, raw2))
        soft = []
        for seq, pos, raw, raw2 in state:
            slot = first + (lane >> 1)
            ahead = (slot - pos) & (slots - 1)
            ok = ((lane & 1) == (sub >> 2)) & (slot < pos) & (ahead > (sub & 3))
            bias = jnp.where(ok, 0.0, NEG_BIG).astype(F32)
            new_slot = ((pos + new_step) & (slots - 1)) - first
            here = (new_slot >= 0) & (new_slot < rows // kvs)
            bias2 = jnp.where(new_ok & here, 0.0, NEG_BIG).astype(F32)
            score = raw.reshape(group, tile, rows) * coef + bias[None]
            score2 = raw2.reshape(group, tile, 16) * coef + bias2[None]
            top = jnp.maximum(jnp.max(score, axis=-1, keepdims=True), jnp.max(score2, axis=-1, keepdims=True))
            top = jnp.maximum(top, NEG_HALF)
            w = jnp.exp2(score - top)
            w2 = jnp.exp2(score2 - top)
            total = jnp.sum(w, axis=-1, keepdims=True) + jnp.sum(w2, axis=-1, keepdims=True)
            soft.append((top, total, w.reshape(per_row, rows).astype(BF16), w2.reshape(per_row, 16).astype(BF16)))
        for one in range(PER):
            seq, pos = state[one][:2]
            top, total, w, w2 = soft[one]
            out = jnp.dot(w, v_buf[slot_now, one], preferred_element_type=F32)
            out = out + jnp.dot(w2, vn_ref[seq], preferred_element_type=F32)
            some = total > 0.0
            safe = jnp.where(some, total, 1.0)
            lse = jnp.where(some, top + jnp.log2(safe), NEG_BIG)
            out = out.reshape(group, tile, LANES) * (1.0 / safe)
            stats = jnp.zeros((tile, LANES), F32)
            for n in range(group):
                stats = jnp.where(stat_lane == n, lse[n], stats)
            seat = lax.rem(i, blocks_per_tile) * PER + one
            o_rows[pl.ds(pl.multiple_of(seat * per_row, 8), per_row), :] = out.reshape(per_row, LANES)
            stat_rows[pl.ds(pl.multiple_of(seat * tile, 8), tile), :] = stats
        @pl.when(lax.rem(i, blocks_per_tile) == blocks_per_tile - 1)
        def _():
            t = i // blocks_per_tile
            for s in range(steps):
                o_tile[t, s, :, lse_cols] = sum(stat_rows[pl.ds(h * steps + s, 8, stride=tile), :] for h in range(kvs))
                for h in range(kvs):
                    for n in range(group):
                        col = (h * group + n) * LANES
                        o_tile[t, s, :, col:col + LANES] = o_rows[pl.ds(n * tile + h * steps + s, 8, stride=per_row), :]

    renew(jnp.int32(n_blocks - 1))
    for copy in put(n_blocks - 1):
        copy.start()
    tiles = n_blocks // blocks_per_tile
    put_tile(tiles - 1).start()
    for j in range(AHEAD):
        for copy in put(n_blocks - AHEAD + j):
            copy.wait()
    for t in range(tiles):
        put_tile(t).wait()


def attend(positions, q, k_new, v_new, k_rows, v_rows, steps, kvs, group, slots, handed=()):
    batch, rows, dim = k_rows.shape
    half = batch // 2
    hbm = pl.BlockSpec(memory_space=pl.ANY)
    return pl.pallas_call(
        functools.partial(attend_kernel, (steps, kvs, group, slots, half // PER, bool(handed))),
        in_specs=[pl.BlockSpec(memory_space=pltpu.SMEM)] + [hbm] * (5 + len(handed)),
        out_specs=[hbm, hbm, hbm],
        out_shape=[
            jax.ShapeDtypeStruct(k_rows.shape, BF16),
            jax.ShapeDtypeStruct(v_rows.shape, BF16),
            jax.ShapeDtypeStruct((steps, half, (kvs * group + 1) * dim), F32),
        ],
        input_output_aliases={6: 0, 7: 1} if handed else {},
        scratch_shapes=[
            pltpu.VMEM((DEPTH, PER, rows, dim), BF16),
            pltpu.VMEM((DEPTH, PER, rows, dim), BF16),
            pltpu.VMEM((half, q.shape[1], dim), BF16),
            pltpu.VMEM((half, k_new.shape[1], dim), BF16),
            pltpu.VMEM((half, v_new.shape[1], dim), BF16),
            pltpu.VMEM((half // 8, steps, 8, (kvs * group + 1) * dim), F32),
            pltpu.VMEM((8 * q.shape[1], dim), F32),
            pltpu.VMEM((8 * steps * kvs, dim), F32),
            pltpu.SemaphoreType.DMA((DEPTH,)),
            pltpu.SemaphoreType.DMA((DEPTH,)),
            pltpu.SemaphoreType.DMA((DEPTH,)),
            pltpu.SemaphoreType.DMA((DEPTH,)),
            pltpu.SemaphoreType.DMA((3,)),
            pltpu.SemaphoreType.DMA((half // 8,)),
        ],
        compiler_params=pltpu.CompilerParams(vmem_limit_bytes=VMEM_CAP),
        cost_estimate=pl.CostEstimate(flops=20_000_000_000, bytes_accessed=4 * batch * rows * dim,
                                      transcendentals=half * rows * q.shape[1]),
        name="attend_own" if handed else "attend_peer",
    )(positions, q, k_new, v_new, k_rows, v_rows, *handed)


CHUNK = 512
PIECE = 256
RING = 9
WO_SLOTS = 3
(C_OWN_O, C_X_O, C_OWN_E, C_X_E) = range(4)
(W_CORE, W_Y, J_CORE, J_Y, J_OWN_X, J_OWN_C, J_FWD_C, W_MID) = range(8)


def tail_kernel(cfg, own_hbm, xin_hbm, x_hbm, wo_hbm, wfc_hbm, wproj_hbm, bo_ref, gain_ref, shift_ref, bfc_ref, bproj_ref,
                y_ref,
                my_own, my_x, my_own_e, my_x_e, sib_own, sib_x, sib_own_e, sib_x_e, a_buf, w_part, w_core, w_half, w_y, x_buf, x_mid, hid, hid_b,
                ring, g_buf, p_part, p_core, p_half, p_y, y_all, bo_rows, bfc_rows, bproj_rows,
                send_a, recv_a, send_j, recv_j, local_sem, wo_sem, x_sem, ring_sem):
    steps, batch, group, chunks, kvs = cfg
    half = batch // 2
    pair = steps // 2 * half
    head_cols = group * LANES
    ff_own = wfc_hbm.shape[1] // 2
    pieces = chunks * CHUNK // PIECE
    per = CHUNK // PIECE
    y = lax.axis_index("tp")
    sq = lax.axis_index("sq")
    x, c = sq // 2, sq % 2
    sib = {"sq": x * 2 + 1 - c}
    xpeer = {"sq": (1 - x) * 2 + c}
    ypeer = {"tp": 1 - y}
    MESH = pl.DeviceIdType.MESH

    barrier = pltpu.get_barrier_semaphore()
    for who in (sib, xpeer, ypeer):
        pl.semaphore_signal(barrier, inc=1, device_id=who, device_id_type=MESH)

    def chunk_cols(j):
        return pl.ds(pl.multiple_of(j * CHUNK, CHUNK), CHUNK)

    def load_item(item, slot):
        @pl.when(item < chunks)
        def _():
            col = pl.multiple_of(c * ff_own + item * CHUNK, CHUNK)
            pltpu.make_async_copy(wfc_hbm.at[:, pl.ds(col, CHUNK)], ring.at[slot], ring_sem.at[slot]).start()

        @pl.when(item >= chunks)
        def _():
            row = pl.multiple_of(c * ff_own, CHUNK)
            pltpu.make_async_copy(wproj_hbm.at[pl.ds(row, ff_own), chunk_cols(item - chunks)], ring.at[slot], ring_sem.at[slot]).start()

    def wait_item(slot):
        pltpu.make_async_copy(wfc_hbm.at[:, pl.ds(0, CHUNK)], ring.at[slot], ring_sem.at[slot]).wait()

    wo_rows = pl.ds(pl.multiple_of(c * head_cols, LANES), head_cols)
    per_slot = ring.shape[1] // head_cols

    def wo_place(j):
        return ring.at[j // per_slot, pl.ds(pl.multiple_of(lax.rem(j, per_slot) * head_cols, LANES), head_cols), :]

    def wo_copy(j):
        return pltpu.make_async_copy(wo_hbm.at[wo_rows, chunk_cols(j)], wo_place(j), wo_sem.at[j])

    def slot_of(item):
        return lax.rem(item + WO_SLOTS, RING)

    my_cols = pl.ds(pl.multiple_of(c * head_cols, LANES), head_cols)
    stat_cols = slice(kvs * head_cols, kvs * head_cols + LANES)
    locals_ = [pltpu.make_async_copy(src, dst, local_sem.at[n]) for n, (src, dst) in enumerate((
        (own_hbm.at[:, :, stat_cols], my_own_e), (xin_hbm.at[:, :, stat_cols], my_x_e),
        (own_hbm.at[:, :, my_cols], my_own), (xin_hbm.at[:, :, my_cols], my_x)))]
    for copy in locals_:
        copy.start()
    x_copy = pltpu.make_async_copy(x_hbm.at[pl.ds(2 * c, 2), pl.ds(pl.multiple_of(x * half, 8), half), :], x_buf, x_sem)
    x_copy.start()
    pl.semaphore_wait(barrier, 3)

    def remote(src, dst, kind, who):
        return pltpu.make_async_remote_copy(src_ref=src, dst_ref=dst, send_sem=send_a.at[kind], recv_sem=recv_a.at[kind],
                                            device_id=who, device_id_type=MESH)

    sib_cols = pl.ds(pl.multiple_of((1 - c) * head_cols, LANES), head_cols)
    swaps = [remote(own_hbm.at[:, :, stat_cols], sib_own_e, C_OWN_E, sib), remote(xin_hbm.at[:, :, stat_cols], sib_x_e, C_X_E, sib),
             remote(own_hbm.at[:, :, sib_cols], sib_own, C_OWN_O, sib), remote(xin_hbm.at[:, :, sib_cols], sib_x, C_X_O, sib)]
    for copy in swaps:
        copy.start()
    for j in range(chunks):
        wo_copy(jnp.int32(j)).start()
    bo_rows[...] = bo_ref[...].astype(F32)
    bfc_rows[...] = bfc_ref[...].astype(F32)
    bproj_rows[...] = bproj_ref[...].astype(F32)

    def flat(block):
        return block.reshape(steps * half, LANES)

    def my_lanes(stat):
        stat = flat(stat)
        return jnp.where(c == 0, stat, pltpu.roll(stat, LANES - group, 1))

    for copy in locals_:
        copy.wait()
    swaps[0].wait_recv()
    swaps[1].wait_recv()
    logs = [my_lanes(my_own_e[...]), my_lanes(sib_own_e[...]), my_lanes(my_x_e[...]), my_lanes(sib_x_e[...])]
    top = functools.reduce(jnp.maximum, logs)
    shares = [jnp.exp2(e - top) for e in logs]
    inv = 1.0 / sum(shares)
    shares = [w * inv for w in shares]
    swaps[2].wait_recv()
    swaps[3].wait_recv()
    for i in range(group):
        cols = slice(i * LANES, (i + 1) * LANES)
        parts = [part[:, :, cols] for part in (my_own, sib_own, my_x, sib_x)]
        a_buf[:, cols] = sum(w[:, i:i + 1] * flat(part) for w, part in zip(shares, parts)).astype(BF16)

    def jcopy(src, dst, kind, j, who):
        return pltpu.make_async_remote_copy(src_ref=src, dst_ref=dst, send_sem=send_j.at[kind, j], recv_sem=recv_j.at[kind, j],
                                            device_id=who, device_id_type=MESH)

    def pair_rows(core):
        return pl.ds(pl.multiple_of(core * pair, 8), pair)

    def to_core(part, inbox, kind, j):
        return jcopy(part.at[j, pair_rows(1 - c), :], inbox.at[j], kind, j, sib)

    def to_y(total, inbox, kind, j):
        return jcopy(total.at[j], inbox.at[j], kind, j, ypeer)

    def core_sum(part, inbox, total, inbox_y, kind, kind_y, j):
        to_core(part, inbox, kind, j).wait_recv()
        total[j] = part[j, pair_rows(c), :] + inbox[j]
        to_y(total, inbox_y, kind_y, j).start()

    def bias_of(rows, j, width):
        n = width // LANES
        return jnp.concatenate([rows[pl.ds(j * n + e, 1), :] for e in range(n)], axis=-1)

    def piece_cols(u):
        return pl.ds(pl.multiple_of(u * PIECE, PIECE), PIECE)

    def send_product(product, part, inbox, kind, j):
        for e in range(per):
            part[j * per + e] = product[:, e * PIECE:(e + 1) * PIECE]
        for e in range(per):
            to_core(part, inbox, kind, j * per + e).start()

    def y_sum(total, inbox):
        low = jnp.where(y == 0, total, inbox)
        high = jnp.where(y == 0, inbox, total)
        return low + high

    def stage(it, lag, body):
        u = it - lag

        @pl.when((u >= 0) & (u < pieces))
        def _():
            body(u)

    def product_stage(it, body):
        @pl.when((it < pieces) & (lax.rem(it, per) == 0))
        def _():
            body(it // per)

    def o_product(j):
        wo_copy(j).wait()
        product = jnp.dot(a_buf[...], wo_place(j)[...], preferred_element_type=F32)
        send_product(product, w_part, w_core, W_CORE, j)

    def o_core_sum(j):
        core_sum(w_part, w_core, w_half, w_y, W_CORE, W_Y, j)

    for k in range(RING - WO_SLOTS):
        load_item(jnp.int32(k), slot_of(k))

    @pl.loop(0, pieces + 6)
    def _(it):
        product_stage(it, o_product)
        stage(it, 6, o_core_sum)

    for k in range(RING - WO_SLOTS, RING):
        load_item(jnp.int32(k), slot_of(k))
    x_copy.wait()

    def share_mid(u):
        piece = hid.at[pair_rows(c), piece_cols(u)]
        return jcopy(piece, piece, W_MID, u, sib)

    @pl.loop(0, pieces)
    def _(u):
        cols = piece_cols(u)
        to_y(w_half, w_y, W_Y, u).wait_recv()
        x_in = x_buf[:, :, cols].astype(F32).reshape(pair, PIECE)
        x_new = (x_in + y_sum(w_half[u], w_y[u]) + bias_of(bo_rows, u, PIECE)).astype(BF16).astype(F32)
        x_mid[:, cols] = x_new
        hid[pair_rows(c), cols] = x_new
        share_mid(u).start()

    gain = gain_ref[...].astype(F32)
    shift = shift_ref[...].astype(F32)
    d_model = x_mid.shape[1]
    for part in range(2):
        if part == 1:
            @pl.loop(0, pieces)
            def _(u):
                share_mid(u).wait_recv()

        where = pl.ds(pl.multiple_of((c if part == 0 else 1 - c) * pair, 16), pair)
        rows = hid[where, :]
        mean = jnp.mean(rows, axis=-1, keepdims=True)
        cent = rows - mean
        rstd = lax.rsqrt(jnp.mean(cent * cent, axis=-1, keepdims=True) + LN_EPS)
        for n in range(d_model // LANES):
            cols = slice(n * LANES, (n + 1) * LANES)
            hid_b[where, cols] = (cent[:, cols] * rstd * gain[n:n + 1, :] + shift[n:n + 1, :]).astype(BF16)

    together = 3

    @pl.loop(0, chunks // together)
    def _(first):
        group_of = [first * together + e for e in range(together)]
        for j in group_of:
            wait_item(slot_of(j))
        for j in group_of:
            pre = jnp.dot(hid_b[...], ring[slot_of(j)], preferred_element_type=F32) + bias_of(bfc_rows, c * chunks + j, CHUNK)
            cube = pre * pre * pre
            act = 0.5 * pre * (1.0 + jnp.tanh(math.sqrt(2.0 / math.pi) * (pre + 0.044715 * cube)))
            g_buf[:, chunk_cols(j)] = act.astype(BF16)
        for j in group_of:
            load_item(j + RING, slot_of(j))

    def block(j, core, xx):
        return y_all.at[j, pl.ds(2 * core, 2), pl.ds(pl.multiple_of(xx * half, 8), half), :]

    def spread(kind, j):
        ref, who = {J_OWN_X: (block(j, c, x), xpeer), J_OWN_C: (block(j, c, x), sib), J_FWD_C: (block(j, c, 1 - x), sib)}[kind]
        return jcopy(ref, ref, kind, j, who)

    def do_product(j):
        item = chunks + j
        slot = slot_of(item)
        wait_item(slot)
        product = jnp.dot(g_buf[...], ring[slot], preferred_element_type=F32)
        send_product(product, p_part, p_core, J_CORE, j)

        @pl.when(item + RING < 2 * chunks)
        def _():
            load_item(item + RING, slot)

    def do_core_sum(j):
        core_sum(p_part, p_core, p_half, p_y, J_CORE, J_Y, j)

    def do_y_sum(j):
        to_y(p_half, p_y, J_Y, j).wait_recv()
        full = x_mid[:, piece_cols(j)] + y_sum(p_half[j], p_y[j]) + bias_of(bproj_rows, j, PIECE)
        y_all[j, pl.ds(2 * c, 2), pl.ds(pl.multiple_of(x * half, 8), half), :] = full.astype(BF16).astype(F32).reshape(2, half, PIECE)
        spread(J_OWN_X, j).start()
        spread(J_OWN_C, j).start()

    def do_forward(j):
        spread(J_OWN_X, j).wait_recv()
        spread(J_FWD_C, j).start()

    def do_store(j):
        spread(J_OWN_C, j).wait_recv()
        spread(J_FWD_C, j).wait_recv()
        y_ref[:, :, piece_cols(j)] = y_all[j].astype(BF16)

    @pl.loop(0, pieces + 13)
    def _(it):
        product_stage(it, do_product)
        stage(it, 2, do_core_sum)
        stage(it, 7, do_y_sum)
        stage(it, 11, do_forward)
        stage(it, 13, do_store)

    for copy in swaps:
        copy.wait_send()

    @pl.loop(0, pieces)
    def _(j):
        to_core(w_part, w_core, W_CORE, j).wait_send()
        to_y(w_half, w_y, W_Y, j).wait_send()
        share_mid(j).wait_send()
        to_core(p_part, p_core, J_CORE, j).wait_send()
        to_y(p_half, p_y, J_Y, j).wait_send()
        for kind in (J_OWN_X, J_OWN_C, J_FWD_C):
            spread(kind, j).wait_send()


def tail(own, x_in, x_steps, w_o, w_fc, w_proj, b_o, gain, shift, b_fc, b_proj, group, kvs):
    steps, half, _ = own.shape
    batch = 2 * half
    rows = steps * half
    pair = rows // 2
    d_model = w_o.shape[1]
    chunks = d_model // CHUNK
    pieces = d_model // PIECE
    ff_own = w_fc.shape[1] // 2
    assert ff_own == d_model and steps == 4 and kvs == 2
    head_cols = group * LANES
    vm = pl.BlockSpec(memory_space=pltpu.VMEM)
    hbm = pl.BlockSpec(memory_space=pl.ANY)
    cfg = (steps, batch, group, chunks, kvs)
    tiles = lambda vec: vec.reshape(-1, LANES)
    scratch = [
        pltpu.VMEM((steps, half, head_cols), F32),
        pltpu.VMEM((steps, half, head_cols), F32),
        pltpu.VMEM((steps, half, LANES), F32),
        pltpu.VMEM((steps, half, LANES), F32),
        pltpu.VMEM((steps, half, head_cols), F32),
        pltpu.VMEM((steps, half, head_cols), F32),
        pltpu.VMEM((steps, half, LANES), F32),
        pltpu.VMEM((steps, half, LANES), F32),
        pltpu.VMEM((rows, head_cols), BF16),
        pltpu.VMEM((pieces, rows, PIECE), F32),
        pltpu.VMEM((pieces, pair, PIECE), F32),
        pltpu.VMEM((pieces, pair, PIECE), F32),
        pltpu.VMEM((pieces, pair, PIECE), F32),
        pltpu.VMEM((2, half, d_model), BF16),
        pltpu.VMEM((pair, d_model), F32),
        pltpu.VMEM((rows, d_model), F32),
        pltpu.VMEM((rows, d_model), BF16),
        pltpu.VMEM((RING, d_model, CHUNK), BF16),
        pltpu.VMEM((rows, ff_own), BF16),
        pltpu.VMEM((pieces, rows, PIECE), F32),
        pltpu.VMEM((pieces, pair, PIECE), F32),
        pltpu.VMEM((pieces, pair, PIECE), F32),
        pltpu.VMEM((pieces, pair, PIECE), F32),
        pltpu.VMEM((pieces, steps, batch, PIECE), F32),
        pltpu.VMEM((d_model // LANES, LANES), F32),
        pltpu.VMEM((2 * ff_own // LANES, LANES), F32),
        pltpu.VMEM((d_model // LANES, LANES), F32),
        pltpu.SemaphoreType.DMA((4,)),
        pltpu.SemaphoreType.DMA((4,)),
        pltpu.SemaphoreType.DMA((8, pieces)),
        pltpu.SemaphoreType.DMA((8, pieces)),
        pltpu.SemaphoreType.DMA((4,)),
        pltpu.SemaphoreType.DMA((chunks,)),
        pltpu.SemaphoreType.DMA,
        pltpu.SemaphoreType.DMA((RING,)),
    ]
    return pl.pallas_call(
        functools.partial(tail_kernel, cfg),
        out_shape=pltpu.VMEM((steps, batch, d_model), BF16),
        in_specs=[hbm] * 6 + [vm] * 5,
        out_specs=vm,
        scratch_shapes=scratch,
        compiler_params=pltpu.CompilerParams(collective_id=0, has_side_effects=True, vmem_limit_bytes=TAIL_VMEM),
        cost_estimate=pl.CostEstimate(flops=2 * rows * d_model * (head_cols + 2 * ff_own), bytes_accessed=100_000_000, transcendentals=0),
        name="tail",
    )(own, x_in, x_steps, w_o, w_fc, w_proj, tiles(b_o), tiles(gain), tiles(shift), tiles(b_fc), tiles(b_proj))


def solution(mesh):
    sq_size = mesh.shape["sq"]
    act_spec = P(None, "dp", None)
    cache_spec = P("dp", "sq", "tp", None)
    col_spec = P(None, "tp")
    row_spec = P("tp", None)
    vec_spec = P("tp")
    rep_spec = P(None)
    in_specs = (act_spec, P("dp"), cache_spec, cache_spec, col_spec, vec_spec, col_spec, vec_spec,
                col_spec, vec_spec, row_spec, rep_spec, rep_spec, rep_spec, rep_spec, rep_spec,
                col_spec, vec_spec, row_spec, rep_spec)
    out_specs = (act_spec, cache_spec, cache_spec)

    def per_device(x_steps, positions, key_buf, val_buf, w_q, b_q, w_k, b_k, w_v, b_v, w_o, b_o,
                   ln1_gain, ln1_bias, ln2_gain, ln2_bias, w_fc, b_fc, w_proj, b_proj):
        steps, batch, d_model = x_steps.shape
        slots_local, kvs, dim = key_buf.shape[1], key_buf.shape[2], key_buf.shape[3]
        slots = slots_local * sq_size
        group = w_q.shape[1] // (kvs * dim)
        q_rows, k_new, v_new = front(positions, x_steps, ln1_gain, ln1_bias, b_q, b_k, b_v, w_q, w_k, w_v, kvs)
        k_rows = key_buf.reshape(batch, slots_local * kvs, dim)
        v_rows = val_buf.reshape(batch, slots_local * kvs, dim)
        caches = (positions, q_rows, k_new, v_new, k_rows, v_rows, steps, kvs, group, slots)
        k_out, v_out, for_peer = attend(*caches)
        from_peer = lax.ppermute(for_peer, "sq", [(d, d ^ 2) for d in range(sq_size)])
        k_out, v_out, own = attend(*caches, handed=(k_out, v_out))
        ys = tail(own, from_peer, x_steps, w_o, w_fc, w_proj, b_o, ln2_gain, ln2_bias, b_fc, b_proj, group, kvs)
        return ys, k_out.reshape(key_buf.shape), v_out.reshape(val_buf.shape)

    return jax.shard_map(per_device, mesh=mesh, in_specs=in_specs, out_specs=out_specs, check_vma=False)
```
